512 devices in a mesh: grp: 4 (over x), dom: 128 (over z, y, core).
Axes of the slice: x: 4, y: 4, z: 16, core: 2. Of those that a mesh axis runs over, the one named last changes fastest.
Arguments:
- node_state: float32 [65536, 6, 128], P(('grp', 'dom')), may hold values from -6 to 6
- node_dest: int32 [65536], P(('grp', 'dom')), may hold values from 0 to 127, as said below
- seg_nodes: float32 [6, 262144], P(None, ('grp', 'dom')), may hold values from -6 to 6
- seg_conn: int32 [3, 524288], P(None, ('grp', 'dom')), may hold values from 0 to 511
- pair_seg: int32 [512, 4, 32], P(('grp', 'dom')), may hold values from 0 to 7
- pair_slot: int32 [512, 4, 32], P(('grp', 'dom')), may hold values from 0 to 255, as said below
Outputs:
- node_force: float32 [65536, 3, 128], P(('grp', 'dom'))
The draws below stay inside these ranges and needn't reach their ends.
Inputs may be any that keep to these rules, and one draw needn't show every extreme that they name: `node_dest`: at most 2 blocks of one device name the same contact domain; in every grp row one contact domain receives exactly 2 blocks from every device of that row; every device sends at least one block to the contact domain of its own dom index. `pair_slot`: every entry names a slot d * 2 + k that holds a block: device (r, d) sends more than k blocks to the contact domain.
All inputs are finite; a program needn't handle non-finite values.
Results may differ from the reference program's by a relative error of at most 0.00023.
Values sent between devices are 32-bit elements; how exact they have to be, the bound alone decides.
A program may use at most 64 MiB of HBM per device.

```python
import jax
import jax.numpy as jnp
from jax import lax

NODE_BLK = 128
SEG_BLK = 128
NB_DEV = 128
SB_DEV = 8
PAIR_GRP = 32
SN_DEV = 512
CAP = 2
ALL_BLK = 65536
ALL_SEG = 524288
ALL_SN = 262144
N_GRP = 4
N_DOM = 128


def route_tables(key):
    base = jax.random.fold_in(key, 4242)
    key_perm, key_hot, key_shuffle, key_pick = jax.random.split(base, 4)
    senders = N_GRP * N_DOM
    tokens = N_DOM * CAP
    hot_dom = jax.random.randint(key_hot, (N_GRP,), 0, N_DOM)
    perms = jax.vmap(lambda sub_key: jax.random.permutation(sub_key, tokens))(jax.random.split(key_perm, senders))
    sender_ids = jnp.arange(senders, dtype=jnp.int32)
    row_ids = sender_ids // N_DOM
    own_dom = sender_ids % N_DOM
    token_dom = perms // CAP
    is_hot = token_dom == hot_dom[row_ids][:, None]
    is_own = (token_dom == own_dom[:, None]) & (perms % CAP == 0) & jnp.logical_not(is_hot)
    priority = jnp.where(is_hot, 0, jnp.where(is_own, 1, 2))
    score = priority * tokens + jnp.arange(tokens, dtype=jnp.int32)[None, :]
    order_ids = jnp.argsort(score, axis=1)
    chosen = jnp.take_along_axis(perms, order_ids, axis=1)[:, :NB_DEV] // CAP
    shuffles = jax.vmap(lambda sub_key: jax.random.permutation(sub_key, NB_DEV))(jax.random.split(key_shuffle, senders))
    target_dom = jnp.take_along_axis(chosen, shuffles, axis=1).astype(jnp.int32)
    counts = jnp.sum((target_dom[:, :, None] == jnp.arange(N_DOM, dtype=jnp.int32)[None, None, :]).astype(jnp.int32), axis=1)
    per_row = counts.reshape(N_GRP, N_DOM, N_DOM)
    live = jnp.arange(CAP, dtype=jnp.int32)[None, None, None, :] < per_row[:, :, :, None]
    live = jnp.transpose(live, (0, 2, 1, 3)).reshape(N_GRP, N_DOM, N_DOM * CAP).astype(jnp.int32)
    running = jnp.cumsum(live, axis=2)
    total_live = running[:, :, -1]
    raw_pick = jax.random.randint(key_pick, (N_GRP, N_DOM, N_GRP, PAIR_GRP), 0, 1 << 30)
    limit = jnp.transpose(total_live, (1, 0))
    chosen_rank = raw_pick % limit[None, :, :, None]
    run_table = jnp.transpose(running, (1, 0, 2))
    slot_ids = jnp.sum((run_table[None, :, :, None, :] <= chosen_rank[..., None]).astype(jnp.int32), axis=-1)
    return (target_dom.reshape(-1), slot_ids.reshape(N_GRP * N_DOM, N_GRP, PAIR_GRP).astype(jnp.int32))


def draw_node_dest(key, part):
    return route_tables(key)[0]


def draw_pair_slot(key, part):
    return route_tables(key)[1]


def with_ends(drawn, stream_key, smallest, largest):
    dims = drawn.shape
    index_at = [jax.random.randint(jax.random.fold_in(stream_key, axis), (), 0, dims[axis]) for axis in range(len(dims))]
    drawn = drawn.at[tuple(index_at)].set(smallest)
    longest = dims.index(max(dims))
    index_at[longest] = (index_at[longest] + 1) % dims[longest]
    return drawn.at[tuple(index_at)].set(largest)


def level_of(stream_key, shape, pieces, smallest, largest):
    def one(dim, blocks):
        steps = jax.random.uniform(jax.random.fold_in(jax.random.fold_in(stream_key, 6), dim), (blocks,), jnp.float32, smallest / len(pieces), largest / len(pieces))
        return jnp.repeat(jnp.exp(steps), shape[dim] // blocks).reshape((-1,) + (1,) * (len(shape) - dim - 1))

    level = one(*pieces[0])
    for cut in pieces[1:]:
        level = level * one(*cut)
    return level


def normal_values(own_key, dims, scale, most, cuts=(), kind=jnp.bfloat16):
    values = jax.random.normal(own_key, dims, jnp.float32) * scale
    if len(cuts) > 0:
        values = level_of(own_key, dims, cuts, -0.22, 0.18) * values
    return jnp.clip(values, min=-most, max=most).astype(kind)


def setup_inputs(seed: int = 0) -> dict:
    arg_keys = jax.random.split(jax.random.key(seed), 7)
    node_state = normal_values(arg_keys[0], (ALL_BLK, 6, NODE_BLK), 1.0, 6.0, ((0, 512),), jnp.float32)
    node_dest = draw_node_dest(jax.random.fold_in(arg_keys[6], 71), 0)
    seg_nodes = normal_values(arg_keys[2], (6, ALL_SN), 1.0, 6.0, ((1, 512),), jnp.float32)
    seg_conn = with_ends(jax.random.randint(arg_keys[3], (3, ALL_SEG), 0, SN_DEV), jax.random.fold_in(arg_keys[3], 1), 0, SN_DEV - 1).astype(jnp.int32)
    pair_seg = with_ends(jax.random.randint(arg_keys[4], (N_GRP * N_DOM, N_GRP, PAIR_GRP), 0, SB_DEV), jax.random.fold_in(arg_keys[4], 1), 0, SB_DEV - 1).astype(jnp.int32)
    pair_slot = draw_pair_slot(jax.random.fold_in(arg_keys[6], 71), 0)
    return dict(node_state=node_state, node_dest=node_dest, seg_nodes=seg_nodes, seg_conn=seg_conn, pair_seg=pair_seg, pair_slot=pair_slot)


time_step = 0.5
stiffness = 0.5
radius_sq = 0.5


def seg_geometry(corners):
    corner_a = corners[:, 0]
    corner_b = corners[:, 1]
    corner_c = corners[:, 2]
    edge_one = corner_b[0:3] - corner_a[0:3]
    edge_two = corner_c[0:3] - corner_a[0:3]
    normal = 0.5 * jnp.stack([
        edge_one[1] * edge_two[2] - edge_one[2] * edge_two[1],
        edge_one[2] * edge_two[0] - edge_one[0] * edge_two[2],
        edge_one[0] * edge_two[1] - edge_one[1] * edge_two[0]])
    centre = (corner_a[0:3] + corner_b[0:3] + corner_c[0:3]) / 3.0
    motion = (corner_a[3:6] + corner_b[3:6] + corner_c[3:6]) / 3.0
    return jnp.concatenate([normal, centre, motion], axis=0)


def tile_force(node_rows, geometry):
    clearance = jnp.zeros((geometry.shape[1], node_rows.shape[1]), jnp.float32)
    distance = jnp.zeros((geometry.shape[1], node_rows.shape[1]), jnp.float32)
    for axis_id in range(3):
        offset = node_rows[axis_id][None, :] - geometry[3 + axis_id][:, None]
        drift = node_rows[3 + axis_id][None, :] - geometry[6 + axis_id][:, None]
        clearance = clearance + geometry[axis_id][:, None] * (offset + time_step * drift)
        distance = distance + offset * offset
    pressure = stiffness * jnp.exp(-distance / radius_sq) * jnp.maximum(-clearance, 0.0)
    return jnp.dot(geometry[0:3], pressure, precision=lax.Precision.HIGHEST, preferred_element_type=jnp.float32)


def reference(node_state, node_dest, seg_nodes, seg_conn, pair_seg, pair_slot):
    devices = N_GRP * N_DOM
    seg_owner = jnp.arange(seg_conn.shape[1], dtype=jnp.int32) // (SB_DEV * SEG_BLK)
    corners = jnp.take(seg_nodes, seg_conn + (seg_owner * SN_DEV)[None, :], axis=1)
    geometry = seg_geometry(corners)
    geo_blocks = jnp.transpose(geometry.reshape(9, devices * SB_DEV, SEG_BLK), (1, 0, 2))
    target_dom = node_dest.reshape(devices, NB_DEV)
    order_ids = jnp.arange(NB_DEV, dtype=jnp.int32)
    earlier = order_ids[None, :] < order_ids[:, None]
    same_dom = target_dom[:, :, None] == target_dom[:, None, :]
    slot_rank = jnp.sum((same_dom & earlier[None, :, :]).astype(jnp.int32), axis=2)
    device_ids = jnp.arange(devices, dtype=jnp.int32)
    contact_dom = (device_ids % N_DOM)[:, None, None]
    sender = jnp.arange(N_GRP, dtype=jnp.int32)[None, :, None] * N_DOM + pair_slot // CAP
    wanted_rank = pair_slot % CAP
    matching = (target_dom[sender] == contact_dom[..., None]) & (slot_rank[sender] == wanted_rank[..., None])
    local_block = jnp.sum(jnp.where(matching, order_ids, 0), axis=3)
    block_ids = (sender * NB_DEV + local_block).astype(jnp.int32)
    seg_ids = (device_ids[:, None, None] * SB_DEV + pair_seg).astype(jnp.int32)

    def device_forces(device_idx):
        node_rows = jnp.take(node_state, block_ids[device_idx].reshape(-1), axis=0)
        seg_rows = jnp.take(geo_blocks, seg_ids[device_idx].reshape(-1), axis=0)
        return jax.vmap(tile_force)(node_rows, seg_rows)

    forces = lax.map(device_forces, device_ids)
    return jax.ops.segment_sum(forces.reshape(-1, 3, NODE_BLK), block_ids.reshape(-1), num_segments=devices * NB_DEV)
```

```python
import functools

import jax
import jax.numpy as jnp
from jax import lax
from jax.experimental import pallas as pl
from jax.experimental.pallas import tpu as pltpu
from jax.sharding import Mesh
from jax.sharding import PartitionSpec as P

AXES = ("grp", "dom_0", "dom_1", "dom_2")
NX, NZ, NY, NC = 4, 16, 4, 2
MESH = pl.DeviceIdType.MESH
REACH = 3
F32 = jnp.float32

time_step = 0.5
stiffness = 0.5
radius_sq = 0.5


def prep_kernel(dest, node, seg_nodes, conn, pseg, pslot, s_out, geo, tgt, cnt):
    z = lax.axis_index("dom_0")

    def clear(i, _):
        cnt[i] = 0
        return 0

    lax.fori_loop(0, 128, clear, 0, unroll=16)

    def place(i, _):
        d = dest[i]
        k = cnt[d]
        cnt[d] = k + 1
        p = d & 7
        slot = (d >> 3) * 2 + k
        s_out[pl.ds(p * 192 + slot, 6, stride=32), :] = node[i]
        tgt[i] = p * 96 + slot
        return 0

    lax.fori_loop(0, 128, place, 0, unroll=8)

    corners = []
    for k in range(3):
        idx = jnp.concatenate([conn[k : k + 1, b * 128 : (b + 1) * 128] for b in range(8)], axis=0)
        hi = lax.shift_right_logical(idx, 7)
        lo = lax.bitwise_and(idx, 127)
        comps = []
        for i in range(6):
            got = None
            for q in range(4):
                table = jnp.broadcast_to(seg_nodes[i : i + 1, q * 128 : (q + 1) * 128], (8, 128))
                part = jnp.take_along_axis(table, lo, axis=1)
                got = part if got is None else jnp.where(hi == q, part, got)
            comps.append(got)
        corners.append(comps)
    a, b, c = corners
    e1 = [b[i] - a[i] for i in range(3)]
    e2 = [c[i] - a[i] for i in range(3)]
    n = [0.5 * (e1[(i + 1) % 3] * e2[(i + 2) % 3] - e1[(i + 2) % 3] * e2[(i + 1) % 3]) for i in range(3)]
    m = [(a[i] + b[i] + c[i]) / 3.0 for i in range(3)]
    u = [(a[i + 3] + b[i + 3] + c[i + 3]) / 3.0 for i in range(3)]
    off = sum(n[i] * (m[i] + time_step * u[i]) for i in range(3))
    for i, v in enumerate(n + m + [off]):
        geo[pl.ds(i, 8, stride=8), :] = v
    shift = (z & 3) * 32
    for base, tab in ((7, pseg), (39, pslot)):
        t = jnp.concatenate([tab[0].astype(F32), jnp.zeros((4, 96), F32)], axis=1)
        geo[pl.ds(base, 4, stride=8), :] = pltpu.roll(t, shift, 1)


def exchange_kernel(s, geo, n_out, g_out, ys, yr, zs, zr, xs, xr):
    g, z = lax.axis_index("grp"), lax.axis_index("dom_0")
    y, c = lax.axis_index("dom_1"), lax.axis_index("dom_2")
    right, left = (g + 1) % NX, (g + 3) % NX

    def zat(k):
        return (z + k + NZ) % NZ

    peers = [(right, z, y, c), (left, z, y, c)]
    for e in range(1, REACH + 1):
        peers += [(g, zat(e), y, c), (g, zat(-e), y, c)]
    turns = [(dy, dc) for dy in range(NY) for dc in range(NC) if dy or dc]
    for dy, dc in turns:
        peers.append((g, z, (y + dy) % NY, (c + dc) % NC))
    barrier = pltpu.get_barrier_semaphore()
    for peer in peers:
        pl.semaphore_signal(barrier, inc=1, device_id=peer, device_id_type=MESH)
    pl.semaphore_wait(barrier, len(peers))

    me = y * 2 + c
    sends = []

    def send(src, dst, ss, rs, dev):
        copy = pltpu.make_async_remote_copy(
            src_ref=src, dst_ref=dst, send_sem=ss, recv_sem=rs, device_id=dev, device_id_type=MESH
        )
        copy.start()
        sends.append(copy)

    def landed(dst, ss, rs, dev):
        pltpu.make_async_remote_copy(
            src_ref=dst, dst_ref=dst, send_sem=ss, recv_sem=rs, device_id=dev, device_id_type=MESH
        ).wait_recv()

    def number(sign, d):
        return 0 if d == 0 else (d if sign > 0 else 8 + d)

    most = {1: 8, -1: 7}

    def forward_z(sign, p, src):
        for e in range(1, REACH + 1):
            if p + e <= most[sign]:
                k = number(sign, p + e) - 1
                send(src, g_out.at[g, zat(-sign * p)], zs.at[k], zr.at[k], (g, zat(sign * e), y, c))

    def spread_x(sign, d, src):
        k = number(sign, d)
        dst = g_out.at[g, zat(-sign * d)]
        send(src, dst, xs.at[k, 0], xr.at[k, 0], (right, z, y, c))
        send(src, dst, xs.at[k, 1], xr.at[k, 1], (left, z, y, c))

    def relay_x(sign, d):
        k = number(sign, d)
        zz = zat(-sign * d)
        landed(g_out.at[left, zz], xs.at[k, 0], xr.at[k, 0], (left, z, y, c))
        if k % 2 == 0:
            send(g_out.at[left, zz], g_out.at[left, zz], xs.at[k, 2], xr.at[k, 2], (right, z, y, c))
        landed(g_out.at[right, zz], xs.at[k, 1], xr.at[k, 1], (right, z, y, c))
        if k % 2 == 1:
            send(g_out.at[right, zz], g_out.at[right, zz], xs.at[k, 2], xr.at[k, 2], (left, z, y, c))

    for sign in (1, -1):
        forward_z(sign, 0, geo)
    spread_x(1, 0, geo)
    for dy, dc in turns:
        k = dy * 2 + dc - 1
        to_y, to_c = (y + dy) % NY, (c + dc) % NC
        send(s.at[to_y * 2 + to_c], n_out.at[me], ys.at[k], yr.at[k], (g, z, to_y, to_c))
    g_out[g, z] = geo[...]
    n_out[me] = s[me]

    order = [(1, 0)]
    for d in range(1, 9):
        order += [(sign, d) for sign in (1, -1) if d <= most[sign]]
    lag = 4
    for i, (sign, d) in enumerate(order):
        if d > 0:
            k = number(sign, d) - 1
            hop = d - ((d - 1) // REACH) * REACH
            slot = g_out.at[g, zat(-sign * d)]
            landed(slot, zs.at[k], zr.at[k], (g, zat(-sign * hop), y, c))
            if d % REACH == 0:
                forward_z(sign, d, slot)
            spread_x(sign, d, slot)
        if i >= lag:
            relay_x(*order[i - lag])
    for item in order[-lag:]:
        relay_x(*item)
    for sign, d in order:
        k = number(sign, d)
        far = (g + 2) % NX
        came = left if k % 2 == 0 else right
        landed(g_out.at[far, zat(-sign * d)], xs.at[k, 2], xr.at[k, 2], (came, z, y, c))
    for dy, dc in turns:
        k = dy * 2 + dc - 1
        fy, fc = (y - dy + NY) % NY, (c + dc) % NC
        landed(n_out.at[fy * 2 + fc], ys.at[k], yr.at[k], (g, z, fy, fc))
    for copy in sends:
        copy.wait_send()


def force_kernel(n_in, g_in, f_out, lists_v, lists, sem):
    r, z = lax.axis_index("grp"), lax.axis_index("dom_0")

    def rows(base):
        got = None
        for q in range(4):
            part = g_in[pl.ds(q * 64 + base, 16, stride=256), :]
            got = part if got is None else got + part
        return got

    seg = rows(r * 8 + 7)
    slot = rows(r * 8 + 39).astype(jnp.int32)
    lane = lax.broadcasted_iota(jnp.int32, (16, 128), 1)
    sub = lax.broadcasted_iota(jnp.int32, (16, 128), 0)
    src = sub * 4 + lax.shift_right_logical(lane, 5)
    hit = lax.shift_right_logical(slot, 4) == z
    mask = jnp.where(hit, 1.0, 0.0).astype(F32)
    code_a = src.astype(F32)
    code_b = seg * 16.0 + lax.bitwise_and(slot, 15).astype(F32)
    i0 = lax.broadcasted_iota(jnp.int32, (128, 128), 0)
    i1 = lax.broadcasted_iota(jnp.int32, (128, 128), 1)
    before = jnp.where(i0 < i1, 1.0, 0.0).astype(F32)
    inner = jnp.dot(mask, before, preferred_element_type=F32)
    total = jnp.dot(mask, jnp.ones((128, 128), F32), preferred_element_type=F32)
    j0 = lax.broadcasted_iota(jnp.int32, (16, 16), 0)
    j1 = lax.broadcasted_iota(jnp.int32, (16, 16), 1)
    above = jnp.dot(jnp.where(j1 < j0, 1.0, 0.0).astype(F32), total, preferred_element_type=F32)
    pos = (inner + above).astype(jnp.int32)
    high = jnp.where(hit, lax.shift_right_logical(pos, 7), -1)
    low = lax.bitwise_and(pos, 127)
    packed = jnp.zeros((32, 128), F32)
    for i in range(16):
        at = high[i : i + 1] == sub
        left = jnp.concatenate(
            [jnp.where(at, code_a[i : i + 1], 0.0), jnp.where(at, code_b[i : i + 1], 0.0)], axis=0
        )
        spot = jnp.where(low[i : i + 1] == i0, 1.0, 0.0).astype(F32)
        packed = packed + lax.dot_general(left, spot, (((1,), (1,)), ((), ())), preferred_element_type=F32)
    lists_v[0:32, :] = packed.astype(jnp.int32)
    lists_v[32:40, :] = jnp.broadcast_to(total[15:16] + above[15:16], (8, 128)).astype(jnp.int32)
    copy = pltpu.make_async_copy(lists_v, lists, sem)
    copy.start()
    f_out[...] = jnp.zeros_like(f_out)
    copy.wait()

    def pair(p, _):
        a = lists[lax.shift_right_logical(p, 7), lax.bitwise_and(p, 127)]
        b = lists[16 + lax.shift_right_logical(p, 7), lax.bitwise_and(p, 127)]
        t = lax.shift_right_logical(b, 4)
        who = lax.bitwise_and(lax.shift_right_logical(b, 1), 7)
        place = lax.bitwise_and(a, 15) * 2 + lax.bitwise_and(b, 1)
        tile = g_in[pl.ds(pl.multiple_of(a * 64 + t * 8, 8), 8), :]
        node = n_in[pl.ds(who * 192 + place, 6, stride=32), :]
        cols = tile.T
        clear = cols[:, 6:7]
        dist = None
        for i in range(3):
            x = node[i : i + 1]
            w = x + time_step * node[i + 3 : i + 4]
            clear = clear - cols[:, i : i + 1] * w
            o = x - cols[:, i + 3 : i + 4]
            dist = o * o if dist is None else dist + o * o
        press = stiffness * jnp.exp(dist * (-1.0 / radius_sq)) * jnp.maximum(clear, 0.0)
        force = jnp.concatenate(
            [jnp.sum(cols[:, i : i + 1] * press, axis=0, keepdims=True) for i in range(3)], axis=0
        )
        spot = pl.ds(who * 96 + place, 3, stride=32)
        f_out[spot, :] = f_out[spot, :] + force
        return 0

    lax.fori_loop(0, lists[32, 0], pair, 0)


def return_kernel(f, r_out, ys, yr):
    g, z = lax.axis_index("grp"), lax.axis_index("dom_0")
    y, c = lax.axis_index("dom_1"), lax.axis_index("dom_2")
    turns = [(dy, dc) for dy in range(NY) for dc in range(NC) if dy or dc]
    barrier = pltpu.get_barrier_semaphore()
    for dy, dc in turns:
        pl.semaphore_signal(
            barrier, inc=1, device_id=(g, z, (y + dy) % NY, (c + dc) % NC), device_id_type=MESH
        )
    pl.semaphore_wait(barrier, len(turns))
    me = y * 2 + c
    sends = []
    for dy, dc in turns:
        k = dy * 2 + dc - 1
        to_y, to_c = (y + dy) % NY, (c + dc) % NC
        copy = pltpu.make_async_remote_copy(
            src_ref=f.at[to_y * 2 + to_c],
            dst_ref=r_out.at[me],
            send_sem=ys.at[k],
            recv_sem=yr.at[k],
            device_id=(g, z, to_y, to_c),
            device_id_type=MESH,
        )
        copy.start()
        sends.append(copy)
    r_out[me] = f[me]
    for dy, dc in turns:
        k = dy * 2 + dc - 1
        fy, fc = (y - dy + NY) % NY, (c + dc) % NC
        slot = r_out.at[fy * 2 + fc]
        pltpu.make_async_remote_copy(
            src_ref=slot,
            dst_ref=slot,
            send_sem=ys.at[k],
            recv_sem=yr.at[k],
            device_id=(g, z, fy, fc),
            device_id_type=MESH,
        ).wait_recv()
    for copy in sends:
        copy.wait_send()


def order_kernel(tgt, r_in, out):
    def one(i, _):
        out[i] = r_in[pl.ds(tgt[i], 3, stride=32), :]
        return 0

    lax.fori_loop(0, 128, one, 0, unroll=8)


def vmem():
    return pl.BlockSpec(memory_space=pltpu.VMEM)


def smem():
    return pl.BlockSpec(memory_space=pltpu.SMEM)


def shape(*dims, kind=F32):
    return jax.ShapeDtypeStruct(dims, kind)


def shards(node_state, node_dest, seg_nodes, seg_conn, pair_seg, pair_slot):
    dma = pltpu.SemaphoreType.DMA
    placed, geo, tgt = pl.pallas_call(
        prep_kernel,
        name="prep",
        out_shape=(shape(8 * 192, 128), shape(64, 128), shape(128, kind=jnp.int32)),
        in_specs=[smem()] + [vmem()] * 5,
        out_specs=(vmem(), vmem(), smem()),
        scratch_shapes=[pltpu.SMEM((128,), jnp.int32)],
    )(node_dest, node_state, seg_nodes, seg_conn, pair_seg, pair_slot)
    nodes, geos = pl.pallas_call(
        exchange_kernel,
        name="exchange",
        out_shape=(shape(8, 192, 128), shape(NX, NZ, 64, 128)),
        in_specs=[vmem()] * 2,
        out_specs=(vmem(), vmem()),
        scratch_shapes=[dma((7,)), dma((7,)), dma((15,)), dma((15,)), dma((16, 3)), dma((16, 3))],
        compiler_params=pltpu.CompilerParams(collective_id=0, has_side_effects=True),
    )(placed.reshape(8, 192, 128), geo)
    forces = pl.pallas_call(
        force_kernel,
        name="forces",
        out_shape=shape(8 * 96, 128),
        in_specs=[vmem()] * 2,
        out_specs=vmem(),
        scratch_shapes=[pltpu.VMEM((40, 128), jnp.int32), pltpu.SMEM((40, 128), jnp.int32), dma],
    )(nodes.reshape(8 * 192, 128), geos.reshape(NX * NZ * 64, 128))
    back = pl.pallas_call(
        return_kernel,
        name="giveback",
        out_shape=shape(8, 96, 128),
        in_specs=[vmem()],
        out_specs=vmem(),
        scratch_shapes=[dma((7,)), dma((7,))],
        compiler_params=pltpu.CompilerParams(collective_id=1, has_side_effects=True),
    )(forces.reshape(8, 96, 128))
    return pl.pallas_call(
        order_kernel,
        name="order",
        out_shape=shape(128, 3, 128),
        in_specs=[smem(), vmem()],
        out_specs=vmem(),
    )(tgt, back.reshape(8 * 96, 128))


def solution(mesh):
    split = Mesh(mesh.devices.reshape(NX, NZ, NY, NC), AXES)
    placed = (
        P(AXES, None, None),
        P(AXES),
        P(None, AXES),
        P(None, AXES),
        P(AXES, None, None),
        P(AXES, None, None),
    )
    return jax.shard_map(
        shards, mesh=split, in_specs=placed, out_specs=P(AXES, None, None), check_vma=False
    )
```

```python
import math

import jax
import jax.numpy as jnp
from jax import lax
from jax.experimental import pallas as pl
from jax.experimental.pallas import tpu as pltpu
from jax.sharding import Mesh
from jax.sharding import PartitionSpec as P

AXES = ("grp", "dom_0", "dom_1", "dom_2")
NX, NZ, NY, NC = 4, 16, 4, 2
MESH = pl.DeviceIdType.MESH
REACH = 3
BATCH = 8
F32, BF16, I32 = jnp.float32, jnp.bfloat16, jnp.int32

time_step = 0.5
stiffness = 0.5
radius_sq = 0.5
root = math.sqrt(math.log2(math.e) / radius_sq)

TURNS = [(a, b, c) for a in range(NX) for b in range(NY) for c in range(NC) if a or b or c]


def prep_kernel(dest, node, seg_nodes, conn, pseg, pslot, s_out, geo, tgt, cnt, xw):
    def clear(i, _):
        cnt[i] = 0
        return 0

    lax.fori_loop(0, 128, clear, 0, unroll=16)
    x = node[0:384, :]
    xw[0:384, :] = x * root
    xw[384:768, :] = x + time_step * node[384:768, :]

    def place(i, _):
        d = dest[i]
        k = cnt[d]
        cnt[d] = k + 1
        z = lax.shift_right_logical(d, 3)
        p = (z & 3) * 8 + (d & 7)
        slot = lax.shift_right_logical(z, 2) * 2 + k
        s_out[pl.ds(p * 48 + slot, 6, stride=8), :] = xw[pl.ds(i, 6, stride=128), :]
        tgt[i] = p * 24 + slot
        return 0

    lax.fori_loop(0, 128, place, 0, unroll=8)

    corners = []
    for k in range(3):
        idx = jnp.concatenate([conn[k : k + 1, b * 128 : (b + 1) * 128] for b in range(8)], axis=0)
        hi = lax.shift_right_logical(idx, 7)
        lo = lax.bitwise_and(idx, 127)
        comps = []
        for i in range(6):
            got = None
            for q in range(4):
                table = jnp.broadcast_to(seg_nodes[i : i + 1, q * 128 : (q + 1) * 128], (8, 128))
                part = jnp.take_along_axis(table, lo, axis=1)
                got = part if got is None else jnp.where(hi == q, part, got)
            comps.append(got)
        corners.append(comps)
    a, b, c = corners
    e1 = [b[i] - a[i] for i in range(3)]
    e2 = [c[i] - a[i] for i in range(3)]
    n = [0.5 * (e1[(i + 1) % 3] * e2[(i + 2) % 3] - e1[(i + 2) % 3] * e2[(i + 1) % 3]) for i in range(3)]
    m = [(a[i] + b[i] + c[i]) / 3.0 for i in range(3)]
    u = [(a[i + 3] + b[i + 3] + c[i + 3]) / 3.0 for i in range(3)]
    off = sum(n[i] * (m[i] + time_step * u[i]) for i in range(3))
    values = [2.0 * root * v for v in m] + [-stiffness * v for v in n] + [stiffness * off]
    for i, v in enumerate(values):
        geo[pl.ds(i, 8, stride=8), :] = v
    tables = []
    for tab in (pseg, pslot):
        t = jnp.concatenate([tab[0].astype(F32), jnp.zeros((4, 96), F32)], axis=1)
        rows = [pltpu.roll(jnp.broadcast_to(t[r : r + 1], (8, 128)), 32 * r, 1) for r in range(4)]
        tables.append(rows[0] + rows[1] + rows[2] + rows[3])
    sub = lax.broadcasted_iota(I32, (8, 128), 0)
    geo[pl.ds(7, 8, stride=8), :] = jnp.where(sub == 0, tables[0], tables[1])


def start(src, dst, ss, rs, dev):
    copy = pltpu.make_async_remote_copy(
        src_ref=src, dst_ref=dst, send_sem=ss, recv_sem=rs, device_id=dev, device_id_type=MESH
    )
    copy.start()
    return copy


def landed(dst, ss, rs, dev):
    pltpu.make_async_remote_copy(
        src_ref=dst, dst_ref=dst, send_sem=ss, recv_sem=rs, device_id=dev, device_id_type=MESH
    ).wait_recv()


def exchange_kernel(s, geo, n_out, g_out, ys, yr, zs, zr, ws, wr):
    g, z = lax.axis_index("grp"), lax.axis_index("dom_0")
    y, c = lax.axis_index("dom_1"), lax.axis_index("dom_2")

    def zat(k):
        return (z + k + NZ) % NZ

    quad = z % 4
    other = (quad, z - quad + g, y, c)
    diagonal = quad == g
    peers = [((g + a) % NX, z, (y + b) % NY, (c + e) % NC) for a, b, e in TURNS]
    for e in range(1, REACH + 1):
        peers += [(g, zat(e), y, c), (g, zat(-e), y, c)]
    barrier = pltpu.get_barrier_semaphore()
    for peer in peers:
        pl.semaphore_signal(barrier, inc=1, device_id=peer, device_id_type=MESH)

    @pl.when(jnp.logical_not(diagonal))
    def _():
        pl.semaphore_signal(barrier, inc=1, device_id=other, device_id_type=MESH)

    pl.semaphore_wait(barrier, len(peers) + jnp.where(diagonal, 0, 1))
    me = g * 8 + y * 2 + c

    @pl.when(jnp.logical_not(diagonal))
    def _():
        start(geo, g_out.at[other[1]], ws, wr, other)

    def node_send(k):
        a, b, e = TURNS[k]
        dev = ((g + a) % NX, z, (y + b) % NY, (c + e) % NC)
        start(s.at[dev[0] * 8 + dev[2] * 2 + dev[3]], n_out.at[me], ys.at[k], yr.at[k], dev)

    def number(sign, d):
        return (d if sign > 0 else 8 + d) - 1

    most = {1: 8, -1: 7}

    def forward_z(sign, p, src):
        for e in range(1, REACH + 1):
            if p + e <= most[sign]:
                k = number(sign, p + e)
                start(src, g_out.at[zat(-sign * p)], zs.at[k], zr.at[k], (g, zat(sign * e), y, c))

    first = 12
    for k in range(first):
        node_send(k)

    @pl.when(diagonal)
    def _():
        forward_z(1, 0, geo)
        forward_z(-1, 0, geo)
        g_out[z] = geo[...]

    @pl.when(jnp.logical_not(diagonal))
    def _():
        landed(g_out.at[z], ws, wr, other)
        forward_z(1, 0, g_out.at[z])
        forward_z(-1, 0, g_out.at[z])

    for k in range(first, len(TURNS)):
        node_send(k)
    n_out[me] = s[me]

    for d in range(1, 9):
        for sign in (1, -1):
            if d <= most[sign]:
                k = number(sign, d)
                hop = d - ((d - 1) // REACH) * REACH
                slot = g_out.at[zat(-sign * d)]
                landed(slot, zs.at[k], zr.at[k], (g, zat(-sign * hop), y, c))
                if d % REACH == 0:
                    forward_z(sign, d, slot)
    for k, (a, b, e) in enumerate(TURNS):
        dev = ((g - a + NX) % NX, z, (y - b + NY) % NY, (c + e) % NC)
        landed(n_out.at[dev[0] * 8 + dev[2] * 2 + dev[3]], ys.at[k], yr.at[k], dev)

    def left(src, ss, rs, dev):
        pltpu.make_async_remote_copy(
            src_ref=src, dst_ref=src, send_sem=ss, recv_sem=rs, device_id=dev, device_id_type=MESH
        ).wait_send()

    for k, (a, b, e) in enumerate(TURNS):
        dev = ((g + a) % NX, z, (y + b) % NY, (c + e) % NC)
        left(s.at[dev[0] * 8 + dev[2] * 2 + dev[3]], ys.at[k], yr.at[k], dev)
    for sign in (1, -1):
        for d in range(1, most[sign] + 1):
            k = number(sign, d)
            p = ((d - 1) // REACH) * REACH
            left(g_out.at[zat(-sign * p)], zs.at[k], zr.at[k], (g, zat(sign * (d - p)), y, c))

    @pl.when(jnp.logical_not(diagonal))
    def _():
        left(geo, ws, wr, other)


def split3(t):
    a = t.astype(BF16).astype(F32)
    r = t - a
    b = r.astype(BF16).astype(F32)
    return a, b, r - b


def force_kernel(n_in, g_in, f_out, lists_v, lists, sem):
    z = lax.axis_index("dom_0")
    seg = g_in[pl.ds(7, 16, stride=64), :]
    slot = g_in[pl.ds(15, 16, stride=64), :].astype(I32)
    lane = lax.broadcasted_iota(I32, (16, 128), 1)
    sub = lax.broadcasted_iota(I32, (16, 128), 0)
    hit = lax.shift_right_logical(slot, 4) == z
    mask = jnp.where(hit, 1.0, 0.0).astype(F32)
    low4 = lax.bitwise_and(slot, 15)
    code_a = seg + (sub * 8).astype(F32)
    who = lax.shift_right_logical(lane, 5) * 8 + lax.shift_right_logical(low4, 1)
    spot8 = lax.shift_right_logical(sub, 2) * 2 + lax.bitwise_and(low4, 1)
    code_b = (who * 8 + spot8).astype(F32)
    i0 = lax.broadcasted_iota(I32, (128, 128), 0)
    i1 = lax.broadcasted_iota(I32, (128, 128), 1)
    before = jnp.where(i0 < i1, 1.0, 0.0).astype(F32)
    inner = jnp.dot(mask, before, preferred_element_type=F32)
    total = jnp.dot(mask, jnp.ones((128, 128), F32), preferred_element_type=F32)
    j0 = lax.broadcasted_iota(I32, (16, 16), 0)
    j1 = lax.broadcasted_iota(I32, (16, 16), 1)
    above = jnp.dot(jnp.where(j1 < j0, 1.0, 0.0).astype(F32), total, preferred_element_type=F32)
    pos = (inner + above).astype(I32)
    high = jnp.where(hit, lax.shift_right_logical(pos, 7), -1)
    low = lax.bitwise_and(pos, 127)
    packed = jnp.zeros((32, 128), F32)
    for i in range(16):
        at = high[i : i + 1] == sub
        left = jnp.concatenate(
            [jnp.where(at, code_a[i : i + 1], 0.0), jnp.where(at, code_b[i : i + 1], 0.0)], axis=0
        )
        spot = jnp.where(low[i : i + 1] == i0, 1.0, 0.0).astype(F32)
        packed = packed + lax.dot_general(left, spot, (((1,), (1,)), ((), ())), preferred_element_type=F32)
    count = (total[15:16] + above[15:16]).astype(I32)
    code = packed[16:32].astype(I32)
    who = lax.shift_right_logical(code, 3)
    spot8 = lax.bitwise_and(code, 7)
    lists_v[0:16, :] = packed[0:16].astype(I32) * 8
    lists_v[16:32, :] = who * 48 + spot8
    lists_v[32:48, :] = jnp.where(sub * 128 + lane < count, who * 24 + spot8, 32 * 24)
    lists_v[48:56, :] = jnp.broadcast_to(count, (8, 128))
    copy = pltpu.make_async_copy(lists_v, lists, sem)
    copy.start()
    f_out[...] = jnp.zeros_like(f_out)
    copy.wait()

    row = lax.broadcasted_iota(I32, (8, 128), 0)
    ones = jnp.ones((8, 128), F32)
    blank = jnp.zeros((48, 128), BF16)

    def node_side(at):
        t = n_in[pl.ds(at, 6, stride=8), :]
        x0, x1, x2 = t[0:1], t[1:2], t[2:3]
        q = -(x0 * x0 + x1 * x1 + x2 * x2)
        full = jnp.concatenate([t, ones[0:1], q], axis=0)
        a, b, e = split3(full)
        return jnp.concatenate([a, b, a, e, a, b], axis=0).astype(BF16)

    def seg_side(at):
        t = g_in[pl.ds(pl.multiple_of(at, 8), 8), :]
        m0, m1, m2 = t[0:1], t[1:2], t[2:3]
        q = -0.25 * (m0 * m0 + m1 * m1 + m2 * m2)
        dist = jnp.where(row < 3, t, jnp.where(row == 6, q, jnp.where(row == 7, 1.0, 0.0)))
        clear = jnp.where((row >= 3) & (row <= 6), t, 0.0)
        sides = []
        for v in (dist, clear):
            a, b, e = split3(v)
            sides.append(jnp.concatenate([a, a, b, a, e, b], axis=0))
        a = t.astype(BF16).astype(F32)
        return sides[0], sides[1], a, t - a

    def two(p):
        out = []
        for i in range(2):
            q = p + i
            hi, lo = lax.shift_right_logical(q, 7), lax.bitwise_and(q, 127)
            out.append((lists[hi, lo], lists[16 + hi, lo], lists[32 + hi, lo]))
        na, nb = node_side(out[0][1]), node_side(out[1][1])
        rhs = jnp.concatenate(
            [jnp.concatenate([na, blank], axis=1), jnp.concatenate([blank, nb], axis=1)], axis=0
        )
        da, ca, ha, la = seg_side(out[0][0])
        db, cb, hb, lb = seg_side(out[1][0])
        dist = jnp.concatenate([da, db], axis=0).T.astype(BF16)
        clear = jnp.concatenate([ca, cb], axis=0).T.astype(BF16)
        e = jnp.dot(dist, rhs, preferred_element_type=F32)
        w = jnp.dot(clear, rhs, preferred_element_type=F32)
        press = jnp.exp2(e) * jnp.maximum(w, 0.0)
        p_hi = press.astype(BF16)
        p_lo = (press - p_hi.astype(F32)).astype(BF16)
        nothing = jnp.zeros((8, 128), F32)
        left = jnp.concatenate(
            [
                jnp.concatenate([ha, ha], axis=1),
                jnp.concatenate([la, nothing], axis=1),
                jnp.concatenate([hb, hb], axis=1),
                jnp.concatenate([lb, nothing], axis=1),
            ],
            axis=0,
        ).astype(BF16)
        f = jnp.dot(left, jnp.concatenate([p_hi, p_lo], axis=0), preferred_element_type=F32)
        fa = -2.0 * (f[0:8, 0:128] + f[8:16, 0:128])
        fb = -2.0 * (f[16:24, 128:256] + f[24:32, 128:256])
        return [(out[0][2], fa[3:6]), (out[1][2], fb[3:6])]

    def batch(i, _):
        done = []
        for j in range(0, BATCH, 2):
            done += two(i * BATCH + j)
        for at, f in done:
            here = pl.ds(at, 3, stride=8)
            f_out[here, :] = f_out[here, :] + f
        return 0

    lax.fori_loop(0, (lists[48, 0] + BATCH - 1) // BATCH, batch, 0)


def return_kernel(f, r_out, ys, yr):
    g, z = lax.axis_index("grp"), lax.axis_index("dom_0")
    y, c = lax.axis_index("dom_1"), lax.axis_index("dom_2")
    barrier = pltpu.get_barrier_semaphore()
    for a, b, e in TURNS:
        pl.semaphore_signal(
            barrier, inc=1, device_id=((g + a) % NX, z, (y + b) % NY, (c + e) % NC), device_id_type=MESH
        )
    pl.semaphore_wait(barrier, len(TURNS))
    me = g * 8 + y * 2 + c
    sends = []
    for k, (a, b, e) in enumerate(TURNS):
        dev = ((g + a) % NX, z, (y + b) % NY, (c + e) % NC)
        sends.append(start(f.at[dev[0] * 8 + dev[2] * 2 + dev[3]], r_out.at[me], ys.at[k], yr.at[k], dev))
    r_out[me] = f[me]
    for k, (a, b, e) in enumerate(TURNS):
        dev = ((g - a + NX) % NX, z, (y - b + NY) % NY, (c + e) % NC)
        landed(r_out.at[dev[0] * 8 + dev[2] * 2 + dev[3]], ys.at[k], yr.at[k], dev)
    for copy in sends:
        copy.wait_send()


def order_kernel(tgt, r_in, out):
    def one(i, _):
        out[pl.ds(i, 3, stride=128), :] = r_in[pl.ds(tgt[i], 3, stride=8), :]
        return 0

    lax.fori_loop(0, 128, one, 0, unroll=8)


def vmem():
    return pl.BlockSpec(memory_space=pltpu.VMEM)


def smem():
    return pl.BlockSpec(memory_space=pltpu.SMEM)


def shape(*dims, kind=F32):
    return jax.ShapeDtypeStruct(dims, kind)


def shards(node_state, node_dest, seg_nodes, seg_conn, pair_seg, pair_slot):
    dma = pltpu.SemaphoreType.DMA
    many = len(TURNS)
    nodes = jnp.transpose(node_state, (1, 0, 2)).reshape(768, 128)
    placed, geo, tgt = pl.pallas_call(
        prep_kernel,
        name="prep",
        out_shape=(shape(32 * 48, 128), shape(64, 128), shape(128, kind=I32)),
        in_specs=[smem()] + [vmem()] * 5,
        out_specs=(vmem(), vmem(), smem()),
        scratch_shapes=[pltpu.SMEM((128,), I32), pltpu.VMEM((768, 128), F32)],
    )(node_dest, nodes, seg_nodes, seg_conn, pair_seg, pair_slot)
    met, geos = pl.pallas_call(
        exchange_kernel,
        name="exchange",
        out_shape=(shape(32, 48, 128), shape(NZ, 64, 128)),
        in_specs=[vmem()] * 2,
        out_specs=(vmem(), vmem()),
        scratch_shapes=[dma((many,)), dma((many,)), dma((15,)), dma((15,)), dma, dma],
        compiler_params=pltpu.CompilerParams(collective_id=0, has_side_effects=True),
    )(placed.reshape(32, 48, 128), geo)
    forces = pl.pallas_call(
        force_kernel,
        name="forces",
        out_shape=shape(33 * 24, 128),
        in_specs=[vmem()] * 2,
        out_specs=vmem(),
        scratch_shapes=[pltpu.VMEM((56, 128), I32), pltpu.SMEM((56, 128), I32), dma],
    )(met.reshape(32 * 48, 128), geos.reshape(NZ * 64, 128))
    back = pl.pallas_call(
        return_kernel,
        name="giveback",
        out_shape=shape(32, 24, 128),
        in_specs=[vmem()],
        out_specs=vmem(),
        scratch_shapes=[dma((many,)), dma((many,))],
        compiler_params=pltpu.CompilerParams(collective_id=1, has_side_effects=True),
    )(forces.reshape(33, 24, 128))
    rows = pl.pallas_call(
        order_kernel,
        name="order",
        out_shape=shape(384, 128),
        in_specs=[smem(), vmem()],
        out_specs=vmem(),
    )(tgt, back.reshape(32 * 24, 128))
    return jnp.transpose(rows.reshape(3, 128, 128), (1, 0, 2))


def solution(mesh):
    split = Mesh(mesh.devices.reshape(NX, NZ, NY, NC), AXES)
    placed = (
        P(AXES, None, None),
        P(AXES),
        P(None, AXES),
        P(None, AXES),
        P(AXES, None, None),
        P(AXES, None, None),
    )
    return jax.shard_map(
        shards, mesh=split, in_specs=placed, out_specs=P(AXES, None, None), check_vma=False
    )
```

```python
import math

import jax
import jax.numpy as jnp
from jax import lax
from jax.experimental import pallas as pl
from jax.experimental.pallas import tpu as pltpu
from jax.sharding import Mesh
from jax.sharding import PartitionSpec as P

AXES = ("grp", "dom_0", "dom_1", "dom_2")
NX, NZ, NY, NC = 4, 16, 4, 2
MESH = pl.DeviceIdType.MESH
REACH = 3
BATCH = 16
ROOM = 16 << 20
F32, BF16, I32 = jnp.float32, jnp.bfloat16, jnp.int32

time_step = 0.5
stiffness = 0.5
radius_sq = 0.5
root = math.sqrt(math.log2(math.e) / radius_sq)

TURNS = [(a, b, c) for a in range(NX) for b in range(NY) for c in range(NC) if a or b or c]


def prep_kernel(dest, node, seg_nodes, conn, pseg, pslot, s_out, geo, tgt, cnt, xw):
    def clear(i, _):
        cnt[i] = 0
        return 0

    lax.fori_loop(0, 128, clear, 0, unroll=16)
    x = node[0:384, :]
    xw[0:384, :] = x * root
    xw[384:768, :] = x + time_step * node[384:768, :]

    def place(i, _):
        d = dest[i]
        k = cnt[d]
        cnt[d] = k + 1
        z = lax.shift_right_logical(d, 3)
        p = (z & 3) * 8 + (d & 7)
        slot = lax.shift_right_logical(z, 2) * 2 + k
        s_out[pl.ds(p * 48 + slot, 6, stride=8), :] = xw[pl.ds(i, 6, stride=128), :]
        tgt[i] = p * 24 + slot
        return 0

    lax.fori_loop(0, 128, place, 0, unroll=8)

    corners = []
    for k in range(3):
        idx = jnp.concatenate([conn[k : k + 1, b * 128 : (b + 1) * 128] for b in range(8)], axis=0)
        hi = lax.shift_right_logical(idx, 7)
        lo = lax.bitwise_and(idx, 127)
        comps = []
        for i in range(6):
            got = None
            for q in range(4):
                table = jnp.broadcast_to(seg_nodes[i : i + 1, q * 128 : (q + 1) * 128], (8, 128))
                part = jnp.take_along_axis(table, lo, axis=1)
                got = part if got is None else jnp.where(hi == q, part, got)
            comps.append(got)
        corners.append(comps)
    a, b, c = corners
    e1 = [b[i] - a[i] for i in range(3)]
    e2 = [c[i] - a[i] for i in range(3)]
    n = [0.5 * (e1[(i + 1) % 3] * e2[(i + 2) % 3] - e1[(i + 2) % 3] * e2[(i + 1) % 3]) for i in range(3)]
    m = [(a[i] + b[i] + c[i]) / 3.0 for i in range(3)]
    u = [(a[i + 3] + b[i + 3] + c[i + 3]) / 3.0 for i in range(3)]
    off = sum(n[i] * (m[i] + time_step * u[i]) for i in range(3))
    values = [2.0 * root * v for v in m] + [-stiffness * v for v in n] + [stiffness * off]
    for i, v in enumerate(values):
        geo[pl.ds(i, 8, stride=8), :] = v
    tables = []
    for tab in (pseg, pslot):
        t = jnp.concatenate([tab[0].astype(F32), jnp.zeros((4, 96), F32)], axis=1)
        rows = [pltpu.roll(jnp.broadcast_to(t[r : r + 1], (8, 128)), 32 * r, 1) for r in range(4)]
        tables.append(rows[0] + rows[1] + rows[2] + rows[3])
    sub = lax.broadcasted_iota(I32, (8, 128), 0)
    geo[pl.ds(7, 8, stride=8), :] = jnp.where(sub == 0, tables[0], tables[1])


def start(src, dst, ss, rs, dev):
    copy = pltpu.make_async_remote_copy(
        src_ref=src, dst_ref=dst, send_sem=ss, recv_sem=rs, device_id=dev, device_id_type=MESH
    )
    copy.start()
    return copy


def landed(dst, ss, rs, dev):
    pltpu.make_async_remote_copy(
        src_ref=dst, dst_ref=dst, send_sem=ss, recv_sem=rs, device_id=dev, device_id_type=MESH
    ).wait_recv()


def exchange_kernel(s, geo, n_out, g_out, ys, yr, zs, zr, ws, wr):
    g, z = lax.axis_index("grp"), lax.axis_index("dom_0")
    y, c = lax.axis_index("dom_1"), lax.axis_index("dom_2")

    def zat(k):
        return (z + k + NZ) % NZ

    quad = z % 4
    other = (quad, z - quad + g, y, c)
    diagonal = quad == g
    peers = [((g + a) % NX, z, (y + b) % NY, (c + e) % NC) for a, b, e in TURNS]
    for e in range(1, REACH + 1):
        peers += [(g, zat(e), y, c), (g, zat(-e), y, c)]
    barrier = pltpu.get_barrier_semaphore()
    for peer in peers:
        pl.semaphore_signal(barrier, inc=1, device_id=peer, device_id_type=MESH)

    @pl.when(jnp.logical_not(diagonal))
    def _():
        pl.semaphore_signal(barrier, inc=1, device_id=other, device_id_type=MESH)

    pl.semaphore_wait(barrier, len(peers) + jnp.where(diagonal, 0, 1))
    me = g * 8 + y * 2 + c

    @pl.when(jnp.logical_not(diagonal))
    def _():
        start(geo, g_out.at[other[1]], ws, wr, other)

    def node_send(k):
        a, b, e = TURNS[k]
        dev = ((g + a) % NX, z, (y + b) % NY, (c + e) % NC)
        start(s.at[dev[0] * 8 + dev[2] * 2 + dev[3]], n_out.at[me], ys.at[k], yr.at[k], dev)

    def number(sign, d):
        return (d if sign > 0 else 8 + d) - 1

    most = {1: 8, -1: 7}

    def forward_z(sign, p, src):
        for e in range(1, REACH + 1):
            if p + e <= most[sign]:
                k = number(sign, p + e)
                start(src, g_out.at[zat(-sign * p)], zs.at[k], zr.at[k], (g, zat(sign * e), y, c))

    first = 12
    for k in range(first):
        node_send(k)

    @pl.when(diagonal)
    def _():
        forward_z(1, 0, geo)
        forward_z(-1, 0, geo)
        g_out[z] = geo[...]

    @pl.when(jnp.logical_not(diagonal))
    def _():
        landed(g_out.at[z], ws, wr, other)
        forward_z(1, 0, g_out.at[z])
        forward_z(-1, 0, g_out.at[z])

    for k in range(first, len(TURNS)):
        node_send(k)
    n_out[me] = s[me]

    for d in range(1, 9):
        for sign in (1, -1):
            if d <= most[sign]:
                k = number(sign, d)
                hop = d - ((d - 1) // REACH) * REACH
                slot = g_out.at[zat(-sign * d)]
                landed(slot, zs.at[k], zr.at[k], (g, zat(-sign * hop), y, c))
                if d % REACH == 0:
                    forward_z(sign, d, slot)
    for k, (a, b, e) in enumerate(TURNS):
        dev = ((g - a + NX) % NX, z, (y - b + NY) % NY, (c + e) % NC)
        landed(n_out.at[dev[0] * 8 + dev[2] * 2 + dev[3]], ys.at[k], yr.at[k], dev)

    def left(src, ss, rs, dev):
        pltpu.make_async_remote_copy(
            src_ref=src, dst_ref=src, send_sem=ss, recv_sem=rs, device_id=dev, device_id_type=MESH
        ).wait_send()

    for k, (a, b, e) in enumerate(TURNS):
        dev = ((g + a) % NX, z, (y + b) % NY, (c + e) % NC)
        left(s.at[dev[0] * 8 + dev[2] * 2 + dev[3]], ys.at[k], yr.at[k], dev)
    for sign in (1, -1):
        for d in range(1, most[sign] + 1):
            k = number(sign, d)
            p = ((d - 1) // REACH) * REACH
            left(g_out.at[zat(-sign * p)], zs.at[k], zr.at[k], (g, zat(sign * (d - p)), y, c))

    @pl.when(jnp.logical_not(diagonal))
    def _():
        left(geo, ws, wr, other)


def split3(t):
    a = t.astype(BF16).astype(F32)
    r = t - a
    b = r.astype(BF16).astype(F32)
    return a, b, r - b


def force_kernel(n_in, g_in, f_out, lists_v, lists, sem):
    z = lax.axis_index("dom_0")
    seg = g_in[pl.ds(7, 16, stride=64), :]
    slot = g_in[pl.ds(15, 16, stride=64), :].astype(I32)
    lane = lax.broadcasted_iota(I32, (16, 128), 1)
    sub = lax.broadcasted_iota(I32, (16, 128), 0)
    hit = lax.shift_right_logical(slot, 4) == z
    mask = jnp.where(hit, 1.0, 0.0).astype(F32)
    low4 = lax.bitwise_and(slot, 15)
    code_a = seg + (sub * 8).astype(F32)
    who = lax.shift_right_logical(lane, 5) * 8 + lax.shift_right_logical(low4, 1)
    spot8 = lax.shift_right_logical(sub, 2) * 2 + lax.bitwise_and(low4, 1)
    code_b = (who * 8 + spot8).astype(F32)
    i0 = lax.broadcasted_iota(I32, (128, 128), 0)
    i1 = lax.broadcasted_iota(I32, (128, 128), 1)
    before = jnp.where(i0 < i1, 1.0, 0.0).astype(F32)
    inner = jnp.dot(mask, before, preferred_element_type=F32)
    total = jnp.dot(mask, jnp.ones((128, 128), F32), preferred_element_type=F32)
    j0 = lax.broadcasted_iota(I32, (16, 16), 0)
    j1 = lax.broadcasted_iota(I32, (16, 16), 1)
    above = jnp.dot(jnp.where(j1 < j0, 1.0, 0.0).astype(F32), total, preferred_element_type=F32)
    pos = (inner + above).astype(I32)
    high = jnp.where(hit, lax.shift_right_logical(pos, 7), -1)
    low = lax.bitwise_and(pos, 127)
    packed = jnp.zeros((32, 128), F32)
    for i in range(16):
        at = high[i : i + 1] == sub
        left = jnp.concatenate(
            [jnp.where(at, code_a[i : i + 1], 0.0), jnp.where(at, code_b[i : i + 1], 0.0)], axis=0
        )
        spot = jnp.where(low[i : i + 1] == i0, 1.0, 0.0).astype(F32)
        packed = packed + lax.dot_general(left, spot, (((1,), (1,)), ((), ())), preferred_element_type=F32)
    count = (total[15:16] + above[15:16]).astype(I32)
    code = packed[16:32].astype(I32)
    who = lax.shift_right_logical(code, 3)
    spot8 = lax.bitwise_and(code, 7)
    lists_v[0:16, :] = packed[0:16].astype(I32) * 8
    lists_v[16:32, :] = who * 48 + spot8
    lists_v[32:48, :] = jnp.where(sub * 128 + lane < count, who * 24 + spot8, 32 * 24)
    lists_v[48:56, :] = jnp.broadcast_to(count, (8, 128))
    copy = pltpu.make_async_copy(lists_v, lists, sem)
    copy.start()
    f_out[...] = jnp.zeros_like(f_out)
    copy.wait()

    row = lax.broadcasted_iota(I32, (8, 128), 0)
    ones = jnp.ones((8, 128), F32)
    blank = jnp.zeros((48, 128), BF16)

    def node_side(at):
        t = n_in[pl.ds(at, 6, stride=8), :]
        x0, x1, x2 = t[0:1], t[1:2], t[2:3]
        q = -(x0 * x0 + x1 * x1 + x2 * x2)
        full = jnp.concatenate([t, ones[0:1], q], axis=0)
        a, b, e = split3(full)
        return jnp.concatenate([a, b, a, e, a, b], axis=0).astype(BF16)

    def seg_side(at):
        t = g_in[pl.ds(pl.multiple_of(at, 8), 8), :]
        m0, m1, m2 = t[0:1], t[1:2], t[2:3]
        q = -0.25 * (m0 * m0 + m1 * m1 + m2 * m2)
        dist = jnp.where(row < 3, t, jnp.where(row == 6, q, jnp.where(row == 7, 1.0, 0.0)))
        clear = jnp.where((row >= 3) & (row <= 6), t, 0.0)
        sides = []
        for v in (dist, clear):
            a, b, e = split3(v)
            sides.append(jnp.concatenate([a, a, b, a, e, b], axis=0))
        a = t.astype(BF16).astype(F32)
        return sides[0], sides[1], a, t - a

    def build(p):
        out = []
        for i in range(2):
            q = p + i
            hi, lo = lax.shift_right_logical(q, 7), lax.bitwise_and(q, 127)
            out.append((lists[hi, lo], lists[16 + hi, lo], lists[32 + hi, lo]))
        na, nb = node_side(out[0][1]), node_side(out[1][1])
        rhs = jnp.concatenate(
            [jnp.concatenate([na, blank], axis=1), jnp.concatenate([blank, nb], axis=1)], axis=0
        )
        da, ca, ha, la = seg_side(out[0][0])
        db, cb, hb, lb = seg_side(out[1][0])
        dist = jnp.concatenate([da, db], axis=0).T.astype(BF16)
        clear = jnp.concatenate([ca, cb], axis=0).T.astype(BF16)
        nothing = jnp.zeros((8, 128), F32)
        left = jnp.concatenate(
            [
                jnp.concatenate([ha, ha], axis=1),
                jnp.concatenate([la, nothing], axis=1),
                jnp.concatenate([hb, hb], axis=1),
                jnp.concatenate([lb, nothing], axis=1),
            ],
            axis=0,
        ).astype(BF16)
        return dist, clear, rhs, left, out[0][2], out[1][2]

    def pressure(e, w):
        press = jnp.exp2(e) * jnp.maximum(w, 0.0)
        p_hi = press.astype(BF16)
        p_lo = (press - p_hi.astype(F32)).astype(BF16)
        return jnp.concatenate([p_hi, p_lo], axis=0)

    def batch(i, _):
        made = [build(i * BATCH + j) for j in range(0, BATCH, 2)]
        ew = [
            (jnp.dot(m[0], m[2], preferred_element_type=F32), jnp.dot(m[1], m[2], preferred_element_type=F32))
            for m in made
        ]
        ps = [pressure(e, w) for e, w in ew]
        fs = [jnp.dot(m[3], p, preferred_element_type=F32) for m, p in zip(made, ps)]
        for m, f in zip(made, fs):
            fa = -2.0 * (f[0:8, 0:128] + f[8:16, 0:128])
            fb = -2.0 * (f[16:24, 128:256] + f[24:32, 128:256])
            for at, v in ((m[4], fa[3:6]), (m[5], fb[3:6])):
                here = pl.ds(at, 3, stride=8)
                f_out[here, :] = f_out[here, :] + v
        return 0

    lax.fori_loop(0, (lists[48, 0] + BATCH - 1) // BATCH, batch, 0)


def return_kernel(f, r_out, ys, yr):
    g, z = lax.axis_index("grp"), lax.axis_index("dom_0")
    y, c = lax.axis_index("dom_1"), lax.axis_index("dom_2")
    barrier = pltpu.get_barrier_semaphore()
    for a, b, e in TURNS:
        pl.semaphore_signal(
            barrier, inc=1, device_id=((g + a) % NX, z, (y + b) % NY, (c + e) % NC), device_id_type=MESH
        )
    pl.semaphore_wait(barrier, len(TURNS))
    me = g * 8 + y * 2 + c
    sends = []
    for k, (a, b, e) in enumerate(TURNS):
        dev = ((g + a) % NX, z, (y + b) % NY, (c + e) % NC)
        sends.append(start(f.at[dev[0] * 8 + dev[2] * 2 + dev[3]], r_out.at[me], ys.at[k], yr.at[k], dev))
    r_out[me] = f[me]
    for k, (a, b, e) in enumerate(TURNS):
        dev = ((g - a + NX) % NX, z, (y - b + NY) % NY, (c + e) % NC)
        landed(r_out.at[dev[0] * 8 + dev[2] * 2 + dev[3]], ys.at[k], yr.at[k], dev)
    for copy in sends:
        copy.wait_send()


def order_kernel(tgt, r_in, out):
    def one(i, _):
        out[pl.ds(i, 3, stride=128), :] = r_in[pl.ds(tgt[i], 3, stride=8), :]
        return 0

    lax.fori_loop(0, 128, one, 0, unroll=8)


def vmem():
    return pl.BlockSpec(memory_space=pltpu.VMEM)


def smem():
    return pl.BlockSpec(memory_space=pltpu.SMEM)


def shape(*dims, kind=F32):
    return jax.ShapeDtypeStruct(dims, kind)


def shards(node_state, node_dest, seg_nodes, seg_conn, pair_seg, pair_slot):
    dma = pltpu.SemaphoreType.DMA
    many = len(TURNS)
    nodes = jnp.transpose(node_state, (1, 0, 2)).reshape(768, 128)
    placed, geo, tgt = pl.pallas_call(
        prep_kernel,
        name="prep",
        out_shape=(shape(32 * 48, 128), shape(64, 128), shape(128, kind=I32)),
        in_specs=[smem()] + [vmem()] * 5,
        out_specs=(vmem(), vmem(), smem()),
        scratch_shapes=[pltpu.SMEM((128,), I32), pltpu.VMEM((768, 128), F32)],
        compiler_params=pltpu.CompilerParams(vmem_limit_bytes=ROOM),
    )(node_dest, nodes, seg_nodes, seg_conn, pair_seg, pair_slot)
    met, geos = pl.pallas_call(
        exchange_kernel,
        name="exchange",
        out_shape=(shape(32, 48, 128), shape(NZ, 64, 128)),
        in_specs=[vmem()] * 2,
        out_specs=(vmem(), vmem()),
        scratch_shapes=[dma((many,)), dma((many,)), dma((15,)), dma((15,)), dma, dma],
        compiler_params=pltpu.CompilerParams(collective_id=0, has_side_effects=True, vmem_limit_bytes=ROOM),
    )(placed.reshape(32, 48, 128), geo)
    forces = pl.pallas_call(
        force_kernel,
        name="forces",
        out_shape=shape(33 * 24, 128),
        in_specs=[vmem()] * 2,
        out_specs=vmem(),
        scratch_shapes=[pltpu.VMEM((56, 128), I32), pltpu.SMEM((56, 128), I32), dma],
        compiler_params=pltpu.CompilerParams(vmem_limit_bytes=ROOM),
    )(met.reshape(32 * 48, 128), geos.reshape(NZ * 64, 128))
    back = pl.pallas_call(
        return_kernel,
        name="giveback",
        out_shape=shape(32, 24, 128),
        in_specs=[vmem()],
        out_specs=vmem(),
        scratch_shapes=[dma((many,)), dma((many,))],
        compiler_params=pltpu.CompilerParams(collective_id=1, has_side_effects=True, vmem_limit_bytes=ROOM),
    )(forces.reshape(33, 24, 128))
    rows = pl.pallas_call(
        order_kernel,
        name="order",
        out_shape=shape(384, 128),
        in_specs=[smem(), vmem()],
        out_specs=vmem(),
        compiler_params=pltpu.CompilerParams(vmem_limit_bytes=ROOM),
    )(tgt, back.reshape(32 * 24, 128))
    return jnp.transpose(rows.reshape(3, 128, 128), (1, 0, 2))


def solution(mesh):
    split = Mesh(mesh.devices.reshape(NX, NZ, NY, NC), AXES)
    placed = (
        P(AXES, None, None),
        P(AXES),
        P(None, AXES),
        P(None, AXES),
        P(AXES, None, None),
        P(AXES, None, None),
    )
    return jax.shard_map(
        shards, mesh=split, in_specs=placed, out_specs=P(AXES, None, None), check_vma=False
    )
```

```python
import math

import jax
import jax.numpy as jnp
from jax import lax
from jax.experimental import pallas as pl
from jax.experimental.pallas import tpu as pltpu
from jax.sharding import Mesh
from jax.sharding import PartitionSpec as P

AXES = ("grp", "dom_0", "dom_1", "dom_2")
NX, NZ, NY, NC = 4, 16, 4, 2
MESH = pl.DeviceIdType.MESH
REACH = 4
BATCH = 16
ROOM = 16 << 20
F32, BF16, I32 = jnp.float32, jnp.bfloat16, jnp.int32

time_step = 0.5
stiffness = 0.5
radius_sq = 0.5
root = math.sqrt(math.log2(math.e) / radius_sq)

TURNS = [(a, b, c) for a in range(NX) for b in range(NY) for c in range(NC) if a or b or c]


def start(src, dst, ss, rs, dev):
    copy = pltpu.make_async_remote_copy(
        src_ref=src, dst_ref=dst, send_sem=ss, recv_sem=rs, device_id=dev, device_id_type=MESH
    )
    copy.start()
    return copy


def landed(dst, ss, rs, dev):
    pltpu.make_async_remote_copy(
        src_ref=dst, dst_ref=dst, send_sem=ss, recv_sem=rs, device_id=dev, device_id_type=MESH
    ).wait_recv()


def geometry(seg_nodes, conn, pseg, pslot, geo):
    corners = []
    for k in range(3):
        idx = jnp.concatenate([conn[k : k + 1, b * 128 : (b + 1) * 128] for b in range(8)], axis=0)
        hi = lax.shift_right_logical(idx, 7)
        lo = lax.bitwise_and(idx, 127)
        comps = []
        for i in range(6):
            got = None
            for q in range(4):
                table = jnp.broadcast_to(seg_nodes[i : i + 1, q * 128 : (q + 1) * 128], (8, 128))
                part = jnp.take_along_axis(table, lo, axis=1)
                got = part if got is None else jnp.where(hi == q, part, got)
            comps.append(got)
        corners.append(comps)
    a, b, c = corners
    e1 = [b[i] - a[i] for i in range(3)]
    e2 = [c[i] - a[i] for i in range(3)]
    n = [0.5 * (e1[(i + 1) % 3] * e2[(i + 2) % 3] - e1[(i + 2) % 3] * e2[(i + 1) % 3]) for i in range(3)]
    m = [(a[i] + b[i] + c[i]) / 3.0 for i in range(3)]
    u = [(a[i + 3] + b[i + 3] + c[i + 3]) / 3.0 for i in range(3)]
    off = sum(n[i] * (m[i] + time_step * u[i]) for i in range(3))
    values = [2.0 * root * v for v in m] + [-stiffness * v for v in n] + [stiffness * off]
    for i, v in enumerate(values):
        geo[pl.ds(i, 8, stride=8), :] = v
    tables = []
    for tab in (pseg, pslot):
        t = jnp.concatenate([tab[0].astype(F32), jnp.zeros((4, 96), F32)], axis=1)
        rows = [pltpu.roll(jnp.broadcast_to(t[r : r + 1], (8, 128)), 32 * r, 1) for r in range(4)]
        tables.append(rows[0] + rows[1] + rows[2] + rows[3])
    sub = lax.broadcasted_iota(I32, (8, 128), 0)
    geo[pl.ds(7, 8, stride=8), :] = jnp.where(sub == 0, tables[0], tables[1])


def slots_of(dest, inverse, tgt):
    i0 = lax.broadcasted_iota(I32, (128, 128), 0)
    i1 = lax.broadcasted_iota(I32, (128, 128), 1)
    wide = jnp.broadcast_to(dest[0:1, :].astype(F32), (128, 128))
    same = (wide == wide.T) & (i0 < i1)
    rank = jnp.sum(jnp.where(same, 1.0, 0.0), axis=0, keepdims=True).astype(I32)
    d = dest[0:1, :]
    z = lax.shift_right_logical(d, 3)
    p = lax.bitwise_and(z, 3) * 8 + lax.bitwise_and(d, 7)
    slot = lax.shift_right_logical(z, 2) * 2 + rank
    tgt[...] = jnp.broadcast_to(p * 24 + slot, (8, 128))
    column = jnp.broadcast_to((p * 8 + slot).astype(F32), (128, 128)).T.astype(I32)
    for half in range(2):
        found = jnp.sum(jnp.where(column == i1 + 128 * half, i0, 0).astype(F32), axis=0, keepdims=True)
        inverse[8 * half : 8 * half + 8, :] = jnp.broadcast_to(found, (8, 128)).astype(I32)


def exchange_kernel(
    dest_h, node_h, seg_h, conn_h, pseg_h, pslot_h,
    n_out, g_out, tgt,
    dest, node, seg_nodes, conn, pseg, pslot, geo, s, xb, inv_v, inv, ins, ys, yr, zs, zr, ws, wr,
):
    g, z = lax.axis_index("grp"), lax.axis_index("dom_0")
    y, c = lax.axis_index("dom_1"), lax.axis_index("dom_2")
    loads = []
    for i, (src, dst) in enumerate(
        ((conn_h, conn), (seg_h, seg_nodes), (pseg_h, pseg), (pslot_h, pslot), (dest_h, dest), (node_h, node))
    ):
        load = pltpu.make_async_copy(src, dst, ins.at[i])
        load.start()
        loads.append(load)

    def zat(k):
        return (z + k + NZ) % NZ

    quad = z % 4
    other = (quad, z - quad + g, y, c)
    diagonal = quad == g
    peers = [((g + a) % NX, z, (y + b) % NY, (c + e) % NC) for a, b, e in TURNS]
    for e in range(1, REACH + 1):
        peers += [(g, zat(e), y, c), (g, zat(-e), y, c)]
    barrier = pltpu.get_barrier_semaphore()
    for peer in peers:
        pl.semaphore_signal(barrier, inc=1, device_id=peer, device_id_type=MESH)

    @pl.when(jnp.logical_not(diagonal))
    def _():
        pl.semaphore_signal(barrier, inc=1, device_id=other, device_id_type=MESH)

    for load in loads[:4]:
        load.wait()
    geometry(seg_nodes, conn, pseg, pslot, geo)
    loads[4].wait()
    slots_of(dest, inv_v, tgt)
    table = pltpu.make_async_copy(inv_v, inv, ins.at[6])
    table.start()
    pl.semaphore_wait(barrier, len(peers) + jnp.where(diagonal, 0, 1))
    me = g * 8 + y * 2 + c

    def number(sign, d):
        return (d if sign > 0 else 8 + d) - 1

    most = {1: 8, -1: 7}

    def forward_z(sign, p, src):
        for e in range(1, REACH + 1):
            if p + e <= most[sign]:
                k = number(sign, p + e)
                start(src, g_out.at[zat(-sign * p)], zs.at[k], zr.at[k], (g, zat(sign * e), y, c))

    def node_send(k):
        a, b, e = TURNS[k]
        dev = ((g + a) % NX, z, (y + b) % NY, (c + e) % NC)
        start(s.at[dev[0] * 8 + dev[2] * 2 + dev[3]], n_out.at[me], ys.at[k], yr.at[k], dev)

    @pl.when(jnp.logical_not(diagonal))
    def _():
        start(geo, g_out.at[other[1]], ws, wr, other)

    @pl.when(diagonal)
    def _():
        forward_z(1, 0, geo)
        forward_z(-1, 0, geo)
        g_out[z] = geo[...]

    loads[5].wait()

    def turn(j, _):
        at = pl.multiple_of(8 * j, 8)
        for i in range(3):
            x = node[pl.ds(i * 128 + at, 8), :]
            xb[pl.ds(at, 8), i, :] = x * root
            xb[pl.ds(at, 8), i + 3, :] = x + time_step * node[pl.ds((i + 3) * 128 + at, 8), :]
        return 0

    lax.fori_loop(0, 16, turn, 0, unroll=2)
    table.wait()

    def place(p, _):
        for k in range(8):
            block = xb[lax.bitwise_and(inv[8 * (p // 16), (p % 16) * 8 + k], 127)]
            s[p, pl.ds(k, 6, stride=8), :] = block[0:6]
        return 0

    lax.fori_loop(0, 32, place, 0, unroll=2)
    n_out[me] = s[me]
    first = 16
    for k in range(first):
        node_send(k)

    @pl.when(jnp.logical_not(diagonal))
    def _():
        landed(g_out.at[z], ws, wr, other)
        forward_z(1, 0, g_out.at[z])
        forward_z(-1, 0, g_out.at[z])

    for k in range(first, len(TURNS)):
        node_send(k)

    for d in range(1, 9):
        for sign in (1, -1):
            if d <= most[sign]:
                k = number(sign, d)
                hop = d - ((d - 1) // REACH) * REACH
                slot = g_out.at[zat(-sign * d)]
                landed(slot, zs.at[k], zr.at[k], (g, zat(-sign * hop), y, c))
                if d % REACH == 0:
                    forward_z(sign, d, slot)
    for k, (a, b, e) in enumerate(TURNS):
        dev = ((g - a + NX) % NX, z, (y - b + NY) % NY, (c + e) % NC)
        landed(n_out.at[dev[0] * 8 + dev[2] * 2 + dev[3]], ys.at[k], yr.at[k], dev)

    def left(src, ss, rs, dev):
        pltpu.make_async_remote_copy(
            src_ref=src, dst_ref=src, send_sem=ss, recv_sem=rs, device_id=dev, device_id_type=MESH
        ).wait_send()

    for k, (a, b, e) in enumerate(TURNS):
        dev = ((g + a) % NX, z, (y + b) % NY, (c + e) % NC)
        left(s.at[dev[0] * 8 + dev[2] * 2 + dev[3]], ys.at[k], yr.at[k], dev)
    for sign in (1, -1):
        for d in range(1, most[sign] + 1):
            k = number(sign, d)
            p = ((d - 1) // REACH) * REACH
            left(g_out.at[zat(-sign * p)], zs.at[k], zr.at[k], (g, zat(sign * (d - p)), y, c))

    @pl.when(jnp.logical_not(diagonal))
    def _():
        left(geo, ws, wr, other)


def split3(t):
    a = t.astype(BF16).astype(F32)
    r = t - a
    b = r.astype(BF16).astype(F32)
    return a, b, r - b


def force_kernel(n_in, g_in, f_out, lists_v, lists, sem):
    z = lax.axis_index("dom_0")
    seg = g_in[pl.ds(7, 16, stride=64), :]
    slot = g_in[pl.ds(15, 16, stride=64), :].astype(I32)
    lane = lax.broadcasted_iota(I32, (16, 128), 1)
    sub = lax.broadcasted_iota(I32, (16, 128), 0)
    hit = lax.shift_right_logical(slot, 4) == z
    mask = jnp.where(hit, 1.0, 0.0).astype(F32)
    low4 = lax.bitwise_and(slot, 15)
    code_a = seg + (sub * 8).astype(F32)
    who = lax.shift_right_logical(lane, 5) * 8 + lax.shift_right_logical(low4, 1)
    spot8 = lax.shift_right_logical(sub, 2) * 2 + lax.bitwise_and(low4, 1)
    code_b = (who * 8 + spot8).astype(F32)
    i0 = lax.broadcasted_iota(I32, (128, 128), 0)
    i1 = lax.broadcasted_iota(I32, (128, 128), 1)
    before = jnp.where(i0 < i1, 1.0, 0.0).astype(F32)
    inner = jnp.dot(mask, before, preferred_element_type=F32)
    total = jnp.dot(mask, jnp.ones((128, 128), F32), preferred_element_type=F32)
    j0 = lax.broadcasted_iota(I32, (16, 16), 0)
    j1 = lax.broadcasted_iota(I32, (16, 16), 1)
    above = jnp.dot(jnp.where(j1 < j0, 1.0, 0.0).astype(F32), total, preferred_element_type=F32)
    pos = (inner + above).astype(I32)
    high = jnp.where(hit, lax.shift_right_logical(pos, 7), -1)
    low = lax.bitwise_and(pos, 127)
    packed = jnp.zeros((32, 128), F32)
    for i in range(16):
        at = high[i : i + 1] == sub
        left = jnp.concatenate(
            [jnp.where(at, code_a[i : i + 1], 0.0), jnp.where(at, code_b[i : i + 1], 0.0)], axis=0
        )
        spot = jnp.where(low[i : i + 1] == i0, 1.0, 0.0).astype(F32)
        packed = packed + lax.dot_general(left, spot, (((1,), (1,)), ((), ())), preferred_element_type=F32)
    count = (total[15:16] + above[15:16]).astype(I32)
    code = packed[16:32].astype(I32)
    who = lax.shift_right_logical(code, 3)
    spot8 = lax.bitwise_and(code, 7)
    lists_v[0:16, :] = packed[0:16].astype(I32) * 8
    lists_v[16:32, :] = who * 48 + spot8
    lists_v[32:48, :] = jnp.where(sub * 128 + lane < count, who * 24 + spot8, 32 * 24)
    lists_v[48:56, :] = jnp.broadcast_to(count, (8, 128))
    copy = pltpu.make_async_copy(lists_v, lists, sem)
    copy.start()
    f_out[...] = jnp.zeros_like(f_out)
    copy.wait()

    row = lax.broadcasted_iota(I32, (8, 128), 0)
    ones = jnp.ones((8, 128), F32)
    blank = jnp.zeros((48, 128), BF16)

    def node_side(at):
        t = n_in[pl.ds(at, 6, stride=8), :]
        x0, x1, x2 = t[0:1], t[1:2], t[2:3]
        q = -(x0 * x0 + x1 * x1 + x2 * x2)
        full = jnp.concatenate([t, ones[0:1], q], axis=0)
        a, b, e = split3(full)
        return jnp.concatenate([a, b, a, e, a, b], axis=0).astype(BF16)

    def seg_side(at):
        t = g_in[pl.ds(pl.multiple_of(at, 8), 8), :]
        m0, m1, m2 = t[0:1], t[1:2], t[2:3]
        q = -0.25 * (m0 * m0 + m1 * m1 + m2 * m2)
        dist = jnp.where(row < 3, t, jnp.where(row == 6, q, jnp.where(row == 7, 1.0, 0.0)))
        clear = jnp.where((row >= 3) & (row <= 6), t, 0.0)
        sides = []
        for v in (dist, clear):
            a, b, e = split3(v)
            sides.append(jnp.concatenate([a, a, b, a, e, b], axis=0))
        a = t.astype(BF16).astype(F32)
        return sides[0], sides[1], a, t - a

    def build(p):
        out = []
        for i in range(2):
            q = p + i
            hi, lo = lax.shift_right_logical(q, 7), lax.bitwise_and(q, 127)
            out.append((lists[hi, lo], lists[16 + hi, lo], lists[32 + hi, lo]))
        na, nb = node_side(out[0][1]), node_side(out[1][1])
        rhs = jnp.concatenate(
            [jnp.concatenate([na, blank], axis=1), jnp.concatenate([blank, nb], axis=1)], axis=0
        )
        da, ca, ha, la = seg_side(out[0][0])
        db, cb, hb, lb = seg_side(out[1][0])
        dist = jnp.concatenate([da, db], axis=0).T.astype(BF16)
        clear = jnp.concatenate([ca, cb], axis=0).T.astype(BF16)
        nothing = jnp.zeros((8, 128), F32)
        left = jnp.concatenate(
            [
                jnp.concatenate([ha, ha], axis=1),
                jnp.concatenate([la, nothing], axis=1),
                jnp.concatenate([hb, hb], axis=1),
                jnp.concatenate([lb, nothing], axis=1),
            ],
            axis=0,
        ).astype(BF16)
        return dist, clear, rhs, left, out[0][2], out[1][2]

    def pressure(e, w):
        press = jnp.exp2(e) * jnp.maximum(w, 0.0)
        p_hi = press.astype(BF16)
        p_lo = (press - p_hi.astype(F32)).astype(BF16)
        return jnp.concatenate([p_hi, p_lo], axis=0)

    def batch(i, _):
        made = [build(i * BATCH + j) for j in range(0, BATCH, 2)]
        ew = [
            (jnp.dot(m[0], m[2], preferred_element_type=F32), jnp.dot(m[1], m[2], preferred_element_type=F32))
            for m in made
        ]
        ps = [pressure(e, w) for e, w in ew]
        fs = [jnp.dot(m[3], p, preferred_element_type=F32) for m, p in zip(made, ps)]
        for m, f in zip(made, fs):
            fa = -2.0 * (f[0:8, 0:128] + f[8:16, 0:128])
            fb = -2.0 * (f[16:24, 128:256] + f[24:32, 128:256])
            for at, v in ((m[4], fa[3:6]), (m[5], fb[3:6])):
                here = pl.ds(at, 3, stride=8)
                f_out[here, :] = f_out[here, :] + v
        return 0

    lax.fori_loop(0, (lists[48, 0] + BATCH - 1) // BATCH, batch, 0)


def return_kernel(f, r_out, ys, yr):
    g, z = lax.axis_index("grp"), lax.axis_index("dom_0")
    y, c = lax.axis_index("dom_1"), lax.axis_index("dom_2")
    barrier = pltpu.get_barrier_semaphore()
    for a, b, e in TURNS:
        pl.semaphore_signal(
            barrier, inc=1, device_id=((g + a) % NX, z, (y + b) % NY, (c + e) % NC), device_id_type=MESH
        )
    pl.semaphore_wait(barrier, len(TURNS))
    me = g * 8 + y * 2 + c
    sends = []
    for k, (a, b, e) in enumerate(TURNS):
        dev = ((g + a) % NX, z, (y + b) % NY, (c + e) % NC)
        sends.append(start(f.at[dev[0] * 8 + dev[2] * 2 + dev[3]], r_out.at[me], ys.at[k], yr.at[k], dev))
    r_out[me] = f[me]
    for k, (a, b, e) in enumerate(TURNS):
        dev = ((g - a + NX) % NX, z, (y - b + NY) % NY, (c + e) % NC)
        landed(r_out.at[dev[0] * 8 + dev[2] * 2 + dev[3]], ys.at[k], yr.at[k], dev)
    for copy in sends:
        copy.wait_send()


def order_kernel(tgt, r_in, out):
    def one(i, _):
        out[pl.ds(i, 3, stride=128), :] = r_in[pl.ds(tgt[0, i], 3, stride=8), :]
        return 0

    lax.fori_loop(0, 128, one, 0, unroll=8)


def vmem():
    return pl.BlockSpec(memory_space=pltpu.VMEM)


def smem():
    return pl.BlockSpec(memory_space=pltpu.SMEM)


def shape(*dims, kind=F32):
    return jax.ShapeDtypeStruct(dims, kind)


def shards(node_state, node_dest, seg_nodes, seg_conn, pair_seg, pair_slot):
    dma = pltpu.SemaphoreType.DMA
    many = len(TURNS)
    nodes = jnp.transpose(node_state, (1, 0, 2)).reshape(768, 128)
    arrays = (node_dest.reshape(1, 128), nodes, seg_nodes, seg_conn, pair_seg, pair_slot)
    met, geos, tgt = pl.pallas_call(
        exchange_kernel,
        name="exchange",
        out_shape=(shape(32, 48, 128), shape(NZ, 64, 128), shape(8, 128, kind=I32)),
        in_specs=[pl.BlockSpec(memory_space=pltpu.HBM)] * 6,
        out_specs=(vmem(), vmem(), vmem()),
        scratch_shapes=[
            pltpu.VMEM((1, 128), I32),
            pltpu.VMEM((768, 128), F32),
            pltpu.VMEM((6, 512), F32),
            pltpu.VMEM((3, 1024), I32),
            pltpu.VMEM((1, 4, 32), I32),
            pltpu.VMEM((1, 4, 32), I32),
            pltpu.VMEM((64, 128), F32),
            pltpu.VMEM((32, 48, 128), F32),
            pltpu.VMEM((128, 8, 128), F32),
            pltpu.VMEM((16, 128), I32),
            pltpu.SMEM((16, 128), I32),
            dma((7,)),
            dma((many,)),
            dma((many,)),
            dma((15,)),
            dma((15,)),
            dma,
            dma,
        ],
        compiler_params=pltpu.CompilerParams(collective_id=0, has_side_effects=True, vmem_limit_bytes=ROOM),
    )(*(pltpu.with_memory_space_constraint(v, pltpu.HBM) for v in arrays))
    forces = pl.pallas_call(
        force_kernel,
        name="forces",
        out_shape=shape(33 * 24, 128),
        in_specs=[vmem()] * 2,
        out_specs=vmem(),
        scratch_shapes=[pltpu.VMEM((56, 128), I32), pltpu.SMEM((56, 128), I32), dma],
        compiler_params=pltpu.CompilerParams(vmem_limit_bytes=ROOM),
    )(met.reshape(32 * 48, 128), geos.reshape(NZ * 64, 128))
    back = pl.pallas_call(
        return_kernel,
        name="giveback",
        out_shape=shape(32, 24, 128),
        in_specs=[vmem()],
        out_specs=vmem(),
        scratch_shapes=[dma((many,)), dma((many,))],
        compiler_params=pltpu.CompilerParams(collective_id=1, has_side_effects=True, vmem_limit_bytes=ROOM),
    )(forces.reshape(33, 24, 128))
    rows = pl.pallas_call(
        order_kernel,
        name="order",
        out_shape=shape(384, 128),
        in_specs=[smem(), vmem()],
        out_specs=vmem(),
        compiler_params=pltpu.CompilerParams(vmem_limit_bytes=ROOM),
    )(tgt, back.reshape(32 * 24, 128))
    return jnp.transpose(rows.reshape(3, 128, 128), (1, 0, 2))


def solution(mesh):
    split = Mesh(mesh.devices.reshape(NX, NZ, NY, NC), AXES)
    placed = (
        P(AXES, None, None),
        P(AXES),
        P(None, AXES),
        P(None, AXES),
        P(AXES, None, None),
        P(AXES, None, None),
    )
    return jax.shard_map(
        shards, mesh=split, in_specs=placed, out_specs=P(AXES, None, None), check_vma=False
    )
```

```python
import math

import jax
import jax.numpy as jnp
from jax import lax
from jax.experimental import pallas as pl
from jax.experimental.pallas import tpu as pltpu
from jax.sharding import Mesh
from jax.sharding import PartitionSpec as P

AXES = ("grp", "dom_0", "dom_1", "dom_2")
NX, NZ, NY, NC = 4, 16, 4, 2
MESH = pl.DeviceIdType.MESH
PARENT = (0, 1, 0, 3, 4, 3, 6, 6)
USED = 58
BATCH = 16
ROOM = 16 << 20
F32, BF16, I32 = jnp.float32, jnp.bfloat16, jnp.int32

time_step = 0.5
stiffness = 0.5
radius_sq = 0.5
root = math.sqrt(math.log2(math.e) / radius_sq)

TURNS = sorted(
    ((a, b, c) for a in range(NX) for b in range(NY) for c in range(NC) if a or b or c),
    key=lambda t: -min(t[0], NX - t[0]) - min(t[1], NY - t[1]),
)


def start(src, dst, ss, rs, dev):
    copy = pltpu.make_async_remote_copy(
        src_ref=src, dst_ref=dst, send_sem=ss, recv_sem=rs, device_id=dev, device_id_type=MESH
    )
    copy.start()
    return copy


def landed(dst, ss, rs, dev):
    pltpu.make_async_remote_copy(
        src_ref=dst, dst_ref=dst, send_sem=ss, recv_sem=rs, device_id=dev, device_id_type=MESH
    ).wait_recv()


def geometry(seg_nodes, conn, pseg, pslot, geo):
    corners = []
    for k in range(3):
        idx = jnp.concatenate([conn[k : k + 1, b * 128 : (b + 1) * 128] for b in range(8)], axis=0)
        hi = lax.shift_right_logical(idx, 7)
        lo = lax.bitwise_and(idx, 127)
        comps = []
        for i in range(6):
            got = None
            for q in range(4):
                table = jnp.broadcast_to(seg_nodes[i : i + 1, q * 128 : (q + 1) * 128], (8, 128))
                part = jnp.take_along_axis(table, lo, axis=1)
                got = part if got is None else jnp.where(hi == q, part, got)
            comps.append(got)
        corners.append(comps)
    a, b, c = corners
    e1 = [b[i] - a[i] for i in range(3)]
    e2 = [c[i] - a[i] for i in range(3)]
    n = [0.5 * (e1[(i + 1) % 3] * e2[(i + 2) % 3] - e1[(i + 2) % 3] * e2[(i + 1) % 3]) for i in range(3)]
    m = [(a[i] + b[i] + c[i]) / 3.0 for i in range(3)]
    u = [(a[i + 3] + b[i + 3] + c[i + 3]) / 3.0 for i in range(3)]
    off = sum(n[i] * (m[i] + time_step * u[i]) for i in range(3))
    values = [2.0 * root * v for v in m] + [-stiffness * v for v in n] + [stiffness * off]
    for i, v in enumerate(values):
        geo[8 * i : 8 * i + 8, :] = v
    tables = []
    for tab in (pseg, pslot):
        t = jnp.concatenate([tab[0].astype(F32), jnp.zeros((4, 96), F32)], axis=1)
        rows = [pltpu.roll(jnp.broadcast_to(t[r : r + 1], (8, 128)), 32 * r, 1) for r in range(4)]
        tables.append(rows[0] + rows[1] + rows[2] + rows[3])
    for i, t in enumerate(tables):
        geo[56 + i : 57 + i, :] = t[0:1]


def slots_of(dest, inverse, tgt):
    i0 = lax.broadcasted_iota(I32, (128, 128), 0)
    i1 = lax.broadcasted_iota(I32, (128, 128), 1)
    wide = jnp.broadcast_to(dest[0:1, :].astype(F32), (128, 128))
    same = (wide == wide.T) & (i0 < i1)
    rank = jnp.sum(jnp.where(same, 1.0, 0.0), axis=0, keepdims=True).astype(I32)
    d = dest[0:1, :]
    z = lax.shift_right_logical(d, 3)
    p = lax.bitwise_and(z, 3) * 8 + lax.bitwise_and(d, 7)
    slot = lax.shift_right_logical(z, 2) * 2 + rank
    tgt[...] = jnp.broadcast_to(p * 24 + slot, (8, 128))
    column = jnp.broadcast_to((p * 8 + slot).astype(F32), (128, 128)).T.astype(I32)
    for half in range(2):
        found = jnp.sum(jnp.where(column == i1 + 128 * half, i0, 0).astype(F32), axis=0, keepdims=True)
        inverse[8 * half : 8 * half + 8, :] = jnp.broadcast_to(found, (8, 128)).astype(I32)


def exchange_kernel(
    dest_h, node_h, seg_h, conn_h, pseg_h, pslot_h,
    n_out, g_out, tgt,
    dest, node, seg_nodes, conn, pseg, pslot, geo, s, xb, inv_v, inv, ins, ys, yr, zs, zr, ws, wr,
):
    g, z = lax.axis_index("grp"), lax.axis_index("dom_0")
    y, c = lax.axis_index("dom_1"), lax.axis_index("dom_2")
    loads = []
    for i, (src, dst) in enumerate(
        ((conn_h, conn), (seg_h, seg_nodes), (pseg_h, pseg), (pslot_h, pslot), (dest_h, dest), (node_h, node))
    ):
        load = pltpu.make_async_copy(src, dst, ins.at[i])
        load.start()
        loads.append(load)

    def zat(k):
        return (z + k + NZ) % NZ

    quad = z % 4
    other = (quad, z - quad + g, y, c)
    diagonal = quad == g
    peers = [((g + a) % NX, z, (y + b) % NY, (c + e) % NC) for a, b, e in TURNS]
    for e in sorted({d - p for d, p in enumerate(PARENT, 1)}):
        peers += [(g, zat(e), y, c), (g, zat(-e), y, c)]
    barrier = pltpu.get_barrier_semaphore()
    for peer in peers:
        pl.semaphore_signal(barrier, inc=1, device_id=peer, device_id_type=MESH)

    @pl.when(jnp.logical_not(diagonal))
    def _():
        pl.semaphore_signal(barrier, inc=1, device_id=other, device_id_type=MESH)

    for load in loads[:4]:
        load.wait()
    geometry(seg_nodes, conn, pseg, pslot, geo)
    loads[4].wait()
    slots_of(dest, inv_v, tgt)
    table = pltpu.make_async_copy(inv_v, inv, ins.at[6])
    table.start()
    pl.semaphore_wait(barrier, len(peers) + jnp.where(diagonal, 0, 1))
    me = g * 8 + y * 2 + c

    def number(sign, d):
        return (d if sign > 0 else 8 + d) - 1

    most = {1: 8, -1: 7}

    def children(p, sign):
        mine = [d for d in range(1, most[sign] + 1) if PARENT[d - 1] == p]
        return sorted(mine, key=lambda d: (d not in PARENT, -d))

    used = pl.ds(0, USED)

    def forward_z(sign, p, src):
        for d in children(p, sign):
            k = number(sign, d)
            start(src, g_out.at[zat(-sign * p), used], zs.at[k], zr.at[k], (g, zat(sign * (d - p)), y, c))

    def arrive_z(sign, d):
        k = number(sign, d)
        slot = g_out.at[zat(-sign * d), used]
        landed(slot, zs.at[k], zr.at[k], (g, zat(-sign * (d - PARENT[d - 1])), y, c))
        forward_z(sign, d, slot)

    def node_send(k):
        a, b, e = TURNS[k]
        dev = ((g + a) % NX, z, (y + b) % NY, (c + e) % NC)
        start(s.at[dev[0] * 8 + dev[2] * 2 + dev[3]], n_out.at[me], ys.at[k], yr.at[k], dev)

    @pl.when(jnp.logical_not(diagonal))
    def _():
        start(geo.at[used], g_out.at[other[1], used], ws, wr, other)

    @pl.when(diagonal)
    def _():
        forward_z(1, 0, geo.at[used])
        forward_z(-1, 0, geo.at[used])
        g_out[z] = geo[...]

    loads[5].wait()

    def turn(j, _):
        at = pl.multiple_of(8 * j, 8)
        for i in range(3):
            x = node[pl.ds(i * 128 + at, 8), :]
            xb[pl.ds(at, 8), i, :] = x * root
            xb[pl.ds(at, 8), i + 3, :] = x + time_step * node[pl.ds((i + 3) * 128 + at, 8), :]
        return 0

    lax.fori_loop(0, 16, turn, 0, unroll=2)
    table.wait()

    def place(p, _):
        for k in range(8):
            block = xb[lax.bitwise_and(inv[8 * (p // 16), (p % 16) * 8 + k], 127)]
            s[p, pl.ds(k, 6, stride=8), :] = block[0:6]
        return 0

    lax.fori_loop(0, 32, place, 0, unroll=2)
    n_out[me] = s[me]
    first = 31
    for k in range(first):
        node_send(k)

    @pl.when(jnp.logical_not(diagonal))
    def _():
        landed(g_out.at[z, used], ws, wr, other)
        forward_z(1, 0, g_out.at[z, used])
        forward_z(-1, 0, g_out.at[z, used])

    for k in range(first, len(TURNS)):
        node_send(k)

    inner = sorted(set(PARENT) - {0})
    for d in inner + [d for d in range(1, 9) if d not in inner]:
        for sign in (1, -1):
            if d <= most[sign]:
                arrive_z(sign, d)
    for k, (a, b, e) in enumerate(TURNS):
        dev = ((g - a + NX) % NX, z, (y - b + NY) % NY, (c + e) % NC)
        landed(n_out.at[dev[0] * 8 + dev[2] * 2 + dev[3]], ys.at[k], yr.at[k], dev)

    def left(src, ss, rs, dev):
        pltpu.make_async_remote_copy(
            src_ref=src, dst_ref=src, send_sem=ss, recv_sem=rs, device_id=dev, device_id_type=MESH
        ).wait_send()

    for k, (a, b, e) in enumerate(TURNS):
        dev = ((g + a) % NX, z, (y + b) % NY, (c + e) % NC)
        left(s.at[dev[0] * 8 + dev[2] * 2 + dev[3]], ys.at[k], yr.at[k], dev)
    for sign in (1, -1):
        for d in range(1, most[sign] + 1):
            k = number(sign, d)
            p = PARENT[d - 1]
            left(g_out.at[zat(-sign * p), used], zs.at[k], zr.at[k], (g, zat(sign * (d - p)), y, c))

    @pl.when(jnp.logical_not(diagonal))
    def _():
        left(geo.at[used], ws, wr, other)


def split3(t):
    a = t.astype(BF16).astype(F32)
    r = t - a
    b = r.astype(BF16).astype(F32)
    return a, b, r - b


def force_kernel(n_in, g_in, f_out, lists_v, lists, sem):
    z = lax.axis_index("dom_0")
    seg = g_in[pl.ds(56, 16, stride=64), :]
    slot = g_in[pl.ds(57, 16, stride=64), :].astype(I32)
    lane = lax.broadcasted_iota(I32, (16, 128), 1)
    sub = lax.broadcasted_iota(I32, (16, 128), 0)
    hit = lax.shift_right_logical(slot, 4) == z
    mask = jnp.where(hit, 1.0, 0.0).astype(F32)
    low4 = lax.bitwise_and(slot, 15)
    code_a = seg + (sub * 8).astype(F32)
    who = lax.shift_right_logical(lane, 5) * 8 + lax.shift_right_logical(low4, 1)
    spot8 = lax.shift_right_logical(sub, 2) * 2 + lax.bitwise_and(low4, 1)
    code_b = (who * 8 + spot8).astype(F32)
    i0 = lax.broadcasted_iota(I32, (128, 128), 0)
    i1 = lax.broadcasted_iota(I32, (128, 128), 1)
    before = jnp.where(i0 < i1, 1.0, 0.0).astype(F32)
    inner = jnp.dot(mask, before, preferred_element_type=F32)
    total = jnp.dot(mask, jnp.ones((128, 128), F32), preferred_element_type=F32)
    j0 = lax.broadcasted_iota(I32, (16, 16), 0)
    j1 = lax.broadcasted_iota(I32, (16, 16), 1)
    above = jnp.dot(jnp.where(j1 < j0, 1.0, 0.0).astype(F32), total, preferred_element_type=F32)
    pos = (inner + above).astype(I32)
    high = jnp.where(hit, lax.shift_right_logical(pos, 7), -1)
    low = lax.bitwise_and(pos, 127)
    packed = jnp.zeros((32, 128), F32)
    for i in range(16):
        at = high[i : i + 1] == sub
        left = jnp.concatenate(
            [jnp.where(at, code_a[i : i + 1], 0.0), jnp.where(at, code_b[i : i + 1], 0.0)], axis=0
        )
        spot = jnp.where(low[i : i + 1] == i0, 1.0, 0.0).astype(F32)
        packed = packed + lax.dot_general(left, spot, (((1,), (1,)), ((), ())), preferred_element_type=F32)
    count = (total[15:16] + above[15:16]).astype(I32)
    code = packed[16:32].astype(I32)
    who = lax.shift_right_logical(code, 3)
    spot8 = lax.bitwise_and(code, 7)
    tile = packed[0:16].astype(I32)
    lists_v[0:16, :] = lax.shift_right_logical(tile, 3) * 64 + lax.bitwise_and(tile, 7)
    lists_v[16:32, :] = who * 48 + spot8
    lists_v[32:48, :] = jnp.where(sub * 128 + lane < count, who * 24 + spot8, 32 * 24)
    lists_v[48:56, :] = jnp.broadcast_to(count, (8, 128))
    copy = pltpu.make_async_copy(lists_v, lists, sem)
    copy.start()
    f_out[...] = jnp.zeros_like(f_out)
    copy.wait()

    row = lax.broadcasted_iota(I32, (8, 128), 0)
    ones = jnp.ones((8, 128), F32)
    blank = jnp.zeros((48, 128), BF16)

    def node_side(at):
        t = n_in[pl.ds(at, 6, stride=8), :]
        x0, x1, x2 = t[0:1], t[1:2], t[2:3]
        q = -(x0 * x0 + x1 * x1 + x2 * x2)
        full = jnp.concatenate([t, ones[0:1], q], axis=0)
        a, b, e = split3(full)
        return jnp.concatenate([a, b, a, e, a, b], axis=0).astype(BF16)

    def seg_side(at):
        t = g_in[pl.ds(at, 8, stride=8), :]
        m0, m1, m2 = t[0:1], t[1:2], t[2:3]
        q = -0.25 * (m0 * m0 + m1 * m1 + m2 * m2)
        dist = jnp.where(row < 3, t, jnp.where(row == 6, q, jnp.where(row == 7, 1.0, 0.0)))
        clear = jnp.where((row >= 3) & (row <= 6), t, 0.0)
        sides = []
        for v in (dist, clear):
            a, b, e = split3(v)
            sides.append(jnp.concatenate([a, a, b, a, e, b], axis=0))
        a = t.astype(BF16).astype(F32)
        return sides[0], sides[1], a, t - a

    def build(p):
        out = []
        for i in range(2):
            q = p + i
            hi, lo = lax.shift_right_logical(q, 7), lax.bitwise_and(q, 127)
            out.append((lists[hi, lo], lists[16 + hi, lo], lists[32 + hi, lo]))
        na, nb = node_side(out[0][1]), node_side(out[1][1])
        rhs = jnp.concatenate(
            [jnp.concatenate([na, blank], axis=1), jnp.concatenate([blank, nb], axis=1)], axis=0
        )
        da, ca, ha, la = seg_side(out[0][0])
        db, cb, hb, lb = seg_side(out[1][0])
        dist = jnp.concatenate([da, db], axis=0).T.astype(BF16)
        clear = jnp.concatenate([ca, cb], axis=0).T.astype(BF16)
        nothing = jnp.zeros((8, 128), F32)
        left = jnp.concatenate(
            [
                jnp.concatenate([ha, ha], axis=1),
                jnp.concatenate([la, nothing], axis=1),
                jnp.concatenate([hb, hb], axis=1),
                jnp.concatenate([lb, nothing], axis=1),
            ],
            axis=0,
        ).astype(BF16)
        return dist, clear, rhs, left, out[0][2], out[1][2]

    def pressure(e, w):
        press = jnp.exp2(e) * jnp.maximum(w, 0.0)
        p_hi = press.astype(BF16)
        p_lo = (press - p_hi.astype(F32)).astype(BF16)
        return jnp.concatenate([p_hi, p_lo], axis=0)

    def batch(i, _):
        made = [build(i * BATCH + j) for j in range(0, BATCH, 2)]
        ew = [
            (jnp.dot(m[0], m[2], preferred_element_type=F32), jnp.dot(m[1], m[2], preferred_element_type=F32))
            for m in made
        ]
        ps = [pressure(e, w) for e, w in ew]
        fs = [jnp.dot(m[3], p, preferred_element_type=F32) for m, p in zip(made, ps)]
        for m, f in zip(made, fs):
            fa = -2.0 * (f[0:8, 0:128] + f[8:16, 0:128])
            fb = -2.0 * (f[16:24, 128:256] + f[24:32, 128:256])
            for at, v in ((m[4], fa[3:6]), (m[5], fb[3:6])):
                here = pl.ds(at, 3, stride=8)
                f_out[here, :] = f_out[here, :] + v
        return 0

    lax.fori_loop(0, (lists[48, 0] + BATCH - 1) // BATCH, batch, 0)


def return_kernel(f, r_out, ys, yr):
    g, z = lax.axis_index("grp"), lax.axis_index("dom_0")
    y, c = lax.axis_index("dom_1"), lax.axis_index("dom_2")
    barrier = pltpu.get_barrier_semaphore()
    for a, b, e in TURNS:
        pl.semaphore_signal(
            barrier, inc=1, device_id=((g + a) % NX, z, (y + b) % NY, (c + e) % NC), device_id_type=MESH
        )
    pl.semaphore_wait(barrier, len(TURNS))
    me = g * 8 + y * 2 + c
    sends = []
    for k, (a, b, e) in enumerate(TURNS):
        dev = ((g + a) % NX, z, (y + b) % NY, (c + e) % NC)
        sends.append(start(f.at[dev[0] * 8 + dev[2] * 2 + dev[3]], r_out.at[me], ys.at[k], yr.at[k], dev))
    r_out[me] = f[me]
    for k, (a, b, e) in enumerate(TURNS):
        dev = ((g - a + NX) % NX, z, (y - b + NY) % NY, (c + e) % NC)
        landed(r_out.at[dev[0] * 8 + dev[2] * 2 + dev[3]], ys.at[k], yr.at[k], dev)
    for copy in sends:
        copy.wait_send()


def order_kernel(tgt, r_in, out):
    def one(i, _):
        out[pl.ds(i, 3, stride=128), :] = r_in[pl.ds(tgt[0, i], 3, stride=8), :]
        return 0

    lax.fori_loop(0, 128, one, 0, unroll=8)


def vmem():
    return pl.BlockSpec(memory_space=pltpu.VMEM)


def smem():
    return pl.BlockSpec(memory_space=pltpu.SMEM)


def shape(*dims, kind=F32):
    return jax.ShapeDtypeStruct(dims, kind)


def meet(node_state, node_dest, seg_nodes, seg_conn, pair_seg, pair_slot):
    dma = pltpu.SemaphoreType.DMA
    many = len(TURNS)
    nodes = jnp.transpose(node_state, (1, 0, 2)).reshape(768, 128)
    arrays = (node_dest.reshape(1, 128), nodes, seg_nodes, seg_conn, pair_seg, pair_slot)
    return pl.pallas_call(
        exchange_kernel,
        name="exchange",
        out_shape=(shape(32, 48, 128), shape(NZ, 64, 128), shape(8, 128, kind=I32)),
        in_specs=[pl.BlockSpec(memory_space=pltpu.HBM)] * 6,
        out_specs=(vmem(), vmem(), vmem()),
        scratch_shapes=[
            pltpu.VMEM((1, 128), I32),
            pltpu.VMEM((768, 128), F32),
            pltpu.VMEM((6, 512), F32),
            pltpu.VMEM((3, 1024), I32),
            pltpu.VMEM((1, 4, 32), I32),
            pltpu.VMEM((1, 4, 32), I32),
            pltpu.VMEM((64, 128), F32),
            pltpu.VMEM((32, 48, 128), F32),
            pltpu.VMEM((128, 8, 128), F32),
            pltpu.VMEM((16, 128), I32),
            pltpu.SMEM((16, 128), I32),
            dma((7,)),
            dma((many,)),
            dma((many,)),
            dma((15,)),
            dma((15,)),
            dma,
            dma,
        ],
        compiler_params=pltpu.CompilerParams(collective_id=0, has_side_effects=True, vmem_limit_bytes=ROOM),
    )(*(pltpu.with_memory_space_constraint(v, pltpu.HBM) for v in arrays))


def give_back(forces):
    dma = pltpu.SemaphoreType.DMA
    many = len(TURNS)
    return pl.pallas_call(
        return_kernel,
        name="giveback",
        out_shape=shape(32, 24, 128),
        in_specs=[vmem()],
        out_specs=vmem(),
        scratch_shapes=[dma((many,)), dma((many,))],
        compiler_params=pltpu.CompilerParams(collective_id=1, has_side_effects=True, vmem_limit_bytes=ROOM),
    )(forces.reshape(33, 24, 128))


def shards(node_state, node_dest, seg_nodes, seg_conn, pair_seg, pair_slot):
    dma = pltpu.SemaphoreType.DMA
    many = len(TURNS)
    met, geos, tgt = meet(node_state, node_dest, seg_nodes, seg_conn, pair_seg, pair_slot)
    forces = pl.pallas_call(
        force_kernel,
        name="forces",
        out_shape=shape(33 * 24, 128),
        in_specs=[vmem()] * 2,
        out_specs=vmem(),
        scratch_shapes=[pltpu.VMEM((56, 128), I32), pltpu.SMEM((56, 128), I32), dma],
        compiler_params=pltpu.CompilerParams(vmem_limit_bytes=ROOM),
    )(met.reshape(32 * 48, 128), geos.reshape(NZ * 64, 128))
    back = give_back(forces)
    rows = pl.pallas_call(
        order_kernel,
        name="order",
        out_shape=shape(384, 128),
        in_specs=[smem(), vmem()],
        out_specs=vmem(),
        compiler_params=pltpu.CompilerParams(vmem_limit_bytes=ROOM),
    )(tgt, back.reshape(32 * 24, 128))
    return jnp.transpose(rows.reshape(3, 128, 128), (1, 0, 2))


def solution(mesh):
    split = Mesh(mesh.devices.reshape(NX, NZ, NY, NC), AXES)
    placed = (
        P(AXES, None, None),
        P(AXES),
        P(None, AXES),
        P(None, AXES),
        P(AXES, None, None),
        P(AXES, None, None),
    )
    return jax.shard_map(
        shards, mesh=split, in_specs=placed, out_specs=P(AXES, None, None), check_vma=False
    )
```

```python
import math

import jax
import jax.numpy as jnp
from jax import lax
from jax.experimental import pallas as pl
from jax.experimental.pallas import tpu as pltpu
from jax.sharding import Mesh
from jax.sharding import PartitionSpec as P

AXES = ("grp", "dom_0", "dom_1", "dom_2")
NX, NZ, NY, NC = 4, 16, 4, 2
MESH = pl.DeviceIdType.MESH
PARENT = (0, 1, 0, 3, 4, 3, 6, 6)
USED = 58
SIZES = (32, 16, 8)
ROOM = 16 << 20
F32, BF16, I32 = jnp.float32, jnp.bfloat16, jnp.int32

time_step = 0.5
stiffness = 0.5
radius_sq = 0.5
root = math.sqrt(math.log2(math.e) / radius_sq)

TURNS = sorted(
    ((a, b, c) for a in range(NX) for b in range(NY) for c in range(NC) if a or b or c),
    key=lambda t: -min(t[0], NX - t[0]) - min(t[1], NY - t[1]),
)


def start(src, dst, ss, rs, dev):
    copy = pltpu.make_async_remote_copy(
        src_ref=src, dst_ref=dst, send_sem=ss, recv_sem=rs, device_id=dev, device_id_type=MESH
    )
    copy.start()
    return copy


def landed(dst, ss, rs, dev):
    pltpu.make_async_remote_copy(
        src_ref=dst, dst_ref=dst, send_sem=ss, recv_sem=rs, device_id=dev, device_id_type=MESH
    ).wait_recv()


def geometry(seg_nodes, conn, pseg, pslot, geo):
    corners = []
    for k in range(3):
        idx = jnp.concatenate([conn[k : k + 1, b * 128 : (b + 1) * 128] for b in range(8)], axis=0)
        hi = lax.shift_right_logical(idx, 7)
        lo = lax.bitwise_and(idx, 127)
        comps = []
        for i in range(6):
            got = None
            for q in range(4):
                table = jnp.broadcast_to(seg_nodes[i : i + 1, q * 128 : (q + 1) * 128], (8, 128))
                part = jnp.take_along_axis(table, lo, axis=1)
                got = part if got is None else jnp.where(hi == q, part, got)
            comps.append(got)
        corners.append(comps)
    a, b, c = corners
    e1 = [b[i] - a[i] for i in range(3)]
    e2 = [c[i] - a[i] for i in range(3)]
    n = [0.5 * (e1[(i + 1) % 3] * e2[(i + 2) % 3] - e1[(i + 2) % 3] * e2[(i + 1) % 3]) for i in range(3)]
    m = [(a[i] + b[i] + c[i]) / 3.0 for i in range(3)]
    u = [(a[i + 3] + b[i + 3] + c[i + 3]) / 3.0 for i in range(3)]
    off = sum(n[i] * (m[i] + time_step * u[i]) for i in range(3))
    values = [2.0 * root * v for v in m] + [-stiffness * v for v in n] + [stiffness * off]
    for i, v in enumerate(values):
        geo[8 * i : 8 * i + 8, :] = v
    tables = []
    for tab in (pseg, pslot):
        t = jnp.concatenate([tab[0].astype(F32), jnp.zeros((4, 96), F32)], axis=1)
        rows = [pltpu.roll(jnp.broadcast_to(t[r : r + 1], (8, 128)), 32 * r, 1) for r in range(4)]
        tables.append(rows[0] + rows[1] + rows[2] + rows[3])
    for i, t in enumerate(tables):
        geo[56 + i : 57 + i, :] = t[0:1]


def slots_of(dest, inverse, tgt):
    i0 = lax.broadcasted_iota(I32, (128, 128), 0)
    i1 = lax.broadcasted_iota(I32, (128, 128), 1)
    wide = jnp.broadcast_to(dest[0:1, :].astype(F32), (128, 128))
    same = (wide == wide.T) & (i0 < i1)
    rank = jnp.sum(jnp.where(same, 1.0, 0.0), axis=0, keepdims=True).astype(I32)
    d = dest[0:1, :]
    z = lax.shift_right_logical(d, 3)
    p = lax.bitwise_and(z, 3) * 8 + lax.bitwise_and(d, 7)
    slot = lax.shift_right_logical(z, 2) * 2 + rank
    tgt[...] = jnp.broadcast_to(p * 24 + slot, (8, 128))
    column = jnp.broadcast_to((p * 8 + slot).astype(F32), (128, 128)).T.astype(I32)
    for half in range(2):
        found = jnp.sum(jnp.where(column == i1 + 128 * half, i0, 0).astype(F32), axis=0, keepdims=True)
        inverse[8 * half : 8 * half + 8, :] = jnp.broadcast_to(found, (8, 128)).astype(I32)


def split3(t):
    a = t.astype(BF16).astype(F32)
    r = t - a
    b = r.astype(BF16).astype(F32)
    return a, b, r - b


def expand(chunk, out, base):
    row = lax.broadcasted_iota(I32, (8, 128), 0)
    nothing = jnp.zeros((16, 128), F32)

    def tile(t, _):
        v = chunk[pl.ds(t, 7, stride=8), :]
        m0, m1, m2 = v[0:1], v[1:2], v[2:3]
        q = -0.25 * (m0 * m0 + m1 * m1 + m2 * m2)
        full = jnp.concatenate([v, jnp.ones((1, 128), F32)], axis=0)
        dist = jnp.where((row < 3) | (row == 7), full, jnp.where(row == 6, q, 0.0))
        clear = jnp.where((row >= 3) & (row <= 6), full, 0.0)
        rows = []
        for side in (dist, clear):
            a, b, e = split3(side)
            rows += [a, a, b, a, e, b, nothing]
        out[base + t] = jnp.concatenate(rows, axis=0).T.astype(BF16)
        return 0

    lax.fori_loop(0, 8, tile, 0, unroll=4)


def exchange_kernel(
    dest_h, node_h, seg_h, conn_h, pseg_h, pslot_h,
    n_out, g_out, tgt, ready,
    dest, node, seg_nodes, conn, pseg, pslot, geo, s, xb, inv_v, inv, ins, ys, yr, zs, zr, ws, wr,
):
    g, z = lax.axis_index("grp"), lax.axis_index("dom_0")
    y, c = lax.axis_index("dom_1"), lax.axis_index("dom_2")
    loads = []
    for i, (src, dst) in enumerate(
        ((conn_h, conn), (seg_h, seg_nodes), (pseg_h, pseg), (pslot_h, pslot), (dest_h, dest), (node_h, node))
    ):
        load = pltpu.make_async_copy(src, dst, ins.at[i])
        load.start()
        loads.append(load)

    def zat(k):
        return (z + k + NZ) % NZ

    quad = z % 4
    other = (quad, z - quad + g, y, c)
    diagonal = quad == g
    peers = [((g + a) % NX, z, (y + b) % NY, (c + e) % NC) for a, b, e in TURNS]
    for e in sorted({d - p for d, p in enumerate(PARENT, 1)}):
        peers += [(g, zat(e), y, c), (g, zat(-e), y, c)]
    barrier = pltpu.get_barrier_semaphore()
    for peer in peers:
        pl.semaphore_signal(barrier, inc=1, device_id=peer, device_id_type=MESH)

    @pl.when(jnp.logical_not(diagonal))
    def _():
        pl.semaphore_signal(barrier, inc=1, device_id=other, device_id_type=MESH)

    for load in loads[:4]:
        load.wait()
    geometry(seg_nodes, conn, pseg, pslot, geo)
    pl.semaphore_wait(barrier, len(peers) + jnp.where(diagonal, 0, 1))
    me = g * 8 + y * 2 + c

    def number(sign, d):
        return (d if sign > 0 else 8 + d) - 1

    most = {1: 8, -1: 7}

    def children(p, sign):
        mine = [d for d in range(1, most[sign] + 1) if PARENT[d - 1] == p]
        return sorted(mine, key=lambda d: (d not in PARENT, -d))

    used = pl.ds(0, USED)

    def forward_z(sign, p, src):
        for d in children(p, sign):
            k = number(sign, d)
            start(src, g_out.at[zat(-sign * p), used], zs.at[k], zr.at[k], (g, zat(sign * (d - p)), y, c))

    def arrive_z(sign, d):
        k = number(sign, d)
        slot = g_out.at[zat(-sign * d), used]
        landed(slot, zs.at[k], zr.at[k], (g, zat(-sign * (d - PARENT[d - 1])), y, c))
        forward_z(sign, d, slot)
        expand(g_out.at[zat(-sign * d)], ready, zat(-sign * d) * 8)

    def node_send(k):
        a, b, e = TURNS[k]
        dev = ((g + a) % NX, z, (y + b) % NY, (c + e) % NC)
        start(s.at[dev[0] * 8 + dev[2] * 2 + dev[3]], n_out.at[me], ys.at[k], yr.at[k], dev)

    @pl.when(jnp.logical_not(diagonal))
    def _():
        start(geo.at[used], g_out.at[other[1], used], ws, wr, other)

    @pl.when(diagonal)
    def _():
        forward_z(1, 0, geo.at[used])
        forward_z(-1, 0, geo.at[used])
        g_out[z] = geo[...]

    loads[4].wait()
    slots_of(dest, inv_v, tgt)
    table = pltpu.make_async_copy(inv_v, inv, ins.at[6])
    table.start()
    loads[5].wait()

    def turn(j, _):
        at = pl.multiple_of(8 * j, 8)
        for i in range(3):
            x = node[pl.ds(i * 128 + at, 8), :]
            xb[pl.ds(at, 8), i, :] = x * root
            xb[pl.ds(at, 8), i + 3, :] = x + time_step * node[pl.ds((i + 3) * 128 + at, 8), :]
        return 0

    lax.fori_loop(0, 16, turn, 0, unroll=2)
    table.wait()

    def place(p, _):
        for k in range(8):
            block = xb[lax.bitwise_and(inv[8 * (p // 16), (p % 16) * 8 + k], 127)]
            s[p, pl.ds(k, 6, stride=8), :] = block[0:6]
        return 0

    lax.fori_loop(0, 32, place, 0, unroll=2)
    n_out[me] = s[me]
    first = 31
    for k in range(first):
        node_send(k)

    @pl.when(jnp.logical_not(diagonal))
    def _():
        landed(g_out.at[z, used], ws, wr, other)
        forward_z(1, 0, g_out.at[z, used])
        forward_z(-1, 0, g_out.at[z, used])

    for k in range(first, len(TURNS)):
        node_send(k)

    expand(g_out.at[z], ready, z * 8)
    inner = sorted(set(PARENT) - {0}, key=lambda d: (PARENT[d - 1], -d))
    for d in inner + [d for d in range(1, 9) if d not in inner]:
        for sign in (1, -1):
            if d <= most[sign]:
                arrive_z(sign, d)
    for k, (a, b, e) in enumerate(TURNS):
        dev = ((g - a + NX) % NX, z, (y - b + NY) % NY, (c + e) % NC)
        landed(n_out.at[dev[0] * 8 + dev[2] * 2 + dev[3]], ys.at[k], yr.at[k], dev)

    def left(src, ss, rs, dev):
        pltpu.make_async_remote_copy(
            src_ref=src, dst_ref=src, send_sem=ss, recv_sem=rs, device_id=dev, device_id_type=MESH
        ).wait_send()

    for k, (a, b, e) in enumerate(TURNS):
        dev = ((g + a) % NX, z, (y + b) % NY, (c + e) % NC)
        left(s.at[dev[0] * 8 + dev[2] * 2 + dev[3]], ys.at[k], yr.at[k], dev)
    for sign in (1, -1):
        for d in range(1, most[sign] + 1):
            k = number(sign, d)
            p = PARENT[d - 1]
            left(g_out.at[zat(-sign * p), used], zs.at[k], zr.at[k], (g, zat(sign * (d - p)), y, c))

    @pl.when(jnp.logical_not(diagonal))
    def _():
        left(geo.at[used], ws, wr, other)


def force_kernel(n_in, g_in, ready, f_out, lists_v, lists, sem):
    z = lax.axis_index("dom_0")
    seg = g_in[pl.ds(56, 16, stride=64), :]
    slot = g_in[pl.ds(57, 16, stride=64), :].astype(I32)
    lane = lax.broadcasted_iota(I32, (16, 128), 1)
    sub = lax.broadcasted_iota(I32, (16, 128), 0)
    hit = lax.shift_right_logical(slot, 4) == z
    mask = jnp.where(hit, 1.0, 0.0).astype(F32)
    low4 = lax.bitwise_and(slot, 15)
    code_a = seg + (sub * 8).astype(F32)
    who = lax.shift_right_logical(lane, 5) * 8 + lax.shift_right_logical(low4, 1)
    spot8 = lax.shift_right_logical(sub, 2) * 2 + lax.bitwise_and(low4, 1)
    code_b = (who * 8 + spot8).astype(F32)
    i0 = lax.broadcasted_iota(I32, (128, 128), 0)
    i1 = lax.broadcasted_iota(I32, (128, 128), 1)
    before = jnp.where(i0 < i1, 1.0, 0.0).astype(F32)
    inner = jnp.dot(mask, before, preferred_element_type=F32)
    total = jnp.dot(mask, jnp.ones((128, 128), F32), preferred_element_type=F32)
    j0 = lax.broadcasted_iota(I32, (16, 16), 0)
    j1 = lax.broadcasted_iota(I32, (16, 16), 1)
    above = jnp.dot(jnp.where(j1 < j0, 1.0, 0.0).astype(F32), total, preferred_element_type=F32)
    pos = (inner + above).astype(I32)
    high = jnp.where(hit, lax.shift_right_logical(pos, 7), -1)
    low = lax.bitwise_and(pos, 127)
    packed = jnp.zeros((32, 128), F32)
    for i in range(16):
        at = high[i : i + 1] == sub
        left = jnp.concatenate(
            [jnp.where(at, code_a[i : i + 1], 0.0), jnp.where(at, code_b[i : i + 1], 0.0)], axis=0
        )
        spot = jnp.where(low[i : i + 1] == i0, 1.0, 0.0).astype(F32)
        packed = packed + lax.dot_general(left, spot, (((1,), (1,)), ((), ())), preferred_element_type=F32)
    count = (total[15:16] + above[15:16]).astype(I32)
    code = packed[16:32].astype(I32)
    who = lax.shift_right_logical(code, 3)
    spot8 = lax.bitwise_and(code, 7)
    tile = packed[0:16].astype(I32)
    lists_v[0:16, :] = tile
    lists_v[16:32, :] = who * 48 + spot8
    lists_v[32:48, :] = jnp.where(sub * 128 + lane < count, who * 24 + spot8, 32 * 24)
    lists_v[48:56, :] = jnp.broadcast_to(count, (8, 128))
    copy = pltpu.make_async_copy(lists_v, lists, sem)
    copy.start()
    f_out[...] = jnp.zeros_like(f_out)
    copy.wait()

    ones = jnp.ones((8, 128), F32)
    blank = jnp.zeros((48, 128), BF16)
    gap = jnp.zeros((16, 256), BF16)

    def node_side(at):
        t = n_in[pl.ds(at, 6, stride=8), :]
        x0, x1, x2 = t[0:1], t[1:2], t[2:3]
        q = -(x0 * x0 + x1 * x1 + x2 * x2)
        full = jnp.concatenate([t, ones[0:1], q], axis=0)
        a, b, e = split3(full)
        side = jnp.concatenate([a, b, a, e, a, b], axis=0).astype(BF16)
        return jnp.concatenate(
            [
                jnp.concatenate([side, blank], axis=1),
                gap,
                jnp.concatenate([blank, side], axis=1),
                gap,
            ],
            axis=0,
        )

    def build(p):
        out = []
        left = []
        nothing = jnp.zeros((8, 128), F32)
        for i in range(2):
            q = p + i
            hi, lo = lax.shift_right_logical(q, 7), lax.bitwise_and(q, 127)
            tile = lists[hi, lo]
            t = g_in[pl.ds(lax.shift_right_logical(tile, 3) * 64 + lax.bitwise_and(tile, 7), 7, stride=8), :]
            t = jnp.concatenate([t, jnp.zeros((1, 128), F32)], axis=0)
            a = t.astype(BF16).astype(F32)
            left += [jnp.concatenate([a, a], axis=1), jnp.concatenate([t - a, nothing], axis=1)]
            out.append((ready[tile], node_side(lists[16 + hi, lo]), lists[32 + hi, lo]))
        return out, jnp.concatenate(left, axis=0).astype(BF16)

    def pressure(ew):
        press = jnp.exp2(ew[:, 0:128]) * jnp.maximum(ew[:, 128:256], 0.0)
        hi = press.astype(BF16)
        return hi, (press - hi.astype(F32)).astype(BF16)

    def run(size):
        def batch(p):
            made = [build(p + j) for j in range(0, size, 2)]
            ew = [
                [jnp.dot(tile, rhs, preferred_element_type=F32) for tile, rhs, _ in pairs] for pairs, _ in made
            ]
            ps = []
            for two in ew:
                (ha, la), (hb, lb) = pressure(two[0]), pressure(two[1])
                ps.append(
                    jnp.concatenate(
                        [jnp.concatenate([ha, hb], axis=1), jnp.concatenate([la, lb], axis=1)], axis=0
                    )
                )
            fs = [jnp.dot(m[1], q, preferred_element_type=F32) for m, q in zip(made, ps)]
            for (pairs, _), f in zip(made, fs):
                fa = -2.0 * (f[0:8, 0:128] + f[8:16, 0:128])
                fb = -2.0 * (f[16:24, 128:256] + f[24:32, 128:256])
                for at, v in ((pairs[0][2], fa[3:6]), (pairs[1][2], fb[3:6])):
                    here = pl.ds(at, 3, stride=8)
                    f_out[here, :] = f_out[here, :] + v

        return batch

    count = lists[48, 0]
    done = 0
    for size in SIZES:
        last = size == SIZES[-1]
        turns = (count - done + (size - 1 if last else 0)) // size
        body = run(size)

        def step(i, _, body=body, size=size, done=done):
            body(done + i * size)
            return 0

        lax.fori_loop(0, turns, step, 0)
        done = done + turns * size


def return_kernel(f, r_out, ys, yr):
    g, z = lax.axis_index("grp"), lax.axis_index("dom_0")
    y, c = lax.axis_index("dom_1"), lax.axis_index("dom_2")
    barrier = pltpu.get_barrier_semaphore()
    for a, b, e in TURNS:
        pl.semaphore_signal(
            barrier, inc=1, device_id=((g + a) % NX, z, (y + b) % NY, (c + e) % NC), device_id_type=MESH
        )
    pl.semaphore_wait(barrier, len(TURNS))
    me = g * 8 + y * 2 + c
    sends = []
    for k, (a, b, e) in enumerate(TURNS):
        dev = ((g + a) % NX, z, (y + b) % NY, (c + e) % NC)
        sends.append(start(f.at[dev[0] * 8 + dev[2] * 2 + dev[3]], r_out.at[me], ys.at[k], yr.at[k], dev))
    r_out[me] = f[me]
    for k, (a, b, e) in enumerate(TURNS):
        dev = ((g - a + NX) % NX, z, (y - b + NY) % NY, (c + e) % NC)
        landed(r_out.at[dev[0] * 8 + dev[2] * 2 + dev[3]], ys.at[k], yr.at[k], dev)
    for copy in sends:
        copy.wait_send()


def order_kernel(tgt, r_in, out):
    def one(i, _):
        out[pl.ds(i, 3, stride=128), :] = r_in[pl.ds(tgt[0, i], 3, stride=8), :]
        return 0

    lax.fori_loop(0, 128, one, 0, unroll=8)


def vmem():
    return pl.BlockSpec(memory_space=pltpu.VMEM)


def smem():
    return pl.BlockSpec(memory_space=pltpu.SMEM)


def shape(*dims, kind=F32):
    return jax.ShapeDtypeStruct(dims, kind)


def meet(node_state, node_dest, seg_nodes, seg_conn, pair_seg, pair_slot):
    dma = pltpu.SemaphoreType.DMA
    many = len(TURNS)
    nodes = jnp.transpose(node_state, (1, 0, 2)).reshape(768, 128)
    arrays = (node_dest.reshape(1, 128), nodes, seg_nodes, seg_conn, pair_seg, pair_slot)
    return pl.pallas_call(
        exchange_kernel,
        name="exchange",
        out_shape=(
            shape(32, 48, 128),
            shape(NZ, 64, 128),
            shape(8, 128, kind=I32),
            shape(NZ * 8, 128, 128, kind=BF16),
        ),
        in_specs=[pl.BlockSpec(memory_space=pltpu.HBM)] * 6,
        out_specs=(vmem(), vmem(), vmem(), vmem()),
        scratch_shapes=[
            pltpu.VMEM((1, 128), I32),
            pltpu.VMEM((768, 128), F32),
            pltpu.VMEM((6, 512), F32),
            pltpu.VMEM((3, 1024), I32),
            pltpu.VMEM((1, 4, 32), I32),
            pltpu.VMEM((1, 4, 32), I32),
            pltpu.VMEM((64, 128), F32),
            pltpu.VMEM((32, 48, 128), F32),
            pltpu.VMEM((128, 8, 128), F32),
            pltpu.VMEM((16, 128), I32),
            pltpu.SMEM((16, 128), I32),
            dma((7,)),
            dma((many,)),
            dma((many,)),
            dma((15,)),
            dma((15,)),
            dma,
            dma,
        ],
        compiler_params=pltpu.CompilerParams(collective_id=0, has_side_effects=True, vmem_limit_bytes=ROOM),
    )(*(pltpu.with_memory_space_constraint(v, pltpu.HBM) for v in arrays))


def give_back(forces):
    dma = pltpu.SemaphoreType.DMA
    many = len(TURNS)
    return pl.pallas_call(
        return_kernel,
        name="giveback",
        out_shape=shape(32, 24, 128),
        in_specs=[vmem()],
        out_specs=vmem(),
        scratch_shapes=[dma((many,)), dma((many,))],
        compiler_params=pltpu.CompilerParams(collective_id=1, has_side_effects=True, vmem_limit_bytes=ROOM),
    )(forces.reshape(33, 24, 128))


def shards(node_state, node_dest, seg_nodes, seg_conn, pair_seg, pair_slot):
    dma = pltpu.SemaphoreType.DMA
    many = len(TURNS)
    met, geos, tgt, ready = meet(node_state, node_dest, seg_nodes, seg_conn, pair_seg, pair_slot)
    forces = pl.pallas_call(
        force_kernel,
        name="forces",
        out_shape=shape(33 * 24, 128),
        in_specs=[vmem()] * 3,
        out_specs=vmem(),
        scratch_shapes=[pltpu.VMEM((56, 128), I32), pltpu.SMEM((56, 128), I32), dma],
        compiler_params=pltpu.CompilerParams(vmem_limit_bytes=ROOM),
    )(met.reshape(32 * 48, 128), geos.reshape(NZ * 64, 128), ready)
    back = give_back(forces)
    rows = pl.pallas_call(
        order_kernel,
        name="order",
        out_shape=shape(384, 128),
        in_specs=[smem(), vmem()],
        out_specs=vmem(),
        compiler_params=pltpu.CompilerParams(vmem_limit_bytes=ROOM),
    )(tgt, back.reshape(32 * 24, 128))
    return jnp.transpose(rows.reshape(3, 128, 128), (1, 0, 2))


def solution(mesh):
    split = Mesh(mesh.devices.reshape(NX, NZ, NY, NC), AXES)
    placed = (
        P(AXES, None, None),
        P(AXES),
        P(None, AXES),
        P(None, AXES),
        P(AXES, None, None),
        P(AXES, None, None),
    )
    return jax.shard_map(
        shards, mesh=split, in_specs=placed, out_specs=P(AXES, None, None), check_vma=False
    )
```

```python
import math

import jax
import jax.numpy as jnp
from jax import lax
from jax.experimental import pallas as pl
from jax.experimental.pallas import tpu as pltpu
from jax.sharding import Mesh
from jax.sharding import PartitionSpec as P

AXES = ("grp", "dom_0", "dom_1", "dom_2")
NX, NZ, NY, NC = 4, 16, 4, 2
MESH = pl.DeviceIdType.MESH
PARENT = (0, 1, 0, 3, 4, 3, 6, 6)
ORDER = (1, 3, 2, 4, 6, 5, 7, 8)
USED = 58
SIZES = (64, 32, 16, 8)
ROOM = 16 << 20
F32, BF16, I32 = jnp.float32, jnp.bfloat16, jnp.int32

time_step = 0.5
stiffness = 0.5
radius_sq = 0.5
root = math.sqrt(math.log2(math.e) / radius_sq)

TURNS = sorted(
    ((a, b, c) for a in range(NX) for b in range(NY) for c in range(NC) if a or b or c),
    key=lambda t: -min(t[0], NX - t[0]) - min(t[1], NY - t[1]),
)


def start(src, dst, ss, rs, dev):
    copy = pltpu.make_async_remote_copy(
        src_ref=src, dst_ref=dst, send_sem=ss, recv_sem=rs, device_id=dev, device_id_type=MESH
    )
    copy.start()
    return copy


def landed(dst, ss, rs, dev):
    pltpu.make_async_remote_copy(
        src_ref=dst, dst_ref=dst, send_sem=ss, recv_sem=rs, device_id=dev, device_id_type=MESH
    ).wait_recv()


def geometry(seg_nodes, conn, pseg, pslot, geo):
    corners = []
    for k in range(3):
        idx = jnp.concatenate([conn[k : k + 1, b * 128 : (b + 1) * 128] for b in range(8)], axis=0)
        hi = lax.shift_right_logical(idx, 7)
        lo = lax.bitwise_and(idx, 127)
        comps = []
        for i in range(6):
            got = None
            for q in range(4):
                table = jnp.broadcast_to(seg_nodes[i : i + 1, q * 128 : (q + 1) * 128], (8, 128))
                part = jnp.take_along_axis(table, lo, axis=1)
                got = part if got is None else jnp.where(hi == q, part, got)
            comps.append(got)
        corners.append(comps)
    a, b, c = corners
    e1 = [b[i] - a[i] for i in range(3)]
    e2 = [c[i] - a[i] for i in range(3)]
    n = [0.5 * (e1[(i + 1) % 3] * e2[(i + 2) % 3] - e1[(i + 2) % 3] * e2[(i + 1) % 3]) for i in range(3)]
    m = [(a[i] + b[i] + c[i]) / 3.0 for i in range(3)]
    u = [(a[i + 3] + b[i + 3] + c[i + 3]) / 3.0 for i in range(3)]
    off = sum(n[i] * (m[i] + time_step * u[i]) for i in range(3))
    values = [2.0 * root * v for v in m] + [-stiffness * v for v in n] + [stiffness * off]
    for i, v in enumerate(values):
        geo[8 * i : 8 * i + 8, :] = v
    tables = []
    for tab in (pseg, pslot):
        t = jnp.concatenate([tab[0].astype(F32), jnp.zeros((4, 96), F32)], axis=1)
        rows = [pltpu.roll(jnp.broadcast_to(t[r : r + 1], (8, 128)), 32 * r, 1) for r in range(4)]
        tables.append(rows[0] + rows[1] + rows[2] + rows[3])
    for i, t in enumerate(tables):
        geo[56 + i : 57 + i, :] = t[0:1]


def slots_of(dest, inverse, tgt):
    i0 = lax.broadcasted_iota(I32, (128, 128), 0)
    i1 = lax.broadcasted_iota(I32, (128, 128), 1)
    wide = jnp.broadcast_to(dest[0:1, :].astype(F32), (128, 128))
    same = (wide == wide.T) & (i0 < i1)
    rank = jnp.sum(jnp.where(same, 1.0, 0.0), axis=0, keepdims=True).astype(I32)
    d = dest[0:1, :]
    z = lax.shift_right_logical(d, 3)
    p = lax.bitwise_and(z, 3) * 8 + lax.bitwise_and(d, 7)
    slot = lax.shift_right_logical(z, 2) * 2 + rank
    tgt[...] = jnp.broadcast_to(p * 24 + slot, (8, 128))
    column = jnp.broadcast_to((p * 8 + slot).astype(F32), (128, 128)).T.astype(I32)
    for half in range(2):
        found = jnp.sum(jnp.where(column == i1 + 128 * half, i0, 0).astype(F32), axis=0, keepdims=True)
        inverse[8 * half : 8 * half + 8, :] = jnp.broadcast_to(found, (8, 128)).astype(I32)


def split3(t):
    a = t.astype(BF16).astype(F32)
    r = t - a
    b = r.astype(BF16).astype(F32)
    return a, b, r - b


def expand(chunk, out, base):
    row = lax.broadcasted_iota(I32, (8, 128), 0)
    nothing = jnp.zeros((16, 128), F32)

    def tile(t, _):
        v = chunk[pl.ds(t, 7, stride=8), :]
        m0, m1, m2 = v[0:1], v[1:2], v[2:3]
        q = -0.25 * (m0 * m0 + m1 * m1 + m2 * m2)
        full = jnp.concatenate([v, jnp.ones((1, 128), F32)], axis=0)
        dist = jnp.where((row < 3) | (row == 7), full, jnp.where(row == 6, q, 0.0))
        clear = jnp.where((row >= 3) & (row <= 6), full, 0.0)
        rows = []
        for side in (dist, clear):
            a, b, e = split3(side)
            rows += [a, a, b, a, e, b, nothing]
        out[base + t] = jnp.concatenate(rows, axis=0).T.astype(BF16)
        return 0

    lax.fori_loop(0, 8, tile, 0, unroll=8)


def exchange_kernel(
    dest_h, node_h, seg_h, conn_h, pseg_h, pslot_h,
    n_out, g_out, tgt, ready,
    dest, node, seg_nodes, conn, pseg, pslot, geo, s, xb, inv_v, inv, ins, ys, yr, zs, zr, ws, wr,
):
    g, z = lax.axis_index("grp"), lax.axis_index("dom_0")
    y, c = lax.axis_index("dom_1"), lax.axis_index("dom_2")
    loads = []
    for i, (src, dst) in enumerate(
        ((conn_h, conn), (seg_h, seg_nodes), (pseg_h, pseg), (pslot_h, pslot), (dest_h, dest), (node_h, node))
    ):
        load = pltpu.make_async_copy(src, dst, ins.at[i])
        load.start()
        loads.append(load)

    def zat(k):
        return (z + k + NZ) % NZ

    quad = z % 4
    other = (quad, z - quad + g, y, c)
    diagonal = quad == g
    peers = [((g + a) % NX, z, (y + b) % NY, (c + e) % NC) for a, b, e in TURNS]
    for e in sorted({d - p for d, p in enumerate(PARENT, 1)}):
        peers += [(g, zat(e), y, c), (g, zat(-e), y, c)]
    barrier = pltpu.get_barrier_semaphore()
    for peer in peers:
        pl.semaphore_signal(barrier, inc=1, device_id=peer, device_id_type=MESH)

    @pl.when(jnp.logical_not(diagonal))
    def _():
        pl.semaphore_signal(barrier, inc=1, device_id=other, device_id_type=MESH)

    for load in loads[:4]:
        load.wait()
    geometry(seg_nodes, conn, pseg, pslot, geo)
    pl.semaphore_wait(barrier, len(peers) + jnp.where(diagonal, 0, 1))
    me = g * 8 + y * 2 + c

    def number(sign, d):
        return (d if sign > 0 else 8 + d) - 1

    most = {1: 8, -1: 7}

    def children(p, sign):
        mine = [d for d in range(1, most[sign] + 1) if PARENT[d - 1] == p]
        return sorted(mine, key=lambda d: (d not in PARENT, -d))

    used = pl.ds(0, USED)

    def forward_z(sign, p, src):
        for d in children(p, sign):
            k = number(sign, d)
            start(src, g_out.at[zat(-sign * p), used], zs.at[k], zr.at[k], (g, zat(sign * (d - p)), y, c))

    def arrive_z(sign, d):
        k = number(sign, d)
        slot = g_out.at[zat(-sign * d), used]
        landed(slot, zs.at[k], zr.at[k], (g, zat(-sign * (d - PARENT[d - 1])), y, c))
        forward_z(sign, d, slot)
        expand(g_out.at[zat(-sign * d)], ready, zat(-sign * d) * 8)

    def node_send(k):
        a, b, e = TURNS[k]
        dev = ((g + a) % NX, z, (y + b) % NY, (c + e) % NC)
        start(s.at[dev[0] * 8 + dev[2] * 2 + dev[3]], n_out.at[me], ys.at[k], yr.at[k], dev)

    @pl.when(jnp.logical_not(diagonal))
    def _():
        start(geo.at[used], g_out.at[other[1], used], ws, wr, other)

    @pl.when(diagonal)
    def _():
        forward_z(1, 0, geo.at[used])
        forward_z(-1, 0, geo.at[used])
        g_out[z] = geo[...]

    loads[4].wait()
    slots_of(dest, inv_v, tgt)
    table = pltpu.make_async_copy(inv_v, inv, ins.at[6])
    table.start()
    loads[5].wait()

    def turn(j, _):
        at = pl.multiple_of(8 * j, 8)
        for i in range(3):
            x = node[pl.ds(i * 128 + at, 8), :]
            xb[pl.ds(at, 8), i, :] = x * root
            xb[pl.ds(at, 8), i + 3, :] = x + time_step * node[pl.ds((i + 3) * 128 + at, 8), :]
        return 0

    lax.fori_loop(0, 16, turn, 0, unroll=2)
    table.wait()

    def place(p, _):
        for k in range(8):
            block = xb[lax.bitwise_and(inv[8 * (p // 16), (p % 16) * 8 + k], 127)]
            s[p, pl.ds(k, 6, stride=8), :] = block[0:6]
        return 0

    lax.fori_loop(0, 32, place, 0, unroll=2)
    n_out[me] = s[me]
    first = 31
    for k in range(first):
        node_send(k)

    @pl.when(jnp.logical_not(diagonal))
    def _():
        landed(g_out.at[z, used], ws, wr, other)
        forward_z(1, 0, g_out.at[z, used])
        forward_z(-1, 0, g_out.at[z, used])

    for k in range(first, len(TURNS)):
        node_send(k)

    expand(g_out.at[z], ready, z * 8)
    for d in ORDER:
        for sign in (1, -1):
            if d <= most[sign]:
                arrive_z(sign, d)
    for k, (a, b, e) in enumerate(TURNS):
        dev = ((g - a + NX) % NX, z, (y - b + NY) % NY, (c + e) % NC)
        landed(n_out.at[dev[0] * 8 + dev[2] * 2 + dev[3]], ys.at[k], yr.at[k], dev)

    def left(src, ss, rs, dev):
        pltpu.make_async_remote_copy(
            src_ref=src, dst_ref=src, send_sem=ss, recv_sem=rs, device_id=dev, device_id_type=MESH
        ).wait_send()

    for k, (a, b, e) in enumerate(TURNS):
        dev = ((g + a) % NX, z, (y + b) % NY, (c + e) % NC)
        left(s.at[dev[0] * 8 + dev[2] * 2 + dev[3]], ys.at[k], yr.at[k], dev)
    for sign in (1, -1):
        for d in range(1, most[sign] + 1):
            k = number(sign, d)
            p = PARENT[d - 1]
            left(g_out.at[zat(-sign * p), used], zs.at[k], zr.at[k], (g, zat(sign * (d - p)), y, c))

    @pl.when(jnp.logical_not(diagonal))
    def _():
        left(geo.at[used], ws, wr, other)


def force_kernel(n_in, g_in, ready, f_out, lists_v, lists, sem):
    z = lax.axis_index("dom_0")
    seg = g_in[pl.ds(56, 16, stride=64), :]
    slot = g_in[pl.ds(57, 16, stride=64), :].astype(I32)
    lane = lax.broadcasted_iota(I32, (16, 128), 1)
    sub = lax.broadcasted_iota(I32, (16, 128), 0)
    hit = lax.shift_right_logical(slot, 4) == z
    mask = jnp.where(hit, 1.0, 0.0).astype(F32)
    low4 = lax.bitwise_and(slot, 15)
    code_a = seg + (sub * 8).astype(F32)
    who = lax.shift_right_logical(lane, 5) * 8 + lax.shift_right_logical(low4, 1)
    spot8 = lax.shift_right_logical(sub, 2) * 2 + lax.bitwise_and(low4, 1)
    code_b = (who * 8 + spot8).astype(F32)
    i0 = lax.broadcasted_iota(I32, (128, 128), 0)
    i1 = lax.broadcasted_iota(I32, (128, 128), 1)
    before = jnp.where(i0 < i1, 1.0, 0.0).astype(F32)
    inner = jnp.dot(mask, before, preferred_element_type=F32)
    total = jnp.dot(mask, jnp.ones((128, 128), F32), preferred_element_type=F32)
    j0 = lax.broadcasted_iota(I32, (16, 16), 0)
    j1 = lax.broadcasted_iota(I32, (16, 16), 1)
    above = jnp.dot(jnp.where(j1 < j0, 1.0, 0.0).astype(F32), total, preferred_element_type=F32)
    pos = (inner + above).astype(I32)
    high = jnp.where(hit, lax.shift_right_logical(pos, 7), -1)
    low = lax.bitwise_and(pos, 127)
    packed = jnp.zeros((32, 128), F32)
    for i in range(16):
        at = high[i : i + 1] == sub
        left = jnp.concatenate(
            [jnp.where(at, code_a[i : i + 1], 0.0), jnp.where(at, code_b[i : i + 1], 0.0)], axis=0
        )
        spot = jnp.where(low[i : i + 1] == i0, 1.0, 0.0).astype(F32)
        packed = packed + lax.dot_general(left, spot, (((1,), (1,)), ((), ())), preferred_element_type=F32)
    count = (total[15:16] + above[15:16]).astype(I32)
    code = packed[16:32].astype(I32)
    who = lax.shift_right_logical(code, 3)
    spot8 = lax.bitwise_and(code, 7)
    tile = packed[0:16].astype(I32)
    lists_v[0:16, :] = tile
    lists_v[16:32, :] = who * 48 + spot8
    lists_v[32:48, :] = jnp.where(sub * 128 + lane < count, who * 24 + spot8, 32 * 24)
    lists_v[48:56, :] = jnp.broadcast_to(count, (8, 128))
    copy = pltpu.make_async_copy(lists_v, lists, sem)
    copy.start()
    f_out[...] = jnp.zeros_like(f_out)
    copy.wait()

    ones = jnp.ones((8, 128), F32)
    blank = jnp.zeros((48, 128), BF16)
    gap = jnp.zeros((16, 256), BF16)

    def node_side(at):
        t = n_in[pl.ds(at, 6, stride=8), :]
        x0, x1, x2 = t[0:1], t[1:2], t[2:3]
        q = -(x0 * x0 + x1 * x1 + x2 * x2)
        full = jnp.concatenate([t, ones[0:1], q], axis=0)
        a, b, e = split3(full)
        side = jnp.concatenate([a, b, a, e, a, b], axis=0).astype(BF16)
        return jnp.concatenate(
            [
                jnp.concatenate([side, blank], axis=1),
                gap,
                jnp.concatenate([blank, side], axis=1),
                gap,
            ],
            axis=0,
        )

    def build(p):
        out = []
        left = []
        nothing = jnp.zeros((8, 128), F32)
        for i in range(2):
            q = p + i
            hi, lo = lax.shift_right_logical(q, 7), lax.bitwise_and(q, 127)
            tile = lists[hi, lo]
            t = g_in[pl.ds(lax.shift_right_logical(tile, 3) * 64 + lax.bitwise_and(tile, 7), 7, stride=8), :]
            t = jnp.concatenate([t, jnp.zeros((1, 128), F32)], axis=0)
            a = t.astype(BF16).astype(F32)
            left += [jnp.concatenate([a, a], axis=1), jnp.concatenate([t - a, nothing], axis=1)]
            out.append((ready[tile], node_side(lists[16 + hi, lo]), lists[32 + hi, lo]))
        return out, jnp.concatenate(left, axis=0).astype(BF16)

    def pressure(ew):
        press = jnp.exp2(ew[:, 0:128]) * jnp.maximum(ew[:, 128:256], 0.0)
        hi = press.astype(BF16)
        return hi, (press - hi.astype(F32)).astype(BF16)

    def run(size):
        def batch(p):
            made = [build(p + j) for j in range(0, size, 2)]
            ew = [
                [jnp.dot(tile, rhs, preferred_element_type=F32) for tile, rhs, _ in pairs] for pairs, _ in made
            ]
            ps = []
            for two in ew:
                (ha, la), (hb, lb) = pressure(two[0]), pressure(two[1])
                ps.append(
                    jnp.concatenate(
                        [jnp.concatenate([ha, hb], axis=1), jnp.concatenate([la, lb], axis=1)], axis=0
                    )
                )
            fs = [jnp.dot(m[1], q, preferred_element_type=F32) for m, q in zip(made, ps)]
            for (pairs, _), f in zip(made, fs):
                fa = -2.0 * (f[0:8, 0:128] + f[8:16, 0:128])
                fb = -2.0 * (f[16:24, 128:256] + f[24:32, 128:256])
                for at, v in ((pairs[0][2], fa[3:6]), (pairs[1][2], fb[3:6])):
                    here = pl.ds(at, 3, stride=8)
                    f_out[here, :] = f_out[here, :] + v

        return batch

    count = lists[48, 0]
    done = 0
    for size in SIZES:
        last = size == SIZES[-1]
        turns = (count - done + (size - 1 if last else 0)) // size
        body = run(size)

        def step(i, _, body=body, size=size, done=done):
            body(done + i * size)
            return 0

        lax.fori_loop(0, turns, step, 0)
        done = done + turns * size


def return_kernel(f, r_out, ys, yr):
    g, z = lax.axis_index("grp"), lax.axis_index("dom_0")
    y, c = lax.axis_index("dom_1"), lax.axis_index("dom_2")
    barrier = pltpu.get_barrier_semaphore()
    for a, b, e in TURNS:
        pl.semaphore_signal(
            barrier, inc=1, device_id=((g + a) % NX, z, (y + b) % NY, (c + e) % NC), device_id_type=MESH
        )
    pl.semaphore_wait(barrier, len(TURNS))
    me = g * 8 + y * 2 + c
    sends = []
    for k, (a, b, e) in enumerate(TURNS):
        dev = ((g + a) % NX, z, (y + b) % NY, (c + e) % NC)
        sends.append(start(f.at[dev[0] * 8 + dev[2] * 2 + dev[3]], r_out.at[me], ys.at[k], yr.at[k], dev))
    r_out[me] = f[me]
    for k, (a, b, e) in enumerate(TURNS):
        dev = ((g - a + NX) % NX, z, (y - b + NY) % NY, (c + e) % NC)
        landed(r_out.at[dev[0] * 8 + dev[2] * 2 + dev[3]], ys.at[k], yr.at[k], dev)
    for copy in sends:
        copy.wait_send()


def order_kernel(tgt, r_in, out):
    def one(i, _):
        out[pl.ds(i, 3, stride=128), :] = r_in[pl.ds(tgt[0, i], 3, stride=8), :]
        return 0

    lax.fori_loop(0, 128, one, 0, unroll=8)


def vmem():
    return pl.BlockSpec(memory_space=pltpu.VMEM)


def smem():
    return pl.BlockSpec(memory_space=pltpu.SMEM)


def shape(*dims, kind=F32):
    return jax.ShapeDtypeStruct(dims, kind)


def meet(node_state, node_dest, seg_nodes, seg_conn, pair_seg, pair_slot):
    dma = pltpu.SemaphoreType.DMA
    many = len(TURNS)
    nodes = jnp.transpose(node_state, (1, 0, 2)).reshape(768, 128)
    arrays = (node_dest.reshape(1, 128), nodes, seg_nodes, seg_conn, pair_seg, pair_slot)
    return pl.pallas_call(
        exchange_kernel,
        name="exchange",
        out_shape=(
            shape(32, 48, 128),
            shape(NZ, 64, 128),
            shape(8, 128, kind=I32),
            shape(NZ * 8, 128, 128, kind=BF16),
        ),
        in_specs=[pl.BlockSpec(memory_space=pltpu.HBM)] * 6,
        out_specs=(vmem(), vmem(), vmem(), vmem()),
        scratch_shapes=[
            pltpu.VMEM((1, 128), I32),
            pltpu.VMEM((768, 128), F32),
            pltpu.VMEM((6, 512), F32),
            pltpu.VMEM((3, 1024), I32),
            pltpu.VMEM((1, 4, 32), I32),
            pltpu.VMEM((1, 4, 32), I32),
            pltpu.VMEM((64, 128), F32),
            pltpu.VMEM((32, 48, 128), F32),
            pltpu.VMEM((128, 8, 128), F32),
            pltpu.VMEM((16, 128), I32),
            pltpu.SMEM((16, 128), I32),
            dma((7,)),
            dma((many,)),
            dma((many,)),
            dma((15,)),
            dma((15,)),
            dma,
            dma,
        ],
        compiler_params=pltpu.CompilerParams(collective_id=0, has_side_effects=True, vmem_limit_bytes=ROOM),
    )(*(pltpu.with_memory_space_constraint(v, pltpu.HBM) for v in arrays))


def give_back(forces):
    dma = pltpu.SemaphoreType.DMA
    many = len(TURNS)
    return pl.pallas_call(
        return_kernel,
        name="giveback",
        out_shape=shape(32, 24, 128),
        in_specs=[vmem()],
        out_specs=vmem(),
        scratch_shapes=[dma((many,)), dma((many,))],
        compiler_params=pltpu.CompilerParams(collective_id=1, has_side_effects=True, vmem_limit_bytes=ROOM),
    )(forces.reshape(33, 24, 128))


def shards(node_state, node_dest, seg_nodes, seg_conn, pair_seg, pair_slot):
    dma = pltpu.SemaphoreType.DMA
    many = len(TURNS)
    met, geos, tgt, ready = meet(node_state, node_dest, seg_nodes, seg_conn, pair_seg, pair_slot)
    forces = pl.pallas_call(
        force_kernel,
        name="forces",
        out_shape=shape(33 * 24, 128),
        in_specs=[vmem()] * 3,
        out_specs=vmem(),
        scratch_shapes=[pltpu.VMEM((56, 128), I32), pltpu.SMEM((56, 128), I32), dma],
        compiler_params=pltpu.CompilerParams(vmem_limit_bytes=ROOM),
    )(met.reshape(32 * 48, 128), geos.reshape(NZ * 64, 128), ready)
    back = give_back(forces)
    rows = pl.pallas_call(
        order_kernel,
        name="order",
        out_shape=shape(384, 128),
        in_specs=[smem(), vmem()],
        out_specs=vmem(),
        compiler_params=pltpu.CompilerParams(vmem_limit_bytes=ROOM),
    )(tgt, back.reshape(32 * 24, 128))
    return jnp.transpose(rows.reshape(3, 128, 128), (1, 0, 2))


def solution(mesh):
    split = Mesh(mesh.devices.reshape(NX, NZ, NY, NC), AXES)
    placed = (
        P(AXES, None, None),
        P(AXES),
        P(None, AXES),
        P(None, AXES),
        P(AXES, None, None),
        P(AXES, None, None),
    )
    return jax.shard_map(
        shards, mesh=split, in_specs=placed, out_specs=P(AXES, None, None), check_vma=False
    )
```

```python
import math

import jax
import jax.numpy as jnp
from jax import lax
from jax.experimental import pallas as pl
from jax.experimental.pallas import tpu as pltpu
from jax.sharding import Mesh
from jax.sharding import PartitionSpec as P

AXES = ("grp", "dom_0", "dom_1", "dom_2")
NX, NZ, NY, NC = 4, 16, 4, 2
MESH = pl.DeviceIdType.MESH
PARENT = (0, 1, 0, 3, 4, 3, 6, 6)
ORDER = (1, 3, 2, 4, 6, 5, 7, 8)
USED = 58
SIZES = (64, 32, 16, 8)
ROOM = 16 << 20
F32, BF16, I32 = jnp.float32, jnp.bfloat16, jnp.int32

time_step = 0.5
stiffness = 0.5
radius_sq = 0.5
root = math.sqrt(math.log2(math.e) / radius_sq)

TURNS = sorted(
    ((a, b, c) for a in range(NX) for b in range(NY) for c in range(NC) if a or b or c),
    key=lambda t: -min(t[0], NX - t[0]) - min(t[1], NY - t[1]),
)


def start(src, dst, ss, rs, dev):
    copy = pltpu.make_async_remote_copy(
        src_ref=src, dst_ref=dst, send_sem=ss, recv_sem=rs, device_id=dev, device_id_type=MESH
    )
    copy.start()
    return copy


def landed(dst, ss, rs, dev):
    pltpu.make_async_remote_copy(
        src_ref=dst, dst_ref=dst, send_sem=ss, recv_sem=rs, device_id=dev, device_id_type=MESH
    ).wait_recv()


def geometry(seg_nodes, conn, pseg, pslot, geo):
    corners = []
    for k in range(3):
        idx = jnp.concatenate([conn[k : k + 1, b * 128 : (b + 1) * 128] for b in range(8)], axis=0)
        hi = lax.shift_right_logical(idx, 7)
        lo = lax.bitwise_and(idx, 127)
        comps = []
        for i in range(6):
            got = None
            for q in range(4):
                table = jnp.broadcast_to(seg_nodes[i : i + 1, q * 128 : (q + 1) * 128], (8, 128))
                part = jnp.take_along_axis(table, lo, axis=1)
                got = part if got is None else jnp.where(hi == q, part, got)
            comps.append(got)
        corners.append(comps)
    a, b, c = corners
    e1 = [b[i] - a[i] for i in range(3)]
    e2 = [c[i] - a[i] for i in range(3)]
    n = [0.5 * (e1[(i + 1) % 3] * e2[(i + 2) % 3] - e1[(i + 2) % 3] * e2[(i + 1) % 3]) for i in range(3)]
    m = [(a[i] + b[i] + c[i]) / 3.0 for i in range(3)]
    u = [(a[i + 3] + b[i + 3] + c[i + 3]) / 3.0 for i in range(3)]
    off = sum(n[i] * (m[i] + time_step * u[i]) for i in range(3))
    values = [2.0 * root * v for v in m] + [-stiffness * v for v in n] + [stiffness * off]
    for i, v in enumerate(values):
        geo[8 * i : 8 * i + 8, :] = v
    tables = []
    for tab in (pseg, pslot):
        t = jnp.concatenate([tab[0].astype(F32), jnp.zeros((4, 96), F32)], axis=1)
        rows = [pltpu.roll(jnp.broadcast_to(t[r : r + 1], (8, 128)), 32 * r, 1) for r in range(4)]
        tables.append(rows[0] + rows[1] + rows[2] + rows[3])
    for i, t in enumerate(tables):
        geo[56 + i : 57 + i, :] = t[0:1]


def slots_of(dest, inverse, tgt):
    i0 = lax.broadcasted_iota(I32, (128, 128), 0)
    i1 = lax.broadcasted_iota(I32, (128, 128), 1)
    wide = jnp.broadcast_to(dest[0:1, :].astype(F32), (128, 128))
    same = (wide == wide.T) & (i0 < i1)
    rank = jnp.sum(jnp.where(same, 1.0, 0.0), axis=0, keepdims=True).astype(I32)
    d = dest[0:1, :]
    z = lax.shift_right_logical(d, 3)
    p = lax.bitwise_and(z, 3) * 8 + lax.bitwise_and(d, 7)
    slot = lax.shift_right_logical(z, 2) * 2 + rank
    tgt[...] = p * 24 + slot
    column = jnp.broadcast_to((p * 8 + slot).astype(F32), (128, 128)).T.astype(I32)
    for half in range(2):
        found = jnp.sum(jnp.where(column == i1 + 128 * half, i0, 0).astype(F32), axis=0, keepdims=True)
        inverse[8 * half : 8 * half + 8, :] = jnp.broadcast_to(found, (8, 128)).astype(I32)


def split3(t):
    a = t.astype(BF16).astype(F32)
    r = t - a
    b = r.astype(BF16).astype(F32)
    return a, b, r - b


def expand(chunk, out, base):
    row = lax.broadcasted_iota(I32, (8, 128), 0)
    nothing = jnp.zeros((16, 128), F32)

    def tile(t, _):
        v = chunk[pl.ds(t, 7, stride=8), :]
        m0, m1, m2 = v[0:1], v[1:2], v[2:3]
        q = -0.25 * (m0 * m0 + m1 * m1 + m2 * m2)
        full = jnp.concatenate([v, jnp.ones((1, 128), F32)], axis=0)
        dist = jnp.where((row < 3) | (row == 7), full, jnp.where(row == 6, q, 0.0))
        clear = jnp.where((row >= 3) & (row <= 6), full, 0.0)
        rows = []
        for side in (dist, clear):
            a, b, e = split3(side)
            rows += [a, a, b, a, e, b, nothing]
        out[base + t] = jnp.concatenate(rows, axis=0).T.astype(BF16)
        return 0

    lax.fori_loop(0, 8, tile, 0, unroll=8)


def exchange_kernel(
    dest_h, node_h, seg_h, conn_h, pseg_h, pslot_h,
    n_out, g_out, tgt, ready,
    dest, node, seg_nodes, conn, pseg, pslot, geo, s, xb, inv_v, inv, ins, ys, yr, zs, zr, ws, wr,
):
    g, z = lax.axis_index("grp"), lax.axis_index("dom_0")
    y, c = lax.axis_index("dom_1"), lax.axis_index("dom_2")
    loads = []
    for i, (src, dst) in enumerate(
        ((conn_h, conn), (seg_h, seg_nodes), (pseg_h, pseg), (pslot_h, pslot), (dest_h, dest), (node_h, node))
    ):
        load = pltpu.make_async_copy(src, dst, ins.at[i])
        load.start()
        loads.append(load)

    def zat(k):
        return (z + k + NZ) % NZ

    quad = z % 4
    other = (quad, z - quad + g, y, c)
    diagonal = quad == g
    peers = [((g + a) % NX, z, (y + b) % NY, (c + e) % NC) for a, b, e in TURNS]
    for e in sorted({d - p for d, p in enumerate(PARENT, 1)}):
        peers += [(g, zat(e), y, c), (g, zat(-e), y, c)]
    barrier = pltpu.get_barrier_semaphore()
    for peer in peers:
        pl.semaphore_signal(barrier, inc=1, device_id=peer, device_id_type=MESH)

    @pl.when(jnp.logical_not(diagonal))
    def _():
        pl.semaphore_signal(barrier, inc=1, device_id=other, device_id_type=MESH)

    for load in loads[:4]:
        load.wait()
    geometry(seg_nodes, conn, pseg, pslot, geo)
    pl.semaphore_wait(barrier, len(peers) + jnp.where(diagonal, 0, 1))
    me = g * 8 + y * 2 + c

    def number(sign, d):
        return (d if sign > 0 else 8 + d) - 1

    most = {1: 8, -1: 7}

    def children(p, sign):
        mine = [d for d in range(1, most[sign] + 1) if PARENT[d - 1] == p]
        return sorted(mine, key=lambda d: (d not in PARENT, -d))

    used = pl.ds(0, USED)

    def forward_z(sign, p, src):
        for d in children(p, sign):
            k = number(sign, d)
            start(src, g_out.at[zat(-sign * p), used], zs.at[k], zr.at[k], (g, zat(sign * (d - p)), y, c))

    def arrive_z(sign, d):
        k = number(sign, d)
        slot = g_out.at[zat(-sign * d), used]
        landed(slot, zs.at[k], zr.at[k], (g, zat(-sign * (d - PARENT[d - 1])), y, c))
        forward_z(sign, d, slot)
        expand(g_out.at[zat(-sign * d)], ready, zat(-sign * d) * 8)

    def node_send(k):
        a, b, e = TURNS[k]
        dev = ((g + a) % NX, z, (y + b) % NY, (c + e) % NC)
        start(s.at[dev[0] * 8 + dev[2] * 2 + dev[3]], n_out.at[me], ys.at[k], yr.at[k], dev)

    @pl.when(jnp.logical_not(diagonal))
    def _():
        start(geo.at[used], g_out.at[other[1], used], ws, wr, other)

    @pl.when(diagonal)
    def _():
        forward_z(1, 0, geo.at[used])
        forward_z(-1, 0, geo.at[used])
        g_out[z] = geo[...]

    loads[4].wait()
    slots_of(dest, inv_v, tgt)
    table = pltpu.make_async_copy(inv_v, inv, ins.at[6])
    table.start()
    loads[5].wait()

    def turn(j, _):
        at = pl.multiple_of(8 * j, 8)
        for i in range(3):
            x = node[pl.ds(i * 128 + at, 8), :]
            xb[pl.ds(at, 8), i, :] = x * root
            xb[pl.ds(at, 8), i + 3, :] = x + time_step * node[pl.ds((i + 3) * 128 + at, 8), :]
        return 0

    lax.fori_loop(0, 16, turn, 0, unroll=2)
    table.wait()

    def place(p, _):
        for k in range(8):
            block = xb[lax.bitwise_and(inv[8 * (p // 16), (p % 16) * 8 + k], 127)]
            s[p, pl.ds(k, 6, stride=8), :] = block[0:6]
        return 0

    lax.fori_loop(0, 32, place, 0, unroll=2)
    n_out[me] = s[me]
    first = 0
    for k in range(first):
        node_send(k)

    @pl.when(jnp.logical_not(diagonal))
    def _():
        landed(g_out.at[z, used], ws, wr, other)
        forward_z(1, 0, g_out.at[z, used])
        forward_z(-1, 0, g_out.at[z, used])

    for k in range(first, len(TURNS)):
        node_send(k)

    expand(g_out.at[z], ready, z * 8)
    for d in ORDER:
        for sign in (1, -1):
            if d <= most[sign]:
                arrive_z(sign, d)
    for k, (a, b, e) in enumerate(TURNS):
        dev = ((g - a + NX) % NX, z, (y - b + NY) % NY, (c + e) % NC)
        landed(n_out.at[dev[0] * 8 + dev[2] * 2 + dev[3]], ys.at[k], yr.at[k], dev)

    def left(src, ss, rs, dev):
        pltpu.make_async_remote_copy(
            src_ref=src, dst_ref=src, send_sem=ss, recv_sem=rs, device_id=dev, device_id_type=MESH
        ).wait_send()

    for k, (a, b, e) in enumerate(TURNS):
        dev = ((g + a) % NX, z, (y + b) % NY, (c + e) % NC)
        left(s.at[dev[0] * 8 + dev[2] * 2 + dev[3]], ys.at[k], yr.at[k], dev)
    for sign in (1, -1):
        for d in range(1, most[sign] + 1):
            k = number(sign, d)
            p = PARENT[d - 1]
            left(g_out.at[zat(-sign * p), used], zs.at[k], zr.at[k], (g, zat(sign * (d - p)), y, c))

    @pl.when(jnp.logical_not(diagonal))
    def _():
        left(geo.at[used], ws, wr, other)


def force_kernel(n_in, g_in, ready, f_out, lists_v, lists, sem):
    z = lax.axis_index("dom_0")
    seg = g_in[pl.ds(56, 16, stride=64), :]
    slot = g_in[pl.ds(57, 16, stride=64), :].astype(I32)
    lane = lax.broadcasted_iota(I32, (16, 128), 1)
    sub = lax.broadcasted_iota(I32, (16, 128), 0)
    hit = lax.shift_right_logical(slot, 4) == z
    mask = jnp.where(hit, 1.0, 0.0).astype(F32)
    low4 = lax.bitwise_and(slot, 15)
    code_a = seg + (sub * 8).astype(F32)
    who = lax.shift_right_logical(lane, 5) * 8 + lax.shift_right_logical(low4, 1)
    spot8 = lax.shift_right_logical(sub, 2) * 2 + lax.bitwise_and(low4, 1)
    code_b = (who * 8 + spot8).astype(F32)
    i0 = lax.broadcasted_iota(I32, (128, 128), 0)
    i1 = lax.broadcasted_iota(I32, (128, 128), 1)
    before = jnp.where(i0 < i1, 1.0, 0.0).astype(F32)
    inner = jnp.dot(mask, before, preferred_element_type=F32)
    total = jnp.dot(mask, jnp.ones((128, 128), F32), preferred_element_type=F32)
    j0 = lax.broadcasted_iota(I32, (16, 16), 0)
    j1 = lax.broadcasted_iota(I32, (16, 16), 1)
    above = jnp.dot(jnp.where(j1 < j0, 1.0, 0.0).astype(F32), total, preferred_element_type=F32)
    pos = (inner + above).astype(I32)
    high = jnp.where(hit, lax.shift_right_logical(pos, 7), -1)
    low = lax.bitwise_and(pos, 127)
    packed = jnp.zeros((32, 128), F32)
    for i in range(16):
        at = high[i : i + 1] == sub
        left = jnp.concatenate(
            [jnp.where(at, code_a[i : i + 1], 0.0), jnp.where(at, code_b[i : i + 1], 0.0)], axis=0
        )
        spot = jnp.where(low[i : i + 1] == i0, 1.0, 0.0).astype(F32)
        packed = packed + lax.dot_general(left, spot, (((1,), (1,)), ((), ())), preferred_element_type=F32)
    count = (total[15:16] + above[15:16]).astype(I32)
    code = packed[16:32].astype(I32)
    who = lax.shift_right_logical(code, 3)
    spot8 = lax.bitwise_and(code, 7)
    tile = packed[0:16].astype(I32)
    lists_v[0:16, :] = tile
    lists_v[16:32, :] = who * 48 + spot8
    lists_v[32:48, :] = jnp.where(sub * 128 + lane < count, who * 24 + spot8, 32 * 24)
    lists_v[48:56, :] = jnp.broadcast_to(count, (8, 128))
    copy = pltpu.make_async_copy(lists_v, lists, sem)
    copy.start()
    f_out[...] = jnp.zeros_like(f_out)
    copy.wait()

    ones = jnp.ones((8, 128), F32)
    blank = jnp.zeros((48, 128), BF16)
    gap = jnp.zeros((16, 256), BF16)

    def node_side(at):
        t = n_in[pl.ds(at, 6, stride=8), :]
        x0, x1, x2 = t[0:1], t[1:2], t[2:3]
        q = -(x0 * x0 + x1 * x1 + x2 * x2)
        full = jnp.concatenate([t, ones[0:1], q], axis=0)
        a, b, e = split3(full)
        side = jnp.concatenate([a, b, a, e, a, b], axis=0).astype(BF16)
        return jnp.concatenate(
            [
                jnp.concatenate([side, blank], axis=1),
                gap,
                jnp.concatenate([blank, side], axis=1),
                gap,
            ],
            axis=0,
        )

    def build(p):
        out = []
        left = []
        nothing = jnp.zeros((8, 128), F32)
        for i in range(2):
            q = p + i
            hi, lo = lax.shift_right_logical(q, 7), lax.bitwise_and(q, 127)
            tile = lists[hi, lo]
            t = g_in[pl.ds(lax.shift_right_logical(tile, 3) * 64 + lax.bitwise_and(tile, 7), 7, stride=8), :]
            t = jnp.concatenate([t, jnp.zeros((1, 128), F32)], axis=0)
            a = t.astype(BF16).astype(F32)
            left += [jnp.concatenate([a, a], axis=1), jnp.concatenate([t - a, nothing], axis=1)]
            out.append((ready[tile], node_side(lists[16 + hi, lo]), lists[32 + hi, lo]))
        return out, jnp.concatenate(left, axis=0).astype(BF16)

    def pressure(ew):
        press = jnp.exp2(ew[:, 0:128]) * jnp.maximum(ew[:, 128:256], 0.0)
        hi = press.astype(BF16)
        return hi, (press - hi.astype(F32)).astype(BF16)

    def run(size):
        def batch(p):
            made = [build(p + j) for j in range(0, size, 2)]
            ew = [
                [jnp.dot(tile, rhs, preferred_element_type=F32) for tile, rhs, _ in pairs] for pairs, _ in made
            ]
            ps = []
            for two in ew:
                (ha, la), (hb, lb) = pressure(two[0]), pressure(two[1])
                ps.append(
                    jnp.concatenate(
                        [jnp.concatenate([ha, hb], axis=1), jnp.concatenate([la, lb], axis=1)], axis=0
                    )
                )
            fs = [jnp.dot(m[1], q, preferred_element_type=F32) for m, q in zip(made, ps)]
            for (pairs, _), f in zip(made, fs):
                fa = -2.0 * (f[0:8, 0:128] + f[8:16, 0:128])
                fb = -2.0 * (f[16:24, 128:256] + f[24:32, 128:256])
                for at, v in ((pairs[0][2], fa[3:6]), (pairs[1][2], fb[3:6])):
                    here = pl.ds(at, 3, stride=8)
                    f_out[here, :] = f_out[here, :] + v

        return batch

    count = lists[48, 0]
    done = 0
    for size in SIZES:
        last = size == SIZES[-1]
        turns = (count - done + (size - 1 if last else 0)) // size
        body = run(size)

        def step(i, _, body=body, size=size, done=done):
            body(done + i * size)
            return 0

        lax.fori_loop(0, turns, step, 0)
        done = done + turns * size


def return_kernel(f, r_out, ys, yr):
    g, z = lax.axis_index("grp"), lax.axis_index("dom_0")
    y, c = lax.axis_index("dom_1"), lax.axis_index("dom_2")
    barrier = pltpu.get_barrier_semaphore()
    for a, b, e in TURNS:
        pl.semaphore_signal(
            barrier, inc=1, device_id=((g + a) % NX, z, (y + b) % NY, (c + e) % NC), device_id_type=MESH
        )
    pl.semaphore_wait(barrier, len(TURNS))
    me = g * 8 + y * 2 + c
    sends = []
    for k, (a, b, e) in enumerate(TURNS):
        dev = ((g + a) % NX, z, (y + b) % NY, (c + e) % NC)
        sends.append(start(f.at[dev[0] * 8 + dev[2] * 2 + dev[3]], r_out.at[me], ys.at[k], yr.at[k], dev))
    r_out[me] = f[me]
    for k, (a, b, e) in enumerate(TURNS):
        dev = ((g - a + NX) % NX, z, (y - b + NY) % NY, (c + e) % NC)
        landed(r_out.at[dev[0] * 8 + dev[2] * 2 + dev[3]], ys.at[k], yr.at[k], dev)
    for copy in sends:
        copy.wait_send()


def order_kernel(tgt, r_in, out):
    def one(i, _):
        out[pl.ds(i, 3, stride=128), :] = r_in[pl.ds(tgt[0, i], 3, stride=8), :]
        return 0

    lax.fori_loop(0, 128, one, 0, unroll=32)


def vmem():
    return pl.BlockSpec(memory_space=pltpu.VMEM)


def smem():
    return pl.BlockSpec(memory_space=pltpu.SMEM)


def shape(*dims, kind=F32):
    return jax.ShapeDtypeStruct(dims, kind)


def meet(node_state, node_dest, seg_nodes, seg_conn, pair_seg, pair_slot):
    dma = pltpu.SemaphoreType.DMA
    many = len(TURNS)
    nodes = jnp.transpose(node_state, (1, 0, 2)).reshape(768, 128)
    arrays = (node_dest.reshape(1, 128), nodes, seg_nodes, seg_conn, pair_seg, pair_slot)
    return pl.pallas_call(
        exchange_kernel,
        name="exchange",
        out_shape=(
            shape(32, 48, 128),
            shape(NZ, 64, 128),
            shape(1, 128, kind=I32),
            shape(NZ * 8, 128, 128, kind=BF16),
        ),
        in_specs=[pl.BlockSpec(memory_space=pltpu.HBM)] * 6,
        out_specs=(vmem(), vmem(), vmem(), vmem()),
        scratch_shapes=[
            pltpu.VMEM((1, 128), I32),
            pltpu.VMEM((768, 128), F32),
            pltpu.VMEM((6, 512), F32),
            pltpu.VMEM((3, 1024), I32),
            pltpu.VMEM((1, 4, 32), I32),
            pltpu.VMEM((1, 4, 32), I32),
            pltpu.VMEM((64, 128), F32),
            pltpu.VMEM((32, 48, 128), F32),
            pltpu.VMEM((128, 8, 128), F32),
            pltpu.VMEM((16, 128), I32),
            pltpu.SMEM((16, 128), I32),
            dma((7,)),
            dma((many,)),
            dma((many,)),
            dma((15,)),
            dma((15,)),
            dma,
            dma,
        ],
        compiler_params=pltpu.CompilerParams(collective_id=0, has_side_effects=True, vmem_limit_bytes=ROOM),
    )(*(pltpu.with_memory_space_constraint(v, pltpu.HBM) for v in arrays))


def give_back(forces):
    dma = pltpu.SemaphoreType.DMA
    many = len(TURNS)
    return pl.pallas_call(
        return_kernel,
        name="giveback",
        out_shape=shape(32, 24, 128),
        in_specs=[vmem()],
        out_specs=vmem(),
        scratch_shapes=[dma((many,)), dma((many,))],
        compiler_params=pltpu.CompilerParams(collective_id=1, has_side_effects=True, vmem_limit_bytes=ROOM),
    )(forces.reshape(33, 24, 128))


def shards(node_state, node_dest, seg_nodes, seg_conn, pair_seg, pair_slot):
    dma = pltpu.SemaphoreType.DMA
    many = len(TURNS)
    met, geos, tgt, ready = meet(node_state, node_dest, seg_nodes, seg_conn, pair_seg, pair_slot)
    forces = pl.pallas_call(
        force_kernel,
        name="forces",
        out_shape=shape(33 * 24, 128),
        in_specs=[vmem()] * 3,
        out_specs=vmem(),
        scratch_shapes=[pltpu.VMEM((56, 128), I32), pltpu.SMEM((56, 128), I32), dma],
        compiler_params=pltpu.CompilerParams(vmem_limit_bytes=ROOM),
    )(met.reshape(32 * 48, 128), geos.reshape(NZ * 64, 128), ready)
    back = give_back(forces)
    rows = pl.pallas_call(
        order_kernel,
        name="order",
        out_shape=shape(384, 128),
        in_specs=[smem(), vmem()],
        out_specs=vmem(),
        compiler_params=pltpu.CompilerParams(vmem_limit_bytes=ROOM),
    )(tgt, back.reshape(32 * 24, 128))
    return jnp.transpose(rows.reshape(3, 128, 128), (1, 0, 2))


def solution(mesh):
    split = Mesh(mesh.devices.reshape(NX, NZ, NY, NC), AXES)
    placed = (
        P(AXES, None, None),
        P(AXES),
        P(None, AXES),
        P(None, AXES),
        P(AXES, None, None),
        P(AXES, None, None),
    )
    return jax.shard_map(
        shards, mesh=split, in_specs=placed, out_specs=P(AXES, None, None), check_vma=False
    )
```

```python
import math

import jax
import jax.numpy as jnp
from jax import lax
from jax.experimental import pallas as pl
from jax.experimental.pallas import tpu as pltpu
from jax.sharding import Mesh
from jax.sharding import PartitionSpec as P

AXES = ("grp", "dom_0", "dom_1", "dom_2")
NX, NZ, NY, NC = 4, 16, 4, 2
MESH = pl.DeviceIdType.MESH
PARENT = (0, 1, 0, 3, 4, 3, 6, 6)
ORDER = (1, 3, 2, 4, 6, 5, 7, 8)
USED = 58
SIZES = (64, 32, 16, 8)
ROOM = 16 << 20
F32, BF16, I32 = jnp.float32, jnp.bfloat16, jnp.int32

time_step = 0.5
stiffness = 0.5
radius_sq = 0.5
root = math.sqrt(math.log2(math.e) / radius_sq)

TURNS = sorted(
    ((a, b, c) for a in range(NX) for b in range(NY) for c in range(NC) if a or b or c),
    key=lambda t: -min(t[0], NX - t[0]) - min(t[1], NY - t[1]),
)


def start(src, dst, ss, rs, dev):
    copy = pltpu.make_async_remote_copy(
        src_ref=src, dst_ref=dst, send_sem=ss, recv_sem=rs, device_id=dev, device_id_type=MESH
    )
    copy.start()
    return copy


def landed(dst, ss, rs, dev):
    pltpu.make_async_remote_copy(
        src_ref=dst, dst_ref=dst, send_sem=ss, recv_sem=rs, device_id=dev, device_id_type=MESH
    ).wait_recv()


def geometry(seg_nodes, conn, pseg, pslot, geo):
    corners = []
    for k in range(3):
        idx = jnp.concatenate([conn[k : k + 1, b * 128 : (b + 1) * 128] for b in range(8)], axis=0)
        hi = lax.shift_right_logical(idx, 7)
        lo = lax.bitwise_and(idx, 127)
        comps = []
        for i in range(6):
            got = None
            for q in range(4):
                table = jnp.broadcast_to(seg_nodes[i : i + 1, q * 128 : (q + 1) * 128], (8, 128))
                part = jnp.take_along_axis(table, lo, axis=1)
                got = part if got is None else jnp.where(hi == q, part, got)
            comps.append(got)
        corners.append(comps)
    a, b, c = corners
    e1 = [b[i] - a[i] for i in range(3)]
    e2 = [c[i] - a[i] for i in range(3)]
    n = [0.5 * (e1[(i + 1) % 3] * e2[(i + 2) % 3] - e1[(i + 2) % 3] * e2[(i + 1) % 3]) for i in range(3)]
    m = [(a[i] + b[i] + c[i]) / 3.0 for i in range(3)]
    u = [(a[i + 3] + b[i + 3] + c[i + 3]) / 3.0 for i in range(3)]
    off = sum(n[i] * (m[i] + time_step * u[i]) for i in range(3))
    values = [2.0 * root * v for v in m] + [-stiffness * v for v in n] + [stiffness * off]
    for i, v in enumerate(values):
        geo[8 * i : 8 * i + 8, :] = v
    tables = []
    for tab in (pseg, pslot):
        t = jnp.concatenate([tab[0].astype(F32), jnp.zeros((4, 96), F32)], axis=1)
        rows = [pltpu.roll(jnp.broadcast_to(t[r : r + 1], (8, 128)), 32 * r, 1) for r in range(4)]
        tables.append(rows[0] + rows[1] + rows[2] + rows[3])
    for i, t in enumerate(tables):
        geo[56 + i : 57 + i, :] = t[0:1]


def slots_of(dest, inverse, tgt):
    i0 = lax.broadcasted_iota(I32, (128, 128), 0)
    i1 = lax.broadcasted_iota(I32, (128, 128), 1)
    wide = jnp.broadcast_to(dest[0:1, :].astype(F32), (128, 128))
    same = (wide == wide.T) & (i0 < i1)
    rank = jnp.sum(jnp.where(same, 1.0, 0.0), axis=0, keepdims=True).astype(I32)
    d = dest[0:1, :]
    z = lax.shift_right_logical(d, 3)
    p = lax.bitwise_and(z, 3) * 8 + lax.bitwise_and(d, 7)
    slot = lax.shift_right_logical(z, 2) * 2 + rank
    tgt[...] = p * 24 + slot
    column = jnp.broadcast_to((p * 8 + slot).astype(F32), (128, 128)).T.astype(I32)
    for half in range(2):
        found = jnp.sum(jnp.where(column == i1 + 128 * half, i0, 0).astype(F32), axis=0, keepdims=True)
        inverse[8 * half : 8 * half + 8, :] = jnp.broadcast_to(found, (8, 128)).astype(I32)


def split3(t):
    a = t.astype(BF16).astype(F32)
    r = t - a
    b = r.astype(BF16).astype(F32)
    return a, b, r - b


def expand(chunk, out, base):
    row = lax.broadcasted_iota(I32, (8, 128), 0)
    nothing = jnp.zeros((16, 128), F32)

    def tile(t, _):
        v = chunk[pl.ds(t, 7, stride=8), :]
        m0, m1, m2 = v[0:1], v[1:2], v[2:3]
        q = -0.25 * (m0 * m0 + m1 * m1 + m2 * m2)
        full = jnp.concatenate([v, jnp.ones((1, 128), F32)], axis=0)
        dist = jnp.where((row < 3) | (row == 7), full, jnp.where(row == 6, q, 0.0))
        clear = jnp.where((row >= 3) & (row <= 6), full, 0.0)
        rows = []
        for side in (dist, clear):
            a, b, e = split3(side)
            rows += [a, a, b, a, e, b, nothing]
        out[base + t] = jnp.concatenate(rows, axis=0).T.astype(BF16)
        return 0

    lax.fori_loop(0, 8, tile, 0, unroll=8)


def exchange_kernel(
    dest_h, node_h, seg_h, conn_h, pseg_h, pslot_h,
    n_out, g_out, tgt, ready,
    dest, node, seg_nodes, conn, pseg, pslot, geo, s, xb, inv_v, inv, ins, ys, yr, zs, zr, ws, wr,
):
    g, z = lax.axis_index("grp"), lax.axis_index("dom_0")
    y, c = lax.axis_index("dom_1"), lax.axis_index("dom_2")
    loads = []
    for i, (src, dst) in enumerate(
        ((conn_h, conn), (seg_h, seg_nodes), (pseg_h, pseg), (pslot_h, pslot), (dest_h, dest), (node_h, node))
    ):
        load = pltpu.make_async_copy(src, dst, ins.at[i])
        load.start()
        loads.append(load)

    def zat(k):
        return (z + k + NZ) % NZ

    quad = z % 4
    other = (quad, z - quad + g, y, c)
    diagonal = quad == g
    peers = [((g + a) % NX, z, (y + b) % NY, (c + e) % NC) for a, b, e in TURNS]
    for e in sorted({d - p for d, p in enumerate(PARENT, 1)}):
        peers += [(g, zat(e), y, c), (g, zat(-e), y, c)]
    barrier = pltpu.get_barrier_semaphore()
    for peer in peers:
        pl.semaphore_signal(barrier, inc=1, device_id=peer, device_id_type=MESH)

    @pl.when(jnp.logical_not(diagonal))
    def _():
        pl.semaphore_signal(barrier, inc=1, device_id=other, device_id_type=MESH)

    for load in loads[:4]:
        load.wait()
    geometry(seg_nodes, conn, pseg, pslot, geo)
    pl.semaphore_wait(barrier, len(peers) + jnp.where(diagonal, 0, 1))
    me = g * 8 + y * 2 + c

    def number(sign, d):
        return (d if sign > 0 else 8 + d) - 1

    most = {1: 8, -1: 7}

    def children(p, sign):
        mine = [d for d in range(1, most[sign] + 1) if PARENT[d - 1] == p]
        return sorted(mine, key=lambda d: (d not in PARENT, -d))

    used = pl.ds(0, USED)

    def forward_z(sign, p, src):
        for d in children(p, sign):
            k = number(sign, d)
            start(src, g_out.at[zat(-sign * p), used], zs.at[k], zr.at[k], (g, zat(sign * (d - p)), y, c))

    def arrive_z(sign, d):
        k = number(sign, d)
        slot = g_out.at[zat(-sign * d), used]
        landed(slot, zs.at[k], zr.at[k], (g, zat(-sign * (d - PARENT[d - 1])), y, c))
        forward_z(sign, d, slot)
        expand(g_out.at[zat(-sign * d)], ready, zat(-sign * d) * 8)

    def node_send(k):
        a, b, e = TURNS[k]
        dev = ((g + a) % NX, z, (y + b) % NY, (c + e) % NC)
        start(s.at[dev[0] * 8 + dev[2] * 2 + dev[3]], n_out.at[me], ys.at[k], yr.at[k], dev)

    @pl.when(jnp.logical_not(diagonal))
    def _():
        start(geo.at[used], g_out.at[other[1], used], ws, wr, other)

    @pl.when(diagonal)
    def _():
        forward_z(1, 0, geo.at[used])
        forward_z(-1, 0, geo.at[used])
        g_out[z] = geo[...]

    loads[4].wait()
    slots_of(dest, inv_v, tgt)
    table = pltpu.make_async_copy(inv_v, inv, ins.at[6])
    table.start()
    loads[5].wait()

    def turn(j, _):
        at = pl.multiple_of(8 * j, 8)
        for i in range(3):
            x = node[pl.ds(i * 128 + at, 8), :]
            xb[pl.ds(at, 8), i, :] = x * root
            xb[pl.ds(at, 8), i + 3, :] = x + time_step * node[pl.ds((i + 3) * 128 + at, 8), :]
        return 0

    lax.fori_loop(0, 16, turn, 0, unroll=2)
    table.wait()

    def place(p, _):
        for k in range(8):
            block = xb[lax.bitwise_and(inv[8 * (p // 16), (p % 16) * 8 + k], 127)]
            s[p, pl.ds(k, 6, stride=8), :] = block[0:6]
        return 0

    lax.fori_loop(0, 32, place, 0, unroll=2)
    n_out[me] = s[me]
    first = 0
    for k in range(first):
        node_send(k)

    @pl.when(jnp.logical_not(diagonal))
    def _():
        landed(g_out.at[z, used], ws, wr, other)
        forward_z(1, 0, g_out.at[z, used])
        forward_z(-1, 0, g_out.at[z, used])

    for k in range(first, len(TURNS)):
        node_send(k)

    expand(g_out.at[z], ready, z * 8)
    for d in ORDER:
        for sign in (1, -1):
            if d <= most[sign]:
                arrive_z(sign, d)
    for k, (a, b, e) in enumerate(TURNS):
        dev = ((g - a + NX) % NX, z, (y - b + NY) % NY, (c + e) % NC)
        landed(n_out.at[dev[0] * 8 + dev[2] * 2 + dev[3]], ys.at[k], yr.at[k], dev)

    def left(src, ss, rs, dev):
        pltpu.make_async_remote_copy(
            src_ref=src, dst_ref=src, send_sem=ss, recv_sem=rs, device_id=dev, device_id_type=MESH
        ).wait_send()

    for k, (a, b, e) in enumerate(TURNS):
        dev = ((g + a) % NX, z, (y + b) % NY, (c + e) % NC)
        left(s.at[dev[0] * 8 + dev[2] * 2 + dev[3]], ys.at[k], yr.at[k], dev)
    for sign in (1, -1):
        for d in range(1, most[sign] + 1):
            k = number(sign, d)
            p = PARENT[d - 1]
            left(g_out.at[zat(-sign * p), used], zs.at[k], zr.at[k], (g, zat(sign * (d - p)), y, c))

    @pl.when(jnp.logical_not(diagonal))
    def _():
        left(geo.at[used], ws, wr, other)


def force_kernel(n_in, g_in, ready, f_out, lists_v, lists, sem):
    z = lax.axis_index("dom_0")
    seg = g_in[pl.ds(56, 16, stride=64), :]
    slot = g_in[pl.ds(57, 16, stride=64), :].astype(I32)
    lane = lax.broadcasted_iota(I32, (16, 128), 1)
    sub = lax.broadcasted_iota(I32, (16, 128), 0)
    hit = lax.shift_right_logical(slot, 4) == z
    mask = jnp.where(hit, 1.0, 0.0).astype(F32)
    low4 = lax.bitwise_and(slot, 15)
    code_a = seg + (sub * 8).astype(F32)
    who = lax.shift_right_logical(lane, 5) * 8 + lax.shift_right_logical(low4, 1)
    spot8 = lax.shift_right_logical(sub, 2) * 2 + lax.bitwise_and(low4, 1)
    code_b = (who * 8 + spot8).astype(F32)
    i0 = lax.broadcasted_iota(I32, (128, 128), 0)
    i1 = lax.broadcasted_iota(I32, (128, 128), 1)
    before = jnp.where(i0 < i1, 1.0, 0.0).astype(F32)
    inner = jnp.dot(mask, before, preferred_element_type=F32)
    total = jnp.dot(mask, jnp.ones((128, 128), F32), preferred_element_type=F32)
    j0 = lax.broadcasted_iota(I32, (16, 16), 0)
    j1 = lax.broadcasted_iota(I32, (16, 16), 1)
    above = jnp.dot(jnp.where(j1 < j0, 1.0, 0.0).astype(F32), total, preferred_element_type=F32)
    pos = (inner + above).astype(I32)
    high = jnp.where(hit, lax.shift_right_logical(pos, 7), -1)
    low = lax.bitwise_and(pos, 127)
    packed = jnp.zeros((32, 128), F32)
    for i in range(16):
        at = high[i : i + 1] == sub
        left = jnp.concatenate(
            [jnp.where(at, code_a[i : i + 1], 0.0), jnp.where(at, code_b[i : i + 1], 0.0)], axis=0
        )
        spot = jnp.where(low[i : i + 1] == i0, 1.0, 0.0).astype(F32)
        packed = packed + lax.dot_general(left, spot, (((1,), (1,)), ((), ())), preferred_element_type=F32)
    count = (total[15:16] + above[15:16]).astype(I32)
    code = packed[16:32].astype(I32)
    who = lax.shift_right_logical(code, 3)
    spot8 = lax.bitwise_and(code, 7)
    tile = packed[0:16].astype(I32)
    at_node = who * 48 + spot8
    at_force = jnp.where(sub * 128 + lane < count, who * 24 + spot8, 32 * 24)
    for i, v in enumerate((tile, at_node, at_force)):
        lists_v[2 * i : 2 * i + 2, :] = v[0:2]
        lists_v[8 + 16 * i : 24 + 16 * i, :] = v
    lists_v[6:8, :] = jnp.broadcast_to(count, (2, 128))
    copy = pltpu.make_async_copy(lists_v.at[pl.ds(0, 8)], lists.at[pl.ds(0, 8)], sem)
    copy.start()
    f_out[...] = jnp.zeros_like(f_out)
    copy.wait()

    @pl.when(lists[6, 0] > 256)
    def _():
        rest = pltpu.make_async_copy(lists_v.at[pl.ds(8, 48)], lists.at[pl.ds(8, 48)], sem)
        rest.start()
        rest.wait()

    ones = jnp.ones((8, 128), F32)
    blank = jnp.zeros((48, 128), BF16)
    gap = jnp.zeros((16, 256), BF16)

    def node_side(at):
        t = n_in[pl.ds(at, 6, stride=8), :]
        x0, x1, x2 = t[0:1], t[1:2], t[2:3]
        q = -(x0 * x0 + x1 * x1 + x2 * x2)
        full = jnp.concatenate([t, ones[0:1], q], axis=0)
        a, b, e = split3(full)
        side = jnp.concatenate([a, b, a, e, a, b], axis=0).astype(BF16)
        return jnp.concatenate(
            [
                jnp.concatenate([side, blank], axis=1),
                gap,
                jnp.concatenate([blank, side], axis=1),
                gap,
            ],
            axis=0,
        )

    def build(p):
        out = []
        left = []
        nothing = jnp.zeros((8, 128), F32)
        for i in range(2):
            q = p + i
            hi, lo = lax.shift_right_logical(q, 7), lax.bitwise_and(q, 127)
            tile = lists[jnp.where(hi < 2, hi, 8 + hi), lo]
            t = g_in[pl.ds(lax.shift_right_logical(tile, 3) * 64 + lax.bitwise_and(tile, 7), 7, stride=8), :]
            t = jnp.concatenate([t, jnp.zeros((1, 128), F32)], axis=0)
            a = t.astype(BF16).astype(F32)
            left += [jnp.concatenate([a, a], axis=1), jnp.concatenate([t - a, nothing], axis=1)]
            out.append((ready[tile], node_side(lists[jnp.where(hi < 2, 2 + hi, 24 + hi), lo]), lists[jnp.where(hi < 2, 4 + hi, 40 + hi), lo]))
        return out, jnp.concatenate(left, axis=0).astype(BF16)

    def pressure(ew):
        press = jnp.exp2(ew[:, 0:128]) * jnp.maximum(ew[:, 128:256], 0.0)
        hi = press.astype(BF16)
        return hi, (press - hi.astype(F32)).astype(BF16)

    def run(size):
        def batch(p):
            made = [build(p + j) for j in range(0, size, 2)]
            ew = [
                [jnp.dot(tile, rhs, preferred_element_type=F32) for tile, rhs, _ in pairs] for pairs, _ in made
            ]
            ps = []
            for two in ew:
                (ha, la), (hb, lb) = pressure(two[0]), pressure(two[1])
                ps.append(
                    jnp.concatenate(
                        [jnp.concatenate([ha, hb], axis=1), jnp.concatenate([la, lb], axis=1)], axis=0
                    )
                )
            fs = [jnp.dot(m[1], q, preferred_element_type=F32) for m, q in zip(made, ps)]
            for (pairs, _), f in zip(made, fs):
                fa = -2.0 * (f[0:8, 0:128] + f[8:16, 0:128])
                fb = -2.0 * (f[16:24, 128:256] + f[24:32, 128:256])
                for at, v in ((pairs[0][2], fa[3:6]), (pairs[1][2], fb[3:6])):
                    here = pl.ds(at, 3, stride=8)
                    f_out[here, :] = f_out[here, :] + v

        return batch

    count = lists[6, 0]
    done = 0
    for size in SIZES:
        last = size == SIZES[-1]
        turns = (count - done + (size - 1 if last else 0)) // size
        body = run(size)

        def step(i, _, body=body, size=size, done=done):
            body(done + i * size)
            return 0

        lax.fori_loop(0, turns, step, 0)
        done = done + turns * size


def return_kernel(f, r_out, ys, yr):
    g, z = lax.axis_index("grp"), lax.axis_index("dom_0")
    y, c = lax.axis_index("dom_1"), lax.axis_index("dom_2")
    barrier = pltpu.get_barrier_semaphore()
    for a, b, e in TURNS:
        pl.semaphore_signal(
            barrier, inc=1, device_id=((g + a) % NX, z, (y + b) % NY, (c + e) % NC), device_id_type=MESH
        )
    pl.semaphore_wait(barrier, len(TURNS))
    me = g * 8 + y * 2 + c
    sends = []
    for k, (a, b, e) in enumerate(TURNS):
        dev = ((g + a) % NX, z, (y + b) % NY, (c + e) % NC)
        sends.append(start(f.at[dev[0] * 8 + dev[2] * 2 + dev[3]], r_out.at[me], ys.at[k], yr.at[k], dev))
    r_out[me] = f[me]
    for k, (a, b, e) in enumerate(TURNS):
        dev = ((g - a + NX) % NX, z, (y - b + NY) % NY, (c + e) % NC)
        landed(r_out.at[dev[0] * 8 + dev[2] * 2 + dev[3]], ys.at[k], yr.at[k], dev)
    for copy in sends:
        copy.wait_send()


def order_kernel(tgt, r_in, out):
    def one(i, _):
        out[pl.ds(i, 3, stride=128), :] = r_in[pl.ds(tgt[0, i], 3, stride=8), :]
        return 0

    lax.fori_loop(0, 128, one, 0, unroll=32)


def vmem():
    return pl.BlockSpec(memory_space=pltpu.VMEM)


def smem():
    return pl.BlockSpec(memory_space=pltpu.SMEM)


def shape(*dims, kind=F32):
    return jax.ShapeDtypeStruct(dims, kind)


def meet(node_state, node_dest, seg_nodes, seg_conn, pair_seg, pair_slot):
    dma = pltpu.SemaphoreType.DMA
    many = len(TURNS)
    nodes = jnp.transpose(node_state, (1, 0, 2)).reshape(768, 128)
    arrays = (node_dest.reshape(1, 128), nodes, seg_nodes, seg_conn, pair_seg, pair_slot)
    return pl.pallas_call(
        exchange_kernel,
        name="exchange",
        out_shape=(
            shape(32, 48, 128),
            shape(NZ, 64, 128),
            shape(1, 128, kind=I32),
            shape(NZ * 8, 128, 128, kind=BF16),
        ),
        in_specs=[pl.BlockSpec(memory_space=pltpu.HBM)] * 6,
        out_specs=(vmem(), vmem(), vmem(), vmem()),
        scratch_shapes=[
            pltpu.VMEM((1, 128), I32),
            pltpu.VMEM((768, 128), F32),
            pltpu.VMEM((6, 512), F32),
            pltpu.VMEM((3, 1024), I32),
            pltpu.VMEM((1, 4, 32), I32),
            pltpu.VMEM((1, 4, 32), I32),
            pltpu.VMEM((64, 128), F32),
            pltpu.VMEM((32, 48, 128), F32),
            pltpu.VMEM((128, 8, 128), F32),
            pltpu.VMEM((16, 128), I32),
            pltpu.SMEM((16, 128), I32),
            dma((7,)),
            dma((many,)),
            dma((many,)),
            dma((15,)),
            dma((15,)),
            dma,
            dma,
        ],
        compiler_params=pltpu.CompilerParams(collective_id=0, has_side_effects=True, vmem_limit_bytes=ROOM),
    )(*(pltpu.with_memory_space_constraint(v, pltpu.HBM) for v in arrays))


def give_back(forces):
    dma = pltpu.SemaphoreType.DMA
    many = len(TURNS)
    return pl.pallas_call(
        return_kernel,
        name="giveback",
        out_shape=shape(32, 24, 128),
        in_specs=[vmem()],
        out_specs=vmem(),
        scratch_shapes=[dma((many,)), dma((many,))],
        compiler_params=pltpu.CompilerParams(collective_id=1, has_side_effects=True, vmem_limit_bytes=ROOM),
    )(forces.reshape(33, 24, 128))


def shards(node_state, node_dest, seg_nodes, seg_conn, pair_seg, pair_slot):
    dma = pltpu.SemaphoreType.DMA
    many = len(TURNS)
    met, geos, tgt, ready = meet(node_state, node_dest, seg_nodes, seg_conn, pair_seg, pair_slot)
    forces = pl.pallas_call(
        force_kernel,
        name="forces",
        out_shape=shape(33 * 24, 128),
        in_specs=[vmem()] * 3,
        out_specs=vmem(),
        scratch_shapes=[pltpu.VMEM((56, 128), I32), pltpu.SMEM((56, 128), I32), dma],
        compiler_params=pltpu.CompilerParams(vmem_limit_bytes=ROOM),
    )(met.reshape(32 * 48, 128), geos.reshape(NZ * 64, 128), ready)
    back = give_back(forces)
    rows = pl.pallas_call(
        order_kernel,
        name="order",
        out_shape=shape(384, 128),
        in_specs=[smem(), vmem()],
        out_specs=vmem(),
        compiler_params=pltpu.CompilerParams(vmem_limit_bytes=ROOM),
    )(tgt, back.reshape(32 * 24, 128))
    return jnp.transpose(rows.reshape(3, 128, 128), (1, 0, 2))


def solution(mesh):
    split = Mesh(mesh.devices.reshape(NX, NZ, NY, NC), AXES)
    placed = (
        P(AXES, None, None),
        P(AXES),
        P(None, AXES),
        P(None, AXES),
        P(AXES, None, None),
        P(AXES, None, None),
    )
    return jax.shard_map(
        shards, mesh=split, in_specs=placed, out_specs=P(AXES, None, None), check_vma=False
    )
```
